32 devices in a mesh: grp: 2 (over x), ctx: 16 (over z, y, core).
Axes of the slice: x: 2, y: 2, z: 4, core: 2. Of those that a mesh axis runs over, the one named last changes fastest.
Arguments:
- cache_keys: bfloat16 [2048, 512], P(('grp', 'ctx')), parts along dimension 0, may hold values from -4 to 4
- cache_values: bfloat16 [2048, 512], P(('grp', 'ctx')), parts along dimension 0, may hold values from -4 to 4
- new_queries: bfloat16 [2048, 4096], P(('grp', 'ctx')), parts along dimension 0, may hold values from -600 to 600
- new_keys: bfloat16 [2048, 512], P(('grp', 'ctx')), parts along dimension 0, may hold values from -4 to 4
- new_values: bfloat16 [2048, 512], P(('grp', 'ctx')), parts along dimension 0, may hold values from -4 to 4
- cont_queries: bfloat16 [64, 4096], P(('grp', 'ctx')), parts along dimension 0, may hold values from -600 to 600
- suffix_keys: bfloat16 [64, 128, 512], P(('grp', 'ctx')), parts along dimension 0, may hold values from -4 to 4
- suffix_values: bfloat16 [64, 128, 512], P(('grp', 'ctx')), parts along dimension 0, may hold values from -4 to 4
- window_start: int32 [2], P('grp'), parts along dimension 0, may hold values from 0 to 255
- prefix_length: int32 [2], P('grp'), parts along dimension 0, may hold values from 512 to 1024
- suffix_length: int32 [64], P(('grp', 'ctx')), parts along dimension 0, may hold values from 2 to 128
Outputs:
- prompt_out: bfloat16 [2048, 4096], P(('grp', 'ctx')), parts along dimension 0
- cont_out: bfloat16 [64, 4096], P(('grp', 'ctx')), parts along dimension 0
The draws below stay inside these ranges and needn't reach their ends.
There are 2 independent parts, one for each index of `grp`. The reference program is written for one: setup_inputs(seed, part) draws one part's arguments, and reference() takes and returns one part's arrays. A program takes and returns all parts, laid end to end along the dimension named above; each array names one. Nothing has to cross between parts.
All inputs are finite; a program needn't handle non-finite values.
Results may differ from the reference program's by a relative error of at most 0.009.
Values may be sent and summed in bfloat16 or wider, within the bound.
A program may use at most 192 MiB of HBM per device.

```python
import jax
import jax.numpy as jnp
from jax import lax

H = 32
KVH = 4
HD = 128
GROUP = 8
Q_DEV = 64
C_DEV = 2
SUF = 128
NEW = 1024
WIN = 1024
CONT = 32
N_CTX = 16


def prompt_pair(key):
    folded = jax.random.fold_in(key, 71)
    seed_query, seed_key = jax.random.split(folded, 2)
    queries = jnp.clip(jax.random.normal(seed_query, (NEW, H, HD), jnp.float32), -4.0, 4.0)
    key_rows = jnp.clip(jax.random.normal(seed_key, (NEW, KVH, HD), jnp.float32), -4.0, 4.0)
    return (queries.reshape(NEW, H * HD), key_rows.reshape(NEW, KVH * HD))


def cont_pair(key):
    folded = jax.random.fold_in(key, 83)
    seed_query, seed_key = jax.random.split(folded, 2)
    queries = jnp.clip(jax.random.normal(seed_query, (CONT, H, HD), jnp.float32), -4.0, 4.0)
    suffix_rows = jnp.clip(jax.random.normal(seed_key, (CONT, SUF, KVH, HD), jnp.float32), -4.0, 4.0)
    return (queries.reshape(CONT, H * HD), suffix_rows.reshape(CONT, SUF, KVH * HD))


def draw_new_queries(key, part):
    return prompt_pair(key)[0].astype(jnp.bfloat16)


def draw_new_keys(key, part):
    return prompt_pair(key)[1].astype(jnp.bfloat16)


def draw_cont_queries(key, part):
    return cont_pair(key)[0].astype(jnp.bfloat16)


def draw_suffix_keys(key, part):
    return cont_pair(key)[1].astype(jnp.bfloat16)


def set_ends(entries, key, low, top_value):
    shape = entries.shape
    index_at = [jax.random.randint(jax.random.fold_in(key, axis), (), 0, shape[axis]) for axis in range(len(shape))]
    entries = entries.at[tuple(index_at)].set(low)
    longest = shape.index(max(shape))
    index_at[longest] = (index_at[longest] + 1) % shape[longest]
    return entries.at[tuple(index_at)].set(top_value)


def steps_of(own_key, shape, pieces, smallest, largest):
    loudness = 1.0
    for position, parts in pieces:
        draws = jax.random.uniform(jax.random.fold_in(jax.random.fold_in(own_key, 6), position), (parts,), jnp.float32, smallest / len(pieces), largest / len(pieces))
        loudness = loudness * jnp.repeat(jnp.exp(draws), shape[position] // parts).reshape((-1,) + (1,) * (len(shape) - 1 - position))
    return loudness


def normal_values(own_key, shape, deviation, most, cuts=(), kind=jnp.bfloat16):
    factor_of = steps_of(own_key, shape, cuts, -0.22, 0.18) if cuts else 1.0
    values = jax.random.normal(own_key, shape, jnp.float32) * deviation * factor_of
    return jnp.minimum(jnp.maximum(values, -most), most).astype(kind)


def setup_inputs(seed: int = 0, part: int = 0) -> dict:
    seeds = jax.random.split(jax.random.key(seed), 12)
    part_splits = jax.random.split(jax.random.fold_in(seeds[11], part), 12)
    cache_keys = normal_values(part_splits[0], (WIN, KVH * HD), 1.0, 4.0, ((0, 16),))
    cache_values = normal_values(part_splits[1], (WIN, KVH * HD), 1.0, 4.0, ((0, 16),))
    new_queries = draw_new_queries(jax.random.fold_in(jax.random.fold_in(seeds[11], part), 71), part)
    new_keys = draw_new_keys(jax.random.fold_in(jax.random.fold_in(seeds[11], part), 71), part)
    new_values = normal_values(part_splits[4], (NEW, KVH * HD), 1.0, 4.0, ((0, 16),))
    cont_queries = draw_cont_queries(jax.random.fold_in(jax.random.fold_in(seeds[11], part), 71), part)
    suffix_keys = draw_suffix_keys(jax.random.fold_in(jax.random.fold_in(seeds[11], part), 71), part)
    suffix_values = normal_values(part_splits[7], (CONT, SUF, KVH * HD), 1.0, 4.0, ((0, 16),))
    window_start = jax.random.randint(part_splits[8], (1,), 0, WIN // 4).astype(jnp.int32)
    prefix_length = jax.random.randint(part_splits[9], (1,), WIN // 2, WIN + 1).astype(jnp.int32)
    suffix_length = set_ends(jax.random.randint(part_splits[10], (CONT,), 2, SUF + 1), jax.random.fold_in(part_splits[10], 1), 2, SUF).astype(jnp.int32)
    return dict(cache_keys=cache_keys, cache_values=cache_values, new_queries=new_queries, new_keys=new_keys, new_values=new_values, cont_queries=cont_queries, suffix_keys=suffix_keys, suffix_values=suffix_values, window_start=window_start, prefix_length=prefix_length, suffix_length=suffix_length)


def reference(cache_keys, cache_values, new_queries, new_keys, new_values, cont_queries, suffix_keys, suffix_values, window_start, prefix_length, suffix_length):
    score_scale = HD ** -0.5
    total_rows = WIN + NEW
    every_key = jnp.concatenate([cache_keys, new_keys], axis=0).astype(jnp.float32).reshape(total_rows, KVH, HD)
    every_value = jnp.concatenate([cache_values, new_values], axis=0).astype(jnp.float32).reshape(total_rows, KVH, HD)
    key_index = jnp.arange(total_rows, dtype=jnp.int32)
    in_cache = key_index < WIN
    cache_ok = in_cache & (key_index >= window_start[0]) & (key_index < prefix_length[0])
    prompt_index = key_index - WIN

    def prompt_block(block):
        begin_row = (block * Q_DEV).astype(jnp.int32)
        query_rows = lax.dynamic_slice_in_dim(new_queries, begin_row, Q_DEV, 0)
        heads = query_rows.astype(jnp.float32).reshape(Q_DEV, KVH, GROUP, HD)
        query_index = begin_row + jnp.arange(Q_DEV, dtype=jnp.int32)
        visible = cache_ok[None, :] | ((~in_cache)[None, :] & (prompt_index[None, :] <= query_index[:, None]))
        mask = visible[:, None, None, :]
        scores = jnp.einsum('rkgd,lkd->rkgl', heads, every_key) * score_scale
        scores = jnp.where(mask, scores, -1e30)
        row_max = jnp.max(scores, axis=-1, keepdims=True)
        probs = jnp.where(mask, jnp.exp(scores - row_max), 0.0)
        row_sum = jnp.sum(probs, axis=-1)
        rounded = lax.optimization_barrier(probs.astype(jnp.bfloat16)).astype(jnp.float32)
        mixed = jnp.einsum('rkgl,lkd->rkgd', rounded, every_value) / row_sum[..., None]
        return mixed.reshape(Q_DEV, H * HD).astype(jnp.bfloat16)

    prompt_out = lax.map(prompt_block, jnp.arange(N_CTX, dtype=jnp.int32)).reshape(NEW, H * HD)
    prefix_ok = cache_ok | (~in_cache)

    def cont_block(block):
        begin_row = (block * C_DEV).astype(jnp.int32)
        heads = lax.dynamic_slice_in_dim(cont_queries, begin_row, C_DEV, 0).astype(jnp.float32).reshape(C_DEV, KVH, GROUP, HD)
        own_keys = lax.dynamic_slice_in_dim(suffix_keys, begin_row, C_DEV, 0).astype(jnp.float32).reshape(C_DEV, SUF, KVH, HD)
        own_values = lax.dynamic_slice_in_dim(suffix_values, begin_row, C_DEV, 0).astype(jnp.float32).reshape(C_DEV, SUF, KVH, HD)
        lengths = lax.dynamic_slice_in_dim(suffix_length, begin_row, C_DEV, 0)
        prefix_mask = prefix_ok[None, None, None, :]
        suffix_mask = (jnp.arange(SUF, dtype=jnp.int32)[None, :] < lengths[:, None])[:, None, None, :]
        prefix_scores = jnp.einsum('ckgd,lkd->ckgl', heads, every_key) * score_scale
        prefix_scores = jnp.where(prefix_mask, prefix_scores, -1e30)
        suffix_scores = jnp.einsum('ckgd,cskd->ckgs', heads, own_keys) * score_scale
        suffix_scores = jnp.where(suffix_mask, suffix_scores, -1e30)
        row_max = jnp.maximum(jnp.max(prefix_scores, axis=-1), jnp.max(suffix_scores, axis=-1))[..., None]
        prefix_probs = jnp.where(prefix_mask, jnp.exp(prefix_scores - row_max), 0.0)
        suffix_probs = jnp.where(suffix_mask, jnp.exp(suffix_scores - row_max), 0.0)
        row_sum = jnp.sum(prefix_probs, axis=-1) + jnp.sum(suffix_probs, axis=-1)
        prefix_rounded = lax.optimization_barrier(prefix_probs.astype(jnp.bfloat16)).astype(jnp.float32)
        suffix_rounded = lax.optimization_barrier(suffix_probs.astype(jnp.bfloat16)).astype(jnp.float32)
        mixed = jnp.einsum('ckgl,lkd->ckgd', prefix_rounded, every_value) + jnp.einsum('ckgs,cskd->ckgd', suffix_rounded, own_values)
        mixed = mixed / row_sum[..., None]
        return mixed.reshape(C_DEV, H * HD).astype(jnp.bfloat16)

    cont_out = lax.map(cont_block, jnp.arange(N_CTX, dtype=jnp.int32)).reshape(CONT, H * HD)
    return prompt_out, cont_out
```

```python
import functools
import math

import jax
import jax.numpy as jnp
from jax import lax
from jax.experimental import pallas as pl
from jax.experimental.pallas import tpu as pltpu
from jax.sharding import PartitionSpec as P

KVH = 4
HD = 128
GROUP = 8
CORES = 2
PIECES = 4
EXTRA = 3
ORDER = (EXTRA, 0, 1, 2)
MESH = pl.DeviceIdType.MESH
SCALE2 = HD ** (-0.5) * math.log2(math.e)
HIDDEN = 1 << 30


def kernel(
    n_z,
    n_y,
    ck_ref,
    cv_ref,
    nq_ref,
    nk_ref,
    nv_ref,
    cq_hbm,
    sk_ref,
    sv_ref,
    start_hbm,
    prefix_hbm,
    length_hbm,
    out_ref,
    cont_ref,
    kv,
    q,
    sk,
    sv,
    rows16,
    limit,
    row_max,
    row_sum,
    acc,
    cq_ref,
    start_ref,
    prefix_ref,
    length_ref,
    local_sem,
    query_sem,
    suffix_sem,
    recv_sem,
    pair_sem,
    send_sem,
    small_sem,
):
    half = ck_ref.shape[0]
    prompt_rows = nq_ref.shape[0]
    conts = cq_hbm.shape[0]
    suffix_rows = sk_ref.shape[1]
    many = GROUP * prompt_rows
    total = many + GROUP * conts
    me = lax.axis_index("ctx")
    core = me % CORES
    chip = me // CORES
    y = chip % n_y
    z = chip // n_y

    def device(zz, yy, cc):
        return (zz * n_y + yy) * CORES + cc

    own = []
    for p, ref in enumerate((ck_ref, nk_ref, cv_ref, nv_ref)):
        copy = pltpu.make_async_copy(
            ref, kv.at[me, p // 2, pl.ds((p % 2) * half, half)], local_sem.at[p]
        )
        copy.start()
        own.append(copy)
    for h in range(KVH):
        for g in range(GROUP):
            pltpu.make_async_copy(
                nq_ref.at[:, pl.ds((h * GROUP + g) * HD, HD)],
                q.at[h, pl.ds(g * prompt_rows, prompt_rows)],
                query_sem,
            ).start()
    suffix_copies = [
        pltpu.make_async_copy(sk_ref, sk, suffix_sem.at[0]),
        pltpu.make_async_copy(sv_ref, sv, suffix_sem.at[1]),
    ]
    small_copies = [
        pltpu.make_async_copy(src, dst, small_sem.at[i])
        for i, (src, dst) in enumerate(
            (
                (cq_hbm, cq_ref),
                (start_hbm, start_ref),
                (prefix_hbm, prefix_ref),
                (length_hbm, length_ref),
            )
        )
    ]
    for copy in suffix_copies + small_copies:
        copy.start()

    barrier = pltpu.get_barrier_semaphore()

    def greet(target):
        pl.semaphore_signal(barrier, inc=1, device_id={"ctx": target}, device_id_type=MESH)

    greet(device(z, y, 1 - core))
    if n_y == 2:
        greet(device(z, 1 - y, core))

    @pl.when(z > 0)
    def _():
        greet(device(z - 1, y, core))

    @pl.when(z < n_z - 1)
    def _():
        greet(device(z + 1, y, core))

    line_neighbours = (z + n_z - 1) // n_z + (2 * n_z - 2 - z) // n_z
    pl.semaphore_wait(barrier, n_y + line_neighbours)

    def piece(source, p):
        return kv.at[source, p // 2, pl.ds((p % 2) * half, half)]

    def send(source, p, target, kind):
        ref = piece(source, p)
        sem = pair_sem.at[source] if kind == 2 else recv_sem.at[source, p]
        pltpu.make_async_remote_copy(
            src_ref=ref,
            dst_ref=ref,
            send_sem=send_sem.at[source, kind],
            recv_sem=sem,
            device_id={"ctx": target},
            device_id_type=MESH,
        ).start()

    def arrived(source, p):
        ref = piece(source, p)
        pltpu.make_async_copy(ref, ref, recv_sem.at[source, p]).wait()

    def pair_arrived(source):
        pltpu.make_async_copy(kv.at[source], kv.at[source], pair_sem.at[source]).wait()

    def sent(source, kind, pieces=PIECES):
        ref = kv.at[source]
        if pieces == 1:
            ref = piece(source, EXTRA)
        elif pieces < PIECES:
            ref = kv.at[source, :, pl.ds(0, pieces * half // 2)]
        pltpu.make_async_copy(ref, ref, send_sem.at[source, kind]).wait()

    def by_line(zs):
        return ((zs < z) & (zs < n_z - 2)) | ((zs > z) & (zs > 1))

    def not_by_line(zs):
        return ((zs < z) & (zs >= n_z - 2)) | ((zs > z) & (zs <= 1)) | (zs == z)

    partner = device(z, y, 1 - core)
    across = device(z, 1 - y, core)
    above = device(z + 1, y, core)
    below = device(z - 1, y, core)

    for p in ORDER:
        own[p].wait()

        @pl.when(z < n_z - 1)
        def _():
            send(me, p, above, 0)

        if n_y == 2:
            send(me, p, across, 4 if p == EXTRA else 1)

        @pl.when(z > 0)
        def _():
            send(me, p, below, 3)

        send(me, p, partner, 2)

    near = jnp.minimum(z, n_z - 1 - z)

    def z_at(t):
        if isinstance(t, int) and t == 0:
            return z
        step = (t + 1) // 2
        both = z + step * (1 - 2 * (t % 2))
        far = jnp.where(z + z < n_z - 1, t, n_z - 1 - t)
        return jnp.where(t <= 2 * near, both, far)

    row = lax.broadcasted_iota(jnp.int32, (total, HD), 0)
    limit[...] = jnp.where(row < many, me * prompt_rows + row % prompt_rows, HIDDEN - 1)
    row_max[...] = jnp.full_like(row_max, -1e30)
    row_sum[...] = jnp.zeros_like(row_sum)
    acc[...] = jnp.zeros_like(acc)
    for copy in small_copies:
        copy.wait()
    for h in range(KVH):
        for g in range(GROUP):
            column = (h * GROUP + g) * HD
            rows16[h, g * conts : (g + 1) * conts, :] = cq_ref[:, column : column + HD].astype(
                jnp.float32
            )
    q[:, many:, :] = rows16[...].astype(jnp.bfloat16)

    for copy in suffix_copies:
        copy.wait()
    for h in range(KVH):
        keys = sk[:, :, h * HD : (h + 1) * HD].reshape(conts * suffix_rows, HD)
        values = sv[:, :, h * HD : (h + 1) * HD].reshape(conts * suffix_rows, HD)
        s = lax.dot_general(
            q[h, many:, :], keys, (((1,), (1,)), ((), ())), preferred_element_type=jnp.float32
        )
        who = lax.broadcasted_iota(jnp.int32, s.shape, 0) % conts
        column = lax.broadcasted_iota(jnp.int32, s.shape, 1)
        reach = jnp.zeros_like(who)
        for c in range(conts):
            reach = jnp.where(who == c, length_ref[c], reach)
        seen = (column // suffix_rows == who) & (column % suffix_rows < reach)
        s = jnp.where(seen, s * SCALE2, -1e30)
        top = jnp.max(s, axis=1, keepdims=True)
        w = jnp.exp2(s - top)
        row_max[h, many:, :] = jnp.broadcast_to(top, (GROUP * conts, HD))
        folded = w[:, :HD]
        for b in range(1, s.shape[1] // HD):
            folded = folded + w[:, b * HD : (b + 1) * HD]
        row_sum[h, many:, :] = folded
        acc[h, many:, :] = jnp.dot(
            w.astype(jnp.bfloat16), values, preferred_element_type=jnp.float32
        )

    span = CORES * 2 * half
    window_first = start_ref[0]
    prefix_last = prefix_ref[0]

    def places(chip_index):
        column = lax.broadcasted_iota(jnp.int32, (1, span), 1)
        within = column % (2 * half)
        position = (chip_index * CORES + column // (2 * half)) * half + within % half
        cached = jnp.where(
            (position >= window_first) & (position < prefix_last), -1, HIDDEN
        )
        return jnp.where(within < half, cached, position)

    def attend(h, chips, marks):
        cols = slice(h * HD, (h + 1) * HD)
        keys = [kv[pl.ds(c * CORES, CORES), 0, :, cols].reshape(span, HD) for c in chips]
        values = [kv[pl.ds(c * CORES, CORES), 1, :, cols].reshape(span, HD) for c in chips]
        keys = jnp.concatenate(keys, axis=0)
        values = jnp.concatenate(values, axis=0)
        mark = jnp.concatenate(marks, axis=1)
        count = span * len(chips)
        cut = (total // 2 + 15) // 16 * 16
        for lo, hi in ((0, cut), (cut, total)):
            s = lax.dot_general(
                q[h, lo:hi, :], keys, (((1,), (1,)), ((), ())), preferred_element_type=jnp.float32
            )
            bound = limit[lo:hi, :]
            blocks = []
            for b in range(count // HD):
                part = slice(b * HD, (b + 1) * HD)
                blocks.append(jnp.where(mark[:, part] <= bound, s[:, part] * SCALE2, -1e30))
            peak = functools.reduce(jnp.maximum, blocks)
            old = row_max[h, lo:hi, :]
            new = jnp.maximum(old, jnp.max(peak, axis=1, keepdims=True))
            alpha = jnp.exp2(old - new)
            w = [jnp.exp2(b - new) for b in blocks]
            row_max[h, lo:hi, :] = new
            row_sum[h, lo:hi, :] = row_sum[h, lo:hi, :] * alpha + functools.reduce(jnp.add, w)
            wb = jnp.concatenate([b.astype(jnp.bfloat16) for b in w], axis=1)
            acc[h, lo:hi, :] = acc[h, lo:hi, :] * alpha + jnp.dot(
                wb, values, preferred_element_type=jnp.float32
            )

    def onward(source, zs, p):
        @pl.when((zs < z) & (z < n_z - 1))
        def _():
            send(source, p, above, 0)

        @pl.when((zs > z) & (z > 0))
        def _():
            send(source, p, below, 0)

    def receive_z(zs, p):
        source = device(zs, y, core)
        arrived(source, p)
        onward(source, zs, p)
        if n_y == 2 and p == EXTRA:

            @pl.when(not_by_line(zs))
            def _():
                send(source, p, across, 4)

        elif n_y == 2:
            send(source, p, across, 1)
        send(source, p, partner, 2)

    def receive_extra(zs):
        @pl.when(by_line(zs))
        def _():
            source = device(zs, 1 - y, core)
            arrived(source, EXTRA)
            onward(source, zs, EXTRA)
            send(source, EXTRA, partner, 2)

    def receive_line(d, i):
        for zs, inside in ((z - d, z - d >= 0), (z + d, z + d < n_z)):

            @pl.when(inside)
            def _():
                receive_z(zs, ORDER[i])
                if n_y == 2 and i == PIECES - 1:
                    receive_extra(zs)

    def receive_y(zs, i):
        source = device(zs, 1 - y, core)
        p = ORDER[i]

        def take():
            arrived(source, p)
            send(source, p, partner, 2)

        if p == EXTRA:
            pl.when(not_by_line(zs))(take)
        else:
            take()

    def receive_pair(i):
        receive_y(z, i)
        if ORDER[i] == EXTRA:
            source = device(z, 1 - y, core)

            @pl.when(z < n_z - 2)
            def _():
                send(source, EXTRA, above, 0)

            @pl.when(z > 1)
            def _():
                send(source, EXTRA, below, 3)

    pltpu.make_async_copy(q.at[:, pl.ds(0, many)], q.at[:, pl.ds(0, many)], query_sem).wait()
    pair_arrived(partner)
    mark = places(chip)
    for h in range(KVH):
        attend(h, [chip], [mark])
        receive_line(1, h)
        if n_y == 2:
            receive_pair(h)

    def step(t, carry):
        zs, zb = z_at(t), z_at(t - 1)
        pair_arrived(device(zs, y, 1 - core))
        chips = [zs * n_y + y]
        if n_y == 2:
            pair_arrived(device(zb, 1 - y, 1 - core))
            chips.append(zb * n_y + 1 - y)
        marks = [places(c) for c in chips]
        for h in range(KVH):
            attend(h, chips, marks)

            @pl.when(t < n_z - 1)
            def _():
                receive_line(t + 1, h)

            if n_y == 2:
                receive_y(zs, h)
        return carry

    lax.fori_loop(1, n_z, step, 0)
    chips = []
    if n_y == 2:
        zb = z_at(jnp.int32(n_z - 1))
        pair_arrived(device(zb, 1 - y, 1 - core))
        chips = [zb * n_y + 1 - y]
    marks = [places(c) for c in chips]
    for h in range(KVH):
        if n_y == 2:
            attend(h, chips, marks)
        mixed = acc[h] / jnp.sum(row_sum[h], axis=1, keepdims=True)
        for g in range(GROUP):
            column = (h * GROUP + g) * HD
            out_ref[:, column : column + HD] = mixed[
                g * prompt_rows : (g + 1) * prompt_rows, :
            ].astype(jnp.bfloat16)
        rows16[h] = mixed[many:, :]
        for g in range(GROUP):
            column = (h * GROUP + g) * HD
            cont_ref[:, column : column + HD] = rows16[
                h, g * conts : (g + 1) * conts, :
            ].astype(jnp.bfloat16)

    @pl.when(z < n_z - 1)
    def _():
        sent(me, 0)

    @pl.when(z > 0)
    def _():
        sent(me, 3)

    sent(me, 2)
    if n_y == 2:
        pair = device(z, 1 - y, core)
        sent(me, 1, PIECES - 1)
        sent(me, 4, 1)

        @pl.when(z < n_z - 2)
        def _():
            sent(pair, 0, 1)

        @pl.when(z > 1)
        def _():
            sent(pair, 3, 1)

    def drain(zs, carry):
        source = device(zs, y, core)
        middle = ((zs < z) & (z < n_z - 1)) | ((zs > z) & (z > 0))

        @pl.when(middle)
        def _():
            sent(source, 0)

        @pl.when(zs != z)
        def _():
            if n_y == 2:
                sent(source, 1, PIECES - 1)
            sent(source, 2)

        if n_y == 2:
            other = device(zs, 1 - y, core)

            @pl.when((zs != z) & not_by_line(zs))
            def _():
                sent(source, 4, 1)

            @pl.when(middle & by_line(zs))
            def _():
                sent(other, 0, 1)

            sent(other, 2)
        return carry

    lax.fori_loop(0, n_z, drain, 0)


HEADS = (0, 1, 2, 3)
MOVED = None
EXTRA_HEAD = 1


def pack_rows(values):
    lane = lax.broadcasted_iota(jnp.int32, (8, HD), 1)
    tile = jnp.zeros((8, HD), jnp.float32)
    for i in range(values.shape[0] // 8):
        tile = jnp.where(lane == i, values[8 * i : 8 * i + 8, :], tile)
    return tile


def unpack_rows(tile, first, count):
    lane = lax.broadcasted_iota(jnp.int32, (8, HD), 1)
    blocks = [
        jnp.max(jnp.where(lane == i, tile, -3e38), axis=1, keepdims=True)
        for i in range(first // 8, (first + count) // 8)
    ]
    return jnp.concatenate(blocks, axis=0)


def plane_kernel(
    n_z,
    ck_ref,
    cv_ref,
    nq_ref,
    nk_ref,
    nv_ref,
    cq_hbm,
    sk_ref,
    sv_ref,
    start_hbm,
    prefix_hbm,
    length_hbm,
    out_ref,
    cont_ref,
    kv,
    q,
    sk,
    sv,
    rows16,
    limit,
    row_max,
    row_sum,
    acc,
    cq,
    far_cq,
    part_out,
    part_in,
    lse_out,
    lse_in,
    start_ref,
    prefix_ref,
    length_ref,
    local_sem,
    query_sem,
    suffix_sem,
    small_sem,
    recv_sem,
    send_sem,
    far_recv,
    far_send,
    part_recv,
    part_send,
):
    n_y = 2
    half = ck_ref.shape[0]
    prompt_rows = nq_ref.shape[0]
    conts = cq_hbm.shape[0]
    suffix_rows = sk_ref.shape[1]
    many = GROUP * prompt_rows
    few = GROUP * conts
    total = many + few
    me = lax.axis_index("ctx")
    core = me % CORES
    chip = me // CORES
    y = chip % n_y
    z = chip // n_y
    last = n_z - 1
    lines = n_z - 2
    plane = n_y * CORES
    span = plane * half

    def device(zz, yy, cc):
        return (zz * n_y + yy) * CORES + cc

    partner = device(z, y, 1 - core)
    across = device(z, 1 - y, core)
    above = device(z + 1, y, core)
    below = device(z - 1, y, core)

    for h in HEADS:
        cols = pl.ds(h * HD, HD)
        for kind, pair in enumerate(((ck_ref, cv_ref), (nk_ref, nv_ref))):
            for i, ref in enumerate(pair):
                pltpu.make_async_copy(ref.at[:, cols], kv.at[me, h, kind, i], local_sem.at[h]).start()
    small = [
        pltpu.make_async_copy(src, dst, small_sem.at[i])
        for i, (src, dst) in enumerate(
            (
                (cq_hbm, cq),
                (start_hbm, start_ref),
                (prefix_hbm, prefix_ref),
                (length_hbm, length_ref),
            )
        )
    ]
    for copy in small:
        copy.start()
    for h in HEADS:
        for g in range(GROUP):
            pltpu.make_async_copy(
                nq_ref.at[:, pl.ds((h * GROUP + g) * HD, HD)],
                q.at[h, pl.ds(g * prompt_rows, prompt_rows)],
                query_sem,
            ).start()
    suffix_copies = [
        pltpu.make_async_copy(sk_ref, sk, suffix_sem.at[0]),
        pltpu.make_async_copy(sv_ref, sv, suffix_sem.at[1]),
    ]
    for copy in suffix_copies:
        copy.start()

    barrier = pltpu.get_barrier_semaphore()

    def greet(target):
        pl.semaphore_signal(barrier, inc=1, device_id={"ctx": target}, device_id_type=MESH)

    greet(partner)
    greet(across)

    @pl.when(z > 0)
    def _():
        greet(below)

    @pl.when(z < last)
    def _():
        greet(above)

    line_neighbours = (z + n_z - 1) // n_z + (2 * n_z - 2 - z) // n_z
    pl.semaphore_wait(barrier, n_y + line_neighbours)

    def full(source, h):
        return kv.at[source, h]

    def cached(source, h):
        return kv.at[source, h, 0]

    def send(ref, source, h, target, kind):
        pltpu.make_async_remote_copy(
            src_ref=ref,
            dst_ref=ref,
            send_sem=send_sem.at[source, kind],
            recv_sem=recv_sem.at[source, h],
            device_id={"ctx": target},
            device_id_type=MESH,
        ).start()

    def arrived(ref, source, h):
        pltpu.make_async_copy(ref, ref, recv_sem.at[source, h]).wait()

    def far_copy(zs, target):
        return pltpu.make_async_remote_copy(
            src_ref=far_cq.at[zs],
            dst_ref=far_cq.at[zs],
            send_sem=far_send.at[zs],
            recv_sem=far_recv.at[zs],
            device_id={"ctx": target},
            device_id_type=MESH,
        )

    small[0].wait()

    @pl.when(z < last)
    def _():
        pltpu.make_async_remote_copy(
            src_ref=cq,
            dst_ref=far_cq.at[z],
            send_sem=far_send.at[z],
            recv_sem=far_recv.at[z],
            device_id={"ctx": above},
            device_id_type=MESH,
        ).start()

    for h in HEADS:
        pltpu.make_async_copy(full(me, h), full(me, h), local_sem.at[h]).wait()

        @pl.when(z < last)
        def _():
            send(full(me, h), me, h, above, 0)

        send(full(me, h), me, h, across, 1)

        @pl.when(z > 0)
        def _():
            send(cached(me, h), me, h, below, 3)

        send(full(me, h), me, h, partner, 2)

    near = jnp.minimum(z, last - z)

    def z_at(t):
        step = (t + 1) // 2
        both = z + step * (1 - 2 * (t % 2))
        far = jnp.where(z + z < last, t, last - t)
        return jnp.where(t <= 2 * near, both, far)

    row = lax.broadcasted_iota(jnp.int32, (total, HD), 0)
    limit[...] = jnp.where(row < many, (me % plane) * prompt_rows + row % prompt_rows, HIDDEN)
    row_max[...] = jnp.full_like(row_max, -1e30)
    row_sum[...] = jnp.zeros_like(row_sum)
    acc[...] = jnp.zeros_like(acc)

    def spread(rows):
        for h in range(KVH):
            for g in range(GROUP):
                column = (h * GROUP + g) * HD
                rows16[h, g * conts : (g + 1) * conts, :] = rows[:, column : column + HD].astype(
                    jnp.float32
                )

    spread(cq)
    q[:, many:, :] = rows16[...].astype(jnp.bfloat16)
    for copy in small[1:]:
        copy.wait()
    for copy in suffix_copies:
        copy.wait()
    for h in range(KVH):
        keys = sk[:, :, h * HD : (h + 1) * HD].reshape(conts * suffix_rows, HD)
        values = sv[:, :, h * HD : (h + 1) * HD].reshape(conts * suffix_rows, HD)
        s = lax.dot_general(
            q[h, many:, :], keys, (((1,), (1,)), ((), ())), preferred_element_type=jnp.float32
        )
        who = lax.broadcasted_iota(jnp.int32, s.shape, 0) % conts
        column = lax.broadcasted_iota(jnp.int32, s.shape, 1)
        reach = jnp.zeros_like(who)
        for c in range(conts):
            reach = jnp.where(who == c, length_ref[c], reach)
        seen = (column // suffix_rows == who) & (column % suffix_rows < reach)
        s = jnp.where(seen, s * SCALE2, -1e30)
        top = jnp.max(s, axis=1, keepdims=True)
        w = jnp.exp2(s - top)
        row_max[h, many:, :] = jnp.broadcast_to(top, (few, HD))
        folded = w[:, :HD]
        for b in range(1, s.shape[1] // HD):
            folded = folded + w[:, b * HD : (b + 1) * HD]
        row_sum[h, many:, :] = folded
        acc[h, many:, :] = jnp.dot(
            w.astype(jnp.bfloat16), values, preferred_element_type=jnp.float32
        )

    window_first = start_ref[0]
    prefix_last = prefix_ref[0]

    def cache_bias(zs):
        position = zs * span + lax.broadcasted_iota(jnp.int32, (1, span), 1)
        return jnp.where((position >= window_first) & (position < prefix_last), 0.0, -1e30)

    def plane_rows(zs, h, kind, i):
        return kv[pl.ds(zs * plane, plane), h, kind, i].reshape(span, HD)

    def attend(h, zs, mode, bias):
        keys = plane_rows(zs, h, 0, 0)
        values = plane_rows(zs, h, 0, 1)
        if mode != "cache":
            keys = jnp.concatenate([keys, plane_rows(zs, h, 1, 0)], axis=0)
            values = jnp.concatenate([values, plane_rows(zs, h, 1, 1)], axis=0)
        cut = (total // 2 + 15) // 16 * 16
        for lo, hi in ((0, cut), (cut, total)):
            s = lax.dot_general(
                q[h, lo:hi, :], keys, (((1,), (1,)), ((), ())), preferred_element_type=jnp.float32
            )
            blocks = []
            for b in range(keys.shape[0] // HD):
                part = s[:, b * HD : (b + 1) * HD] * SCALE2
                if b < span // HD:
                    part = part + bias[:, b * HD : (b + 1) * HD]
                elif mode == "own":
                    at = (b - span // HD) * HD + lax.broadcasted_iota(jnp.int32, (1, HD), 1)
                    part = jnp.where(at <= limit[lo:hi, :], part, -1e30)
                blocks.append(part)
            peak = functools.reduce(jnp.maximum, blocks)
            old = row_max[h, lo:hi, :]
            new = jnp.maximum(old, jnp.max(peak, axis=1, keepdims=True))
            alpha = jnp.exp2(old - new)
            w = [jnp.exp2(b - new) for b in blocks]
            row_max[h, lo:hi, :] = new
            row_sum[h, lo:hi, :] = row_sum[h, lo:hi, :] * alpha + functools.reduce(jnp.add, w)
            wb = jnp.concatenate([b.astype(jnp.bfloat16) for b in w], axis=1)
            acc[h, lo:hi, :] = acc[h, lo:hi, :] * alpha + jnp.dot(
                wb, values, preferred_element_type=jnp.float32
            )

    def foreign(zs):
        spread(far_cq.at[zs])
        sums = []
        for h in range(KVH):
            s = lax.dot_general(
                rows16[h].astype(jnp.bfloat16),
                plane_rows(z, h, 1, 0),
                (((1,), (1,)), ((), ())),
                preferred_element_type=jnp.float32,
            )
            s = s * SCALE2
            top = jnp.max(s, axis=1, keepdims=True)
            w = jnp.exp2(s - top)
            under = jnp.sum(w, axis=1, keepdims=True)
            mixed = jnp.dot(
                w.astype(jnp.bfloat16), plane_rows(z, h, 1, 1), preferred_element_type=jnp.float32
            )
            part_out[zs, h * few : (h + 1) * few, :] = mixed / under
            sums.append(jnp.broadcast_to(top + jnp.log2(under), (few, HD)))
        lse_out[zs] = pack_rows(jnp.concatenate(sums, axis=0))

    def part_copies(zs):
        return [
            pltpu.make_async_remote_copy(
                src_ref=src.at[zs],
                dst_ref=dst.at[z],
                send_sem=part_send.at[zs, i],
                recv_sem=part_recv.at[z, i],
                device_id={"ctx": device(zs, y, core)},
                device_id_type=MESH,
            )
            for i, (src, dst) in enumerate(((part_out, part_in), (lse_out, lse_in)))
        ]

    def merge(zs):
        for i, ref in enumerate((part_in, lse_in)):
            pltpu.make_async_copy(ref.at[zs], ref.at[zs], part_recv.at[zs, i]).wait()
        tile = lse_in[zs]
        lane = lax.broadcasted_iota(jnp.int32, (few, HD), 1)
        for h in range(KVH):
            level = unpack_rows(tile, h * few, few)
            old = row_max[h, many:, :]
            new = jnp.maximum(old, level)
            alpha = jnp.exp2(old - new)
            beta = jnp.exp2(level - new)
            row_max[h, many:, :] = new
            row_sum[h, many:, :] = row_sum[h, many:, :] * alpha + jnp.where(lane == 0, beta, 0.0)
            acc[h, many:, :] = (
                acc[h, many:, :] * alpha + part_in[zs, h * few : (h + 1) * few, :] * beta
            )

    def receive_line(d, i):
        h = HEADS[i]
        low, high = z - d, z + d

        @pl.when(low >= 0)
        def _():
            source = device(low, y, core)
            ref = full(source, h)
            if i == 0:
                pltpu.make_async_copy(far_cq.at[low], far_cq.at[low], far_recv.at[low]).wait()

                @pl.when(z < last)
                def _():
                    far_copy(low, above).start()

            arrived(ref, source, h)

            @pl.when(z < last)
            def _():
                send(ref, source, h, above, 0)

            if h == EXTRA_HEAD:

                @pl.when(low >= lines)
                def _():
                    send(ref, source, h, across, 1)

            else:
                send(ref, source, h, across, 1)
            send(ref, source, h, partner, 2)
            if i == KVH - 1:

                @pl.when(low < lines)
                def _():
                    other = device(low, 1 - y, core)
                    extra = full(other, EXTRA_HEAD)
                    arrived(extra, other, EXTRA_HEAD)

                    @pl.when(z < last)
                    def _():
                        send(extra, other, EXTRA_HEAD, above, 0)

                    send(extra, other, EXTRA_HEAD, partner, 2)

        @pl.when(high < n_z)
        def _():
            source = device(high, y, core)
            ref = cached(source, h)
            arrived(ref, source, h)

            @pl.when(z > 0)
            def _():
                send(ref, source, h, below, 0)

            send(ref, source, h, across, 1)
            send(ref, source, h, partner, 2)

    def receive_y(zs, i):
        h = HEADS[i]
        source = device(zs, 1 - y, core)

        def take(ref):
            arrived(ref, source, h)
            send(ref, source, h, partner, 2)

        if h == EXTRA_HEAD:
            pl.when((zs <= z) & ((zs == z) | (zs >= lines)))(lambda: take(full(source, h)))
        else:
            pl.when(zs <= z)(lambda: take(full(source, h)))
        pl.when(zs > z)(lambda: take(cached(source, h)))

    def receive_own(i):
        h = HEADS[i]
        arrived(full(across, h), across, h)
        send(full(across, h), across, h, partner, 2)
        if h == EXTRA_HEAD:

            @pl.when((z < last) & (z < lines))
            def _():
                send(full(across, h), across, h, above, 0)

    def pair_arrived(zs, i):
        h = HEADS[i]
        for yy in (y, 1 - y):
            source = device(zs, yy, 1 - core)
            pl.when(zs <= z)(lambda source=source: arrived(full(source, h), source, h))
            pl.when(zs > z)(lambda source=source: arrived(cached(source, h), source, h))

    pltpu.make_async_copy(
        q.at[pl.ds(0, KVH), pl.ds(0, many)], q.at[pl.ds(0, KVH), pl.ds(0, many)], query_sem
    ).wait()
    receive_own(0)
    receive_own(1)
    bias = cache_bias(z)
    for i, h in enumerate(HEADS):
        for yy in (y, 1 - y):
            source = device(z, yy, 1 - core)
            arrived(full(source, h), source, h)
        attend(h, z, "own", bias)
        receive_line(1, i)
        if i + 2 < KVH:
            receive_own(i + 2)

    @pl.when(z > 0)
    def _():
        foreign(z - 1)

    def give(zs):
        for copy in part_copies(zs):
            copy.start()

    def step(t, carry):
        zs = z_at(t)
        bias = cache_bias(zs)
        receive_y(zs, 0)
        for i, h in enumerate(HEADS):
            if i + 1 < KVH:
                receive_y(zs, i + 1)
            pair_arrived(zs, i)
            pl.when(zs < z)(lambda: attend(h, zs, "all", bias))
            pl.when(zs > z)(lambda: attend(h, zs, "cache", bias))

            if i == 0:
                pl.when((t == 1) & (z > 0))(lambda: give(z - 1))

            @pl.when(t < last)
            def _():
                receive_line(t + 1, i)
                if i < 2:
                    pl.when(z - t - 1 >= 0)(lambda: (foreign, give)[i](z - t - 1))

        return carry

    lax.fori_loop(1, n_z, step, 0)

    def collect(zs, carry):
        merge(zs)
        return carry

    lax.fori_loop(z + 1, n_z, collect, 0)
    for h in range(KVH):
        mixed = acc[h] / jnp.sum(row_sum[h], axis=1, keepdims=True)
        for g in range(GROUP):
            column = (h * GROUP + g) * HD
            out_ref[:, column : column + HD] = mixed[
                g * prompt_rows : (g + 1) * prompt_rows, :
            ].astype(jnp.bfloat16)
        rows16[h] = mixed[many:, :]
        for g in range(GROUP):
            column = (h * GROUP + g) * HD
            cont_ref[:, column : column + HD] = rows16[
                h, g * conts : (g + 1) * conts, :
            ].astype(jnp.bfloat16)

    def sent(source, kind, count, cache_only=False):
        ref = kv.at[source, pl.ds(0, count)]
        if cache_only:
            ref = kv.at[source, pl.ds(0, count), 0]
        pltpu.make_async_copy(ref, ref, send_sem.at[source, kind]).wait()

    @pl.when(z < last)
    def _():
        sent(me, 0, KVH)
        pltpu.make_async_copy(cq, cq, far_send.at[z]).wait()

    @pl.when(z > 0)
    def _():
        sent(me, 3, KVH, True)

    sent(me, 1, KVH)
    sent(me, 2, KVH)

    def drain(zs, carry):
        source = device(zs, y, core)
        other = device(zs, 1 - y, core)

        @pl.when(zs < z)
        def _():
            @pl.when(z < last)
            def _():
                sent(source, 0, KVH)
                pltpu.make_async_copy(far_cq.at[zs], far_cq.at[zs], far_send.at[zs]).wait()

            pl.when(zs < lines)(lambda: sent(source, 1, KVH - 1))
            pl.when(zs >= lines)(lambda: sent(source, 1, KVH))
            sent(source, 2, KVH)
            for copy in part_copies(zs):
                copy.wait_send()

        @pl.when(zs > z)
        def _():
            pl.when(z > 0)(lambda: sent(source, 0, KVH, True))
            sent(source, 1, KVH, True)
            sent(source, 2, KVH, True)
            sent(other, 2, KVH, True)

        @pl.when(zs <= z)
        def _():
            sent(other, 2, KVH)
            pl.when((z < last) & (zs < lines))(lambda: sent(other, 0, 1))

        return carry

    lax.fori_loop(0, n_z, drain, 0)


def line_shape(mesh):
    chips = mesh.shape["ctx"] // CORES
    place = mesh.axis_names.index("ctx")
    index = [0] * mesh.devices.ndim
    index[place] = slice(None)
    coords = [getattr(d, "coords", None) for d in mesh.devices[tuple(index)]]
    n_y = 1
    if all(c is not None for c in coords) and len({c[1] for c in coords}) == 2:
        n_y = 2
    return chips // n_y, n_y


def solution(mesh):
    n_z, n_y = line_shape(mesh)
    n_ctx = mesh.shape["ctx"]

    def plane_body(ck, cv, nq, nk, nv, cq, sk, sv, ws, pfx, length):
        half = ck.shape[0]
        few = GROUP * cq.shape[0]
        total = GROUP * nq.shape[0] + few
        anywhere = pl.BlockSpec(memory_space=pl.ANY)
        vmem = pl.BlockSpec(memory_space=pltpu.VMEM)
        state = pltpu.VMEM((KVH, total, HD), jnp.float32)
        part = pltpu.VMEM((n_z, KVH * few, HD), jnp.float32)
        levels = pltpu.VMEM((n_z, 8, HD), jnp.float32)
        return pl.pallas_call(
            functools.partial(plane_kernel, n_z),
            out_shape=(
                pltpu.VMEM(nq.shape, jnp.bfloat16),
                pltpu.VMEM(cq.shape, jnp.bfloat16),
            ),
            in_specs=[anywhere] * 11,
            out_specs=(vmem, vmem),
            scratch_shapes=[
                pltpu.VMEM((n_ctx, KVH, 2, 2, half, HD), jnp.bfloat16),
                pltpu.VMEM((KVH, total, HD), jnp.bfloat16),
                pltpu.VMEM(sk.shape, jnp.bfloat16),
                pltpu.VMEM(sv.shape, jnp.bfloat16),
                pltpu.VMEM((KVH, few, HD), jnp.float32),
                pltpu.VMEM((total, HD), jnp.int32),
                state,
                state,
                state,
                pltpu.VMEM(cq.shape, jnp.bfloat16),
                pltpu.VMEM((n_z,) + cq.shape, jnp.bfloat16),
                part,
                part,
                levels,
                levels,
                pltpu.SMEM(ws.shape, jnp.int32),
                pltpu.SMEM(pfx.shape, jnp.int32),
                pltpu.SMEM(length.shape, jnp.int32),
                pltpu.SemaphoreType.DMA((KVH,)),
                pltpu.SemaphoreType.DMA,
                pltpu.SemaphoreType.DMA((2,)),
                pltpu.SemaphoreType.DMA((4,)),
                pltpu.SemaphoreType.DMA((n_ctx, KVH)),
                pltpu.SemaphoreType.DMA((n_ctx, 4)),
                pltpu.SemaphoreType.DMA((n_z,)),
                pltpu.SemaphoreType.DMA((n_z,)),
                pltpu.SemaphoreType.DMA((n_z, 2)),
                pltpu.SemaphoreType.DMA((n_z, 2)),
            ],
            compiler_params=pltpu.CompilerParams(
                collective_id=0, has_side_effects=True, vmem_limit_bytes=60 * 1024 * 1024
            ),
        )(ck, cv, nq, nk, nv, cq, sk, sv, ws, pfx, length)

    def body(ck, cv, nq, nk, nv, cq, sk, sv, ws, pfx, length):
        half, width = ck.shape
        rows = nq.shape[0]
        conts = cq.shape[0]
        total = GROUP * (rows + conts)
        anywhere = pl.BlockSpec(memory_space=pl.ANY)
        vmem = pl.BlockSpec(memory_space=pltpu.VMEM)
        return pl.pallas_call(
            functools.partial(kernel, n_z, n_y),
            out_shape=(
                pltpu.VMEM(nq.shape, jnp.bfloat16),
                pltpu.VMEM(cq.shape, jnp.bfloat16),
            ),
            in_specs=[anywhere] * 11,
            out_specs=(vmem, vmem),
            scratch_shapes=[
                pltpu.VMEM((n_ctx, 2, 2 * half, width), jnp.bfloat16),
                pltpu.VMEM((KVH, total, HD), jnp.bfloat16),
                pltpu.VMEM(sk.shape, jnp.bfloat16),
                pltpu.VMEM(sv.shape, jnp.bfloat16),
                pltpu.VMEM((KVH, GROUP * conts, HD), jnp.float32),
                pltpu.VMEM((total, HD), jnp.int32),
                pltpu.VMEM((KVH, total, HD), jnp.float32),
                pltpu.VMEM((KVH, total, HD), jnp.float32),
                pltpu.VMEM((KVH, total, HD), jnp.float32),
                pltpu.VMEM(cq.shape, jnp.bfloat16),
                pltpu.SMEM(ws.shape, jnp.int32),
                pltpu.SMEM(pfx.shape, jnp.int32),
                pltpu.SMEM(length.shape, jnp.int32),
                pltpu.SemaphoreType.DMA((PIECES,)),
                pltpu.SemaphoreType.DMA,
                pltpu.SemaphoreType.DMA((2,)),
                pltpu.SemaphoreType.DMA((n_ctx, PIECES)),
                pltpu.SemaphoreType.DMA((n_ctx,)),
                pltpu.SemaphoreType.DMA((n_ctx, 5)),
                pltpu.SemaphoreType.DMA((4,)),
            ],
            compiler_params=pltpu.CompilerParams(
                collective_id=0, has_side_effects=True, vmem_limit_bytes=60 * 1024 * 1024
            ),
        )(ck, cv, nq, nk, nv, cq, sk, sv, ws, pfx, length)

    part = P(("grp", "ctx"), None)
    part3 = P(("grp", "ctx"), None, None)
    in_specs = (part,) * 6 + (part3, part3, P("grp"), P("grp"), P(("grp", "ctx")))
    return jax.shard_map(
        plane_body if n_y == 2 and n_z > 2 else body,
        mesh=mesh, in_specs=in_specs, out_specs=(part, part), check_vma=False
    )
```

```python
import functools
import math

import jax
import jax.numpy as jnp
from jax import lax
from jax.experimental import pallas as pl
from jax.experimental.pallas import tpu as pltpu
from jax.sharding import PartitionSpec as P

KVH = 4
HD = 128
GROUP = 8
CORES = 2
PIECES = 4
EXTRA = 3
ORDER = (EXTRA, 0, 1, 2)
MESH = pl.DeviceIdType.MESH
SCALE2 = HD ** (-0.5) * math.log2(math.e)
HIDDEN = 1 << 30


def kernel(
    n_z,
    n_y,
    ck_ref,
    cv_ref,
    nq_ref,
    nk_ref,
    nv_ref,
    cq_hbm,
    sk_ref,
    sv_ref,
    start_hbm,
    prefix_hbm,
    length_hbm,
    out_ref,
    cont_ref,
    kv,
    q,
    sk,
    sv,
    rows16,
    limit,
    row_max,
    row_sum,
    acc,
    cq_ref,
    start_ref,
    prefix_ref,
    length_ref,
    local_sem,
    query_sem,
    suffix_sem,
    recv_sem,
    pair_sem,
    send_sem,
    small_sem,
):
    half = ck_ref.shape[0]
    prompt_rows = nq_ref.shape[0]
    conts = cq_hbm.shape[0]
    suffix_rows = sk_ref.shape[1]
    many = GROUP * prompt_rows
    total = many + GROUP * conts
    me = lax.axis_index("ctx")
    core = me % CORES
    chip = me // CORES
    y = chip % n_y
    z = chip // n_y

    def device(zz, yy, cc):
        return (zz * n_y + yy) * CORES + cc

    own = []
    for p, ref in enumerate((ck_ref, nk_ref, cv_ref, nv_ref)):
        copy = pltpu.make_async_copy(
            ref, kv.at[me, p // 2, pl.ds((p % 2) * half, half)], local_sem.at[p]
        )
        copy.start()
        own.append(copy)
    for h in range(KVH):
        for g in range(GROUP):
            pltpu.make_async_copy(
                nq_ref.at[:, pl.ds((h * GROUP + g) * HD, HD)],
                q.at[h, pl.ds(g * prompt_rows, prompt_rows)],
                query_sem,
            ).start()
    suffix_copies = [
        pltpu.make_async_copy(sk_ref, sk, suffix_sem.at[0]),
        pltpu.make_async_copy(sv_ref, sv, suffix_sem.at[1]),
    ]
    small_copies = [
        pltpu.make_async_copy(src, dst, small_sem.at[i])
        for i, (src, dst) in enumerate(
            (
                (cq_hbm, cq_ref),
                (start_hbm, start_ref),
                (prefix_hbm, prefix_ref),
                (length_hbm, length_ref),
            )
        )
    ]
    for copy in suffix_copies + small_copies:
        copy.start()

    barrier = pltpu.get_barrier_semaphore()

    def greet(target):
        pl.semaphore_signal(barrier, inc=1, device_id={"ctx": target}, device_id_type=MESH)

    greet(device(z, y, 1 - core))
    if n_y == 2:
        greet(device(z, 1 - y, core))

    @pl.when(z > 0)
    def _():
        greet(device(z - 1, y, core))

    @pl.when(z < n_z - 1)
    def _():
        greet(device(z + 1, y, core))

    line_neighbours = (z + n_z - 1) // n_z + (2 * n_z - 2 - z) // n_z
    pl.semaphore_wait(barrier, n_y + line_neighbours)

    def piece(source, p):
        return kv.at[source, p // 2, pl.ds((p % 2) * half, half)]

    def send(source, p, target, kind):
        ref = piece(source, p)
        sem = pair_sem.at[source] if kind == 2 else recv_sem.at[source, p]
        pltpu.make_async_remote_copy(
            src_ref=ref,
            dst_ref=ref,
            send_sem=send_sem.at[source, kind],
            recv_sem=sem,
            device_id={"ctx": target},
            device_id_type=MESH,
        ).start()

    def arrived(source, p):
        ref = piece(source, p)
        pltpu.make_async_copy(ref, ref, recv_sem.at[source, p]).wait()

    def pair_arrived(source):
        pltpu.make_async_copy(kv.at[source], kv.at[source], pair_sem.at[source]).wait()

    def sent(source, kind, pieces=PIECES):
        ref = kv.at[source]
        if pieces == 1:
            ref = piece(source, EXTRA)
        elif pieces < PIECES:
            ref = kv.at[source, :, pl.ds(0, pieces * half // 2)]
        pltpu.make_async_copy(ref, ref, send_sem.at[source, kind]).wait()

    def by_line(zs):
        return ((zs < z) & (zs < n_z - 2)) | ((zs > z) & (zs > 1))

    def not_by_line(zs):
        return ((zs < z) & (zs >= n_z - 2)) | ((zs > z) & (zs <= 1)) | (zs == z)

    partner = device(z, y, 1 - core)
    across = device(z, 1 - y, core)
    above = device(z + 1, y, core)
    below = device(z - 1, y, core)

    for p in ORDER:
        own[p].wait()

        @pl.when(z < n_z - 1)
        def _():
            send(me, p, above, 0)

        if n_y == 2:
            send(me, p, across, 4 if p == EXTRA else 1)

        @pl.when(z > 0)
        def _():
            send(me, p, below, 3)

        send(me, p, partner, 2)

    near = jnp.minimum(z, n_z - 1 - z)

    def z_at(t):
        if isinstance(t, int) and t == 0:
            return z
        step = (t + 1) // 2
        both = z + step * (1 - 2 * (t % 2))
        far = jnp.where(z + z < n_z - 1, t, n_z - 1 - t)
        return jnp.where(t <= 2 * near, both, far)

    row = lax.broadcasted_iota(jnp.int32, (total, HD), 0)
    limit[...] = jnp.where(row < many, me * prompt_rows + row % prompt_rows, HIDDEN - 1)
    row_max[...] = jnp.full_like(row_max, -1e30)
    row_sum[...] = jnp.zeros_like(row_sum)
    acc[...] = jnp.zeros_like(acc)
    for copy in small_copies:
        copy.wait()
    for h in range(KVH):
        for g in range(GROUP):
            column = (h * GROUP + g) * HD
            rows16[h, g * conts : (g + 1) * conts, :] = cq_ref[:, column : column + HD].astype(
                jnp.float32
            )
    q[:, many:, :] = rows16[...].astype(jnp.bfloat16)

    for copy in suffix_copies:
        copy.wait()
    for h in range(KVH):
        keys = sk[:, :, h * HD : (h + 1) * HD].reshape(conts * suffix_rows, HD)
        values = sv[:, :, h * HD : (h + 1) * HD].reshape(conts * suffix_rows, HD)
        s = lax.dot_general(
            q[h, many:, :], keys, (((1,), (1,)), ((), ())), preferred_element_type=jnp.float32
        )
        who = lax.broadcasted_iota(jnp.int32, s.shape, 0) % conts
        column = lax.broadcasted_iota(jnp.int32, s.shape, 1)
        reach = jnp.zeros_like(who)
        for c in range(conts):
            reach = jnp.where(who == c, length_ref[c], reach)
        seen = (column // suffix_rows == who) & (column % suffix_rows < reach)
        s = jnp.where(seen, s * SCALE2, -1e30)
        top = jnp.max(s, axis=1, keepdims=True)
        w = jnp.exp2(s - top)
        row_max[h, many:, :] = jnp.broadcast_to(top, (GROUP * conts, HD))
        folded = w[:, :HD]
        for b in range(1, s.shape[1] // HD):
            folded = folded + w[:, b * HD : (b + 1) * HD]
        row_sum[h, many:, :] = folded
        acc[h, many:, :] = jnp.dot(
            w.astype(jnp.bfloat16), values, preferred_element_type=jnp.float32
        )

    span = CORES * 2 * half
    window_first = start_ref[0]
    prefix_last = prefix_ref[0]

    def places(chip_index):
        column = lax.broadcasted_iota(jnp.int32, (1, span), 1)
        within = column % (2 * half)
        position = (chip_index * CORES + column // (2 * half)) * half + within % half
        cached = jnp.where(
            (position >= window_first) & (position < prefix_last), -1, HIDDEN
        )
        return jnp.where(within < half, cached, position)

    def attend(h, chips, marks):
        cols = slice(h * HD, (h + 1) * HD)
        keys = [kv[pl.ds(c * CORES, CORES), 0, :, cols].reshape(span, HD) for c in chips]
        values = [kv[pl.ds(c * CORES, CORES), 1, :, cols].reshape(span, HD) for c in chips]
        keys = jnp.concatenate(keys, axis=0)
        values = jnp.concatenate(values, axis=0)
        mark = jnp.concatenate(marks, axis=1)
        count = span * len(chips)
        cut = (total // 2 + 15) // 16 * 16
        for lo, hi in ((0, cut), (cut, total)):
            s = lax.dot_general(
                q[h, lo:hi, :], keys, (((1,), (1,)), ((), ())), preferred_element_type=jnp.float32
            )
            bound = limit[lo:hi, :]
            blocks = []
            for b in range(count // HD):
                part = slice(b * HD, (b + 1) * HD)
                blocks.append(jnp.where(mark[:, part] <= bound, s[:, part] * SCALE2, -1e30))
            peak = functools.reduce(jnp.maximum, blocks)
            old = row_max[h, lo:hi, :]
            new = jnp.maximum(old, jnp.max(peak, axis=1, keepdims=True))
            alpha = jnp.exp2(old - new)
            w = [jnp.exp2(b - new) for b in blocks]
            row_max[h, lo:hi, :] = new
            row_sum[h, lo:hi, :] = row_sum[h, lo:hi, :] * alpha + functools.reduce(jnp.add, w)
            wb = jnp.concatenate([b.astype(jnp.bfloat16) for b in w], axis=1)
            acc[h, lo:hi, :] = acc[h, lo:hi, :] * alpha + jnp.dot(
                wb, values, preferred_element_type=jnp.float32
            )

    def onward(source, zs, p):
        @pl.when((zs < z) & (z < n_z - 1))
        def _():
            send(source, p, above, 0)

        @pl.when((zs > z) & (z > 0))
        def _():
            send(source, p, below, 0)

    def receive_z(zs, p):
        source = device(zs, y, core)
        arrived(source, p)
        onward(source, zs, p)
        if n_y == 2 and p == EXTRA:

            @pl.when(not_by_line(zs))
            def _():
                send(source, p, across, 4)

        elif n_y == 2:
            send(source, p, across, 1)
        send(source, p, partner, 2)

    def receive_extra(zs):
        @pl.when(by_line(zs))
        def _():
            source = device(zs, 1 - y, core)
            arrived(source, EXTRA)
            onward(source, zs, EXTRA)
            send(source, EXTRA, partner, 2)

    def receive_far(d):
        low = z - d

        @pl.when(low >= 0)
        def _():
            pltpu.make_async_copy(far_cq.at[low], far_cq.at[low], far_recv.at[low]).wait()

            @pl.when(z < last)
            def _():
                far_copy(low, above).start()

    def receive_line(d, i):
        for zs, inside in ((z - d, z - d >= 0), (z + d, z + d < n_z)):

            @pl.when(inside)
            def _():
                receive_z(zs, ORDER[i])
                if n_y == 2 and i == PIECES - 1:
                    receive_extra(zs)

    def receive_y(zs, i):
        source = device(zs, 1 - y, core)
        p = ORDER[i]

        def take():
            arrived(source, p)
            send(source, p, partner, 2)

        if p == EXTRA:
            pl.when(not_by_line(zs))(take)
        else:
            take()

    def receive_pair(i):
        receive_y(z, i)
        if ORDER[i] == EXTRA:
            source = device(z, 1 - y, core)

            @pl.when(z < n_z - 2)
            def _():
                send(source, EXTRA, above, 0)

            @pl.when(z > 1)
            def _():
                send(source, EXTRA, below, 3)

    pltpu.make_async_copy(q.at[:, pl.ds(0, many)], q.at[:, pl.ds(0, many)], query_sem).wait()
    pair_arrived(partner)
    mark = places(chip)
    for h in range(KVH):
        attend(h, [chip], [mark])
        receive_line(1, h)
        if n_y == 2:
            receive_pair(h)

    def step(t, carry):
        zs, zb = z_at(t), z_at(t - 1)
        pair_arrived(device(zs, y, 1 - core))
        chips = [zs * n_y + y]
        if n_y == 2:
            pair_arrived(device(zb, 1 - y, 1 - core))
            chips.append(zb * n_y + 1 - y)
        marks = [places(c) for c in chips]
        for h in range(KVH):
            attend(h, chips, marks)

            @pl.when(t < n_z - 1)
            def _():
                receive_line(t + 1, h)

            if n_y == 2:
                receive_y(zs, h)
        return carry

    lax.fori_loop(1, n_z, step, 0)
    chips = []
    if n_y == 2:
        zb = z_at(jnp.int32(n_z - 1))
        pair_arrived(device(zb, 1 - y, 1 - core))
        chips = [zb * n_y + 1 - y]
    marks = [places(c) for c in chips]
    for h in range(KVH):
        if n_y == 2:
            attend(h, chips, marks)
        mixed = acc[h] / jnp.sum(row_sum[h], axis=1, keepdims=True)
        for g in range(GROUP):
            column = (h * GROUP + g) * HD
            out_ref[:, column : column + HD] = mixed[
                g * prompt_rows : (g + 1) * prompt_rows, :
            ].astype(jnp.bfloat16)
        rows16[h] = mixed[many:, :]
        for g in range(GROUP):
            column = (h * GROUP + g) * HD
            cont_ref[:, column : column + HD] = rows16[
                h, g * conts : (g + 1) * conts, :
            ].astype(jnp.bfloat16)

    @pl.when(z < n_z - 1)
    def _():
        sent(me, 0)

    @pl.when(z > 0)
    def _():
        sent(me, 3)

    sent(me, 2)
    if n_y == 2:
        pair = device(z, 1 - y, core)
        sent(me, 1, PIECES - 1)
        sent(me, 4, 1)

        @pl.when(z < n_z - 2)
        def _():
            sent(pair, 0, 1)

        @pl.when(z > 1)
        def _():
            sent(pair, 3, 1)

    def drain(zs, carry):
        source = device(zs, y, core)
        middle = ((zs < z) & (z < n_z - 1)) | ((zs > z) & (z > 0))

        @pl.when(middle)
        def _():
            sent(source, 0)

        @pl.when(zs != z)
        def _():
            if n_y == 2:
                sent(source, 1, PIECES - 1)
            sent(source, 2)

        if n_y == 2:
            other = device(zs, 1 - y, core)

            @pl.when((zs != z) & not_by_line(zs))
            def _():
                sent(source, 4, 1)

            @pl.when(middle & by_line(zs))
            def _():
                sent(other, 0, len(BY_LINE))

            sent(other, 2)
        return carry

    lax.fori_loop(0, n_z, drain, 0)


HEADS = (0, 1, 2, 3)
BY_LINE = (3,)
LEAD = 2
AHEAD = 2


def pack_rows(values):
    lane = lax.broadcasted_iota(jnp.int32, (8, HD), 1)
    tile = jnp.zeros((8, HD), jnp.float32)
    for i in range(values.shape[0] // 8):
        tile = jnp.where(lane == i, values[8 * i : 8 * i + 8, :], tile)
    return tile


def unpack_rows(tile, first, count):
    lane = lax.broadcasted_iota(jnp.int32, (8, HD), 1)
    blocks = [
        jnp.max(jnp.where(lane == i, tile, -3e38), axis=1, keepdims=True)
        for i in range(first // 8, (first + count) // 8)
    ]
    return jnp.concatenate(blocks, axis=0)


def plane_kernel(
    n_z,
    ck_ref,
    cv_ref,
    nq_ref,
    nk_ref,
    nv_ref,
    cq_hbm,
    sk_ref,
    sv_ref,
    start_hbm,
    prefix_hbm,
    length_hbm,
    out_ref,
    cont_ref,
    kv,
    q,
    sk,
    sv,
    rows16,
    limit,
    row_max,
    row_sum,
    acc,
    cq,
    far_cq,
    far_rows,
    part_out,
    part_in,
    lse_out,
    lse_in,
    start_ref,
    prefix_ref,
    length_ref,
    local_sem,
    query_sem,
    suffix_sem,
    small_sem,
    recv_sem,
    send_sem,
    far_recv,
    far_send,
    part_recv,
    part_send,
):
    n_y = 2
    half = ck_ref.shape[0]
    prompt_rows = nq_ref.shape[0]
    conts = cq_hbm.shape[0]
    suffix_rows = sk_ref.shape[1]
    many = GROUP * prompt_rows
    few = GROUP * conts
    total = many + few
    me = lax.axis_index("ctx")
    core = me % CORES
    chip = me // CORES
    y = chip % n_y
    z = chip // n_y
    last = n_z - 1
    lines = n_z - 2
    plane = n_y * CORES
    span = plane * half

    def device(zz, yy, cc):
        return (zz * n_y + yy) * CORES + cc

    partner = device(z, y, 1 - core)
    across = device(z, 1 - y, core)
    above = device(z + 1, y, core)
    below = device(z - 1, y, core)

    for h in HEADS:
        cols = pl.ds(h * HD, HD)
        for kind, pair in enumerate(((ck_ref, cv_ref), (nk_ref, nv_ref))):
            for i, ref in enumerate(pair):
                pltpu.make_async_copy(ref.at[:, cols], kv.at[me, h, kind, i], local_sem.at[h]).start()
    small = [
        pltpu.make_async_copy(src, dst, small_sem.at[i])
        for i, (src, dst) in enumerate(
            (
                (cq_hbm, cq),
                (start_hbm, start_ref),
                (prefix_hbm, prefix_ref),
                (length_hbm, length_ref),
            )
        )
    ]
    for copy in small:
        copy.start()
    for h in HEADS:
        for g in range(GROUP):
            pltpu.make_async_copy(
                nq_ref.at[:, pl.ds((h * GROUP + g) * HD, HD)],
                q.at[h, pl.ds(g * prompt_rows, prompt_rows)],
                query_sem,
            ).start()
    suffix_copies = [
        pltpu.make_async_copy(sk_ref, sk, suffix_sem.at[0]),
        pltpu.make_async_copy(sv_ref, sv, suffix_sem.at[1]),
    ]
    for copy in suffix_copies:
        copy.start()

    barrier = pltpu.get_barrier_semaphore()

    def greet(target):
        pl.semaphore_signal(barrier, inc=1, device_id={"ctx": target}, device_id_type=MESH)

    greet(partner)
    greet(across)

    @pl.when(z > 0)
    def _():
        greet(below)

    @pl.when(z < last)
    def _():
        greet(above)

    line_neighbours = (z + n_z - 1) // n_z + (2 * n_z - 2 - z) // n_z
    pl.semaphore_wait(barrier, n_y + line_neighbours)

    def full(source, h):
        return kv.at[source, h]

    def cached(source, h):
        return kv.at[source, h, 0]

    def send(ref, source, h, target, kind):
        pltpu.make_async_remote_copy(
            src_ref=ref,
            dst_ref=ref,
            send_sem=send_sem.at[source, kind],
            recv_sem=recv_sem.at[source, h],
            device_id={"ctx": target},
            device_id_type=MESH,
        ).start()

    def arrived(ref, source, h):
        pltpu.make_async_copy(ref, ref, recv_sem.at[source, h]).wait()

    def far_copy(zs, target):
        return pltpu.make_async_remote_copy(
            src_ref=far_cq.at[zs],
            dst_ref=far_cq.at[zs],
            send_sem=far_send.at[zs],
            recv_sem=far_recv.at[zs],
            device_id={"ctx": target},
            device_id_type=MESH,
        )

    small[0].wait()

    @pl.when(z < last)
    def _():
        pltpu.make_async_remote_copy(
            src_ref=cq,
            dst_ref=far_cq.at[z],
            send_sem=far_send.at[z],
            recv_sem=far_recv.at[z],
            device_id={"ctx": above},
            device_id_type=MESH,
        ).start()

    for h in HEADS:
        pltpu.make_async_copy(full(me, h), full(me, h), local_sem.at[h]).wait()

        @pl.when(z < last)
        def _():
            send(full(me, h), me, h, above, 0)

        send(full(me, h), me, h, across, 1)

        @pl.when(z > 0)
        def _():
            send(cached(me, h), me, h, below, 3)

        send(full(me, h), me, h, partner, 2)

    near = jnp.minimum(z, last - z)

    def z_at(t):
        step = (t + 1) // 2
        both = z + step * (1 - 2 * (t % 2))
        far = jnp.where(z + z < last, t, last - t)
        return jnp.where(t <= 2 * near, both, far)

    row = lax.broadcasted_iota(jnp.int32, (total, HD), 0)
    limit[...] = jnp.where(row < many, (me % plane) * prompt_rows + row % prompt_rows, HIDDEN)
    row_max[...] = jnp.full_like(row_max, -1e30)
    row_sum[...] = jnp.zeros_like(row_sum)
    acc[...] = jnp.zeros_like(acc)

    def spread(rows):
        for h in range(KVH):
            for g in range(GROUP):
                column = (h * GROUP + g) * HD
                rows16[h, g * conts : (g + 1) * conts, :] = rows[:, column : column + HD].astype(
                    jnp.float32
                )

    for zs in range(last):

        @pl.when(zs >= z)
        def _():
            far_cq[zs] = jnp.zeros(far_cq.shape[1:], jnp.bfloat16)

    spread(cq)
    q[:, many:, :] = rows16[...].astype(jnp.bfloat16)
    for copy in small[1:]:
        copy.wait()
    for copy in suffix_copies:
        copy.wait()
    for h in range(KVH):
        keys = sk[:, :, h * HD : (h + 1) * HD].reshape(conts * suffix_rows, HD)
        values = sv[:, :, h * HD : (h + 1) * HD].reshape(conts * suffix_rows, HD)
        s = lax.dot_general(
            q[h, many:, :], keys, (((1,), (1,)), ((), ())), preferred_element_type=jnp.float32
        )
        who = lax.broadcasted_iota(jnp.int32, s.shape, 0) % conts
        column = lax.broadcasted_iota(jnp.int32, s.shape, 1)
        reach = jnp.zeros_like(who)
        for c in range(conts):
            reach = jnp.where(who == c, length_ref[c], reach)
        seen = (column // suffix_rows == who) & (column % suffix_rows < reach)
        s = jnp.where(seen, s * SCALE2, -1e30)
        top = jnp.max(s, axis=1, keepdims=True)
        w = jnp.exp2(s - top)
        row_max[h, many:, :] = jnp.broadcast_to(top, (few, HD))
        row_sum[h, many:, :] = jnp.broadcast_to(jnp.sum(w, axis=1, keepdims=True), (few, HD))
        acc[h, many:, :] = jnp.dot(
            w.astype(jnp.bfloat16), values, preferred_element_type=jnp.float32
        )

    window_first = start_ref[0]
    prefix_last = prefix_ref[0]

    def cache_bias(zs):
        position = zs * span + lax.broadcasted_iota(jnp.int32, (1, span), 1)
        return jnp.where((position >= window_first) & (position < prefix_last), 0.0, -1e30)

    def plane_rows(zs, h, kind, i):
        return kv[pl.ds(zs * plane, plane), h, kind, i].reshape(span, HD)

    def summed(values):
        return jnp.concatenate([values, jnp.ones(values.shape, jnp.bfloat16)], axis=1)

    def attend(h, zs, mode, bias):
        keys = plane_rows(zs, h, 0, 0)
        values = plane_rows(zs, h, 0, 1)
        if mode != "cache":
            keys = jnp.concatenate([keys, plane_rows(zs, h, 1, 0)], axis=0)
            values = jnp.concatenate([values, plane_rows(zs, h, 1, 1)], axis=0)
        values = summed(values)
        cut = (total // 2 + 15) // 16 * 16
        for lo, hi in ((0, cut), (cut, total)):
            s = lax.dot_general(
                q[h, lo:hi, :], keys, (((1,), (1,)), ((), ())), preferred_element_type=jnp.float32
            )
            blocks = []
            for b in range(keys.shape[0] // HD):
                part = s[:, b * HD : (b + 1) * HD] * SCALE2
                if b < span // HD:
                    part = part + bias[:, b * HD : (b + 1) * HD]
                elif mode == "own":
                    at = (b - span // HD) * HD + lax.broadcasted_iota(jnp.int32, (1, HD), 1)
                    part = jnp.where(at <= limit[lo:hi, :], part, -1e30)
                blocks.append(part)
            peak = functools.reduce(jnp.maximum, blocks)
            old = row_max[h, lo:hi, :]
            new = jnp.maximum(old, jnp.max(peak, axis=1, keepdims=True))
            alpha = jnp.exp2(old - new)
            w = [jnp.exp2(b - new) for b in blocks]
            row_max[h, lo:hi, :] = new
            wb = jnp.concatenate([b.astype(jnp.bfloat16) for b in w], axis=1)
            mixed = jnp.dot(wb, values, preferred_element_type=jnp.float32)
            acc[h, lo:hi, :] = acc[h, lo:hi, :] * alpha + mixed[:, :HD]
            row_sum[h, lo:hi, :] = row_sum[h, lo:hi, :] * alpha + mixed[:, HD:]

    def foreign():
        for zs in range(last):
            rows = far_cq.at[zs]
            for h in range(KVH):
                for g in range(GROUP):
                    column = (h * GROUP + g) * HD
                    first = zs * few + g * conts
                    far_rows[h, first : first + conts, :] = rows[:, column : column + HD].astype(
                        jnp.float32
                    )
        sums = []
        for h in range(KVH):
            s = lax.dot_general(
                far_rows[h].astype(jnp.bfloat16),
                plane_rows(z, h, 1, 0),
                (((1,), (1,)), ((), ())),
                preferred_element_type=jnp.float32,
            )
            s = s * SCALE2
            top = jnp.max(s, axis=1, keepdims=True)
            w = jnp.exp2(s - top)
            both = jnp.dot(
                w.astype(jnp.bfloat16),
                summed(plane_rows(z, h, 1, 1)),
                preferred_element_type=jnp.float32,
            )
            under = both[:, HD:]
            mixed = both[:, :HD] / under
            for zs in range(last):
                part_out[zs, h * few : (h + 1) * few, :] = mixed[zs * few : (zs + 1) * few, :]
            sums.append(top + jnp.log2(under))
        for zs in range(last):
            lse_out[zs] = pack_rows(
                jnp.concatenate([level[zs * few : (zs + 1) * few, :] for level in sums], axis=0)
            )

    def part_copies(zs):
        return [
            pltpu.make_async_remote_copy(
                src_ref=src.at[zs],
                dst_ref=dst.at[z],
                send_sem=part_send.at[zs, i],
                recv_sem=part_recv.at[z, i],
                device_id={"ctx": device(zs, y, core)},
                device_id_type=MESH,
            )
            for i, (src, dst) in enumerate(((part_out, part_in), (lse_out, lse_in)))
        ]

    def merge(zs):
        for i, ref in enumerate((part_in, lse_in)):
            pltpu.make_async_copy(ref.at[zs], ref.at[zs], part_recv.at[zs, i]).wait()
        tile = lse_in[zs]
        for h in range(KVH):
            level = unpack_rows(tile, h * few, few)
            old = row_max[h, many:, :]
            new = jnp.maximum(old, level)
            alpha = jnp.exp2(old - new)
            beta = jnp.exp2(level - new)
            row_max[h, many:, :] = new
            row_sum[h, many:, :] = row_sum[h, many:, :] * alpha + beta
            acc[h, many:, :] = (
                acc[h, many:, :] * alpha + part_in[zs, h * few : (h + 1) * few, :] * beta
            )

    def receive_far(d):
        low = z - d

        @pl.when(low >= 0)
        def _():
            pltpu.make_async_copy(far_cq.at[low], far_cq.at[low], far_recv.at[low]).wait()

            @pl.when(z < last)
            def _():
                far_copy(low, above).start()

    def receive_line(d, i):
        h = HEADS[i]
        low, high = z - d, z + d

        @pl.when(low >= 0)
        def _():
            source = device(low, y, core)
            ref = full(source, h)
            arrived(ref, source, h)

            @pl.when(z < last)
            def _():
                send(ref, source, h, above, 0)

            if h in BY_LINE:

                @pl.when(low >= lines)
                def _():
                    send(ref, source, h, across, 1)

            else:
                send(ref, source, h, across, 1)
            send(ref, source, h, partner, 2)
        @pl.when(high < n_z)
        def _():
            source = device(high, y, core)
            ref = cached(source, h)
            arrived(ref, source, h)

            @pl.when(z > 0)
            def _():
                send(ref, source, h, below, 0)

            send(ref, source, h, across, 1)
            send(ref, source, h, partner, 2)

    def receive_y(zs, i):
        h = HEADS[i]
        source = device(zs, 1 - y, core)

        def take(ref):
            arrived(ref, source, h)
            send(ref, source, h, partner, 2)

        pl.when(zs <= z)(lambda: take(full(source, h)))
        if h in BY_LINE:
            pl.when((zs < lines) & (zs < z) & (z < last))(
                lambda: send(full(source, h), source, h, above, 0)
            )
        pl.when(zs > z)(lambda: take(cached(source, h)))

    def receive_own(i):
        h = HEADS[i]
        arrived(full(across, h), across, h)
        send(full(across, h), across, h, partner, 2)
        if h in BY_LINE:

            @pl.when((z < last) & (z < lines))
            def _():
                send(full(across, h), across, h, above, 0)

    def pair_arrived(zs, i):
        h = HEADS[i]
        for yy in (y, 1 - y):
            source = device(zs, yy, 1 - core)
            pl.when(zs <= z)(lambda source=source: arrived(full(source, h), source, h))
            pl.when(zs > z)(lambda source=source: arrived(cached(source, h), source, h))

    pltpu.make_async_copy(
        q.at[pl.ds(0, KVH), pl.ds(0, many)], q.at[pl.ds(0, KVH), pl.ds(0, many)], query_sem
    ).wait()
    def receive(t, i):
        q, r = divmod(i + AHEAD - 1, KVH)
        receive_line(t + 1 + q, r)
        q, r = divmod(i + LEAD, KVH)
        if isinstance(t, int):
            receive_own(r) if t + q == 0 else receive_y(z_at(t + q), r)
        else:
            pl.when(t + q < n_z)(lambda: receive_y(z_at(t + q), r))

    def give(zs):
        for copy in part_copies(zs):
            copy.start()

    for j in range(AHEAD - 1):
        receive_line(1 + j // KVH, j % KVH)
    for j in range(LEAD):
        receive_own(j)
    bias = cache_bias(z)
    for i, h in enumerate(HEADS):
        receive(0, i)
        for yy in (y, 1 - y):
            source = device(z, yy, 1 - core)
            arrived(full(source, h), source, h)
        attend(h, z, "own", bias)
        if i == 0:
            receive_far(1)

    receive_far(2)

    def step(t, carry):
        zs = z_at(t)
        bias = cache_bias(zs)
        for i, h in enumerate(HEADS):
            receive(t, i)
            pair_arrived(zs, i)
            pl.when(zs < z)(lambda: attend(h, zs, "all", bias))
            pl.when(zs > z)(lambda: attend(h, zs, "cache", bias))
            if i > 0:

                @pl.when((t == 1) & (z > 0))
                def _():
                    if i == 1:
                        for d in range(3, n_z):
                            receive_far(d)
                    if i == 2:
                        foreign()
                    if i == 3:
                        for d in range(1, n_z):
                            pl.when(z >= d)(lambda: give(z - d))

        return carry

    lax.fori_loop(1, n_z, step, 0)

    def collect(zs, carry):
        merge(zs)
        return carry

    lax.fori_loop(z + 1, n_z, collect, 0)
    for h in range(KVH):
        mixed = acc[h] / row_sum[h]
        for g in range(GROUP):
            column = (h * GROUP + g) * HD
            out_ref[:, column : column + HD] = mixed[
                g * prompt_rows : (g + 1) * prompt_rows, :
            ].astype(jnp.bfloat16)
        rows16[h] = mixed[many:, :]
        for g in range(GROUP):
            column = (h * GROUP + g) * HD
            cont_ref[:, column : column + HD] = rows16[
                h, g * conts : (g + 1) * conts, :
            ].astype(jnp.bfloat16)

    def sent(source, kind, count, cache_only=False):
        ref = kv.at[source, pl.ds(0, count)]
        if cache_only:
            ref = kv.at[source, pl.ds(0, count), 0]
        pltpu.make_async_copy(ref, ref, send_sem.at[source, kind]).wait()

    @pl.when(z < last)
    def _():
        sent(me, 0, KVH)
        pltpu.make_async_copy(cq, cq, far_send.at[z]).wait()

    @pl.when(z > 0)
    def _():
        sent(me, 3, KVH, True)

    sent(me, 1, KVH)
    sent(me, 2, KVH)

    def drain(zs, carry):
        source = device(zs, y, core)
        other = device(zs, 1 - y, core)

        @pl.when(zs < z)
        def _():
            @pl.when(z < last)
            def _():
                sent(source, 0, KVH)
                pltpu.make_async_copy(far_cq.at[zs], far_cq.at[zs], far_send.at[zs]).wait()

            pl.when(zs < lines)(lambda: sent(source, 1, KVH - len(BY_LINE)))
            pl.when(zs >= lines)(lambda: sent(source, 1, KVH))
            sent(source, 2, KVH)
            for copy in part_copies(zs):
                copy.wait_send()

        @pl.when(zs > z)
        def _():
            pl.when(z > 0)(lambda: sent(source, 0, KVH, True))
            sent(source, 1, KVH, True)
            sent(source, 2, KVH, True)
            sent(other, 2, KVH, True)

        @pl.when(zs <= z)
        def _():
            sent(other, 2, KVH)
            pl.when((z < last) & (zs < lines))(lambda: sent(other, 0, len(BY_LINE)))

        return carry

    lax.fori_loop(0, n_z, drain, 0)


def line_shape(mesh):
    chips = mesh.shape["ctx"] // CORES
    place = mesh.axis_names.index("ctx")
    index = [0] * mesh.devices.ndim
    index[place] = slice(None)
    coords = [getattr(d, "coords", None) for d in mesh.devices[tuple(index)]]
    n_y = 1
    if all(c is not None for c in coords) and len({c[1] for c in coords}) == 2:
        n_y = 2
    return chips // n_y, n_y


def solution(mesh):
    n_z, n_y = line_shape(mesh)
    n_ctx = mesh.shape["ctx"]

    def plane_body(ck, cv, nq, nk, nv, cq, sk, sv, ws, pfx, length):
        half = ck.shape[0]
        few = GROUP * cq.shape[0]
        total = GROUP * nq.shape[0] + few
        anywhere = pl.BlockSpec(memory_space=pl.ANY)
        vmem = pl.BlockSpec(memory_space=pltpu.VMEM)
        state = pltpu.VMEM((KVH, total, HD), jnp.float32)
        part = pltpu.VMEM((n_z, KVH * few, HD), jnp.float32)
        levels = pltpu.VMEM((n_z, 8, HD), jnp.float32)
        return pl.pallas_call(
            functools.partial(plane_kernel, n_z),
            out_shape=(
                pltpu.VMEM(nq.shape, jnp.bfloat16),
                pltpu.VMEM(cq.shape, jnp.bfloat16),
            ),
            in_specs=[anywhere] * 11,
            out_specs=(vmem, vmem),
            scratch_shapes=[
                pltpu.VMEM((n_ctx, KVH, 2, 2, half, HD), jnp.bfloat16),
                pltpu.VMEM((KVH, total, HD), jnp.bfloat16),
                pltpu.VMEM(sk.shape, jnp.bfloat16),
                pltpu.VMEM(sv.shape, jnp.bfloat16),
                pltpu.VMEM((KVH, few, HD), jnp.float32),
                pltpu.VMEM((total, HD), jnp.int32),
                state,
                state,
                state,
                pltpu.VMEM(cq.shape, jnp.bfloat16),
                pltpu.VMEM((n_z,) + cq.shape, jnp.bfloat16),
                pltpu.VMEM((KVH, few * (n_z - 1), HD), jnp.float32),
                part,
                part,
                levels,
                levels,
                pltpu.SMEM(ws.shape, jnp.int32),
                pltpu.SMEM(pfx.shape, jnp.int32),
                pltpu.SMEM(length.shape, jnp.int32),
                pltpu.SemaphoreType.DMA((KVH,)),
                pltpu.SemaphoreType.DMA,
                pltpu.SemaphoreType.DMA((2,)),
                pltpu.SemaphoreType.DMA((4,)),
                pltpu.SemaphoreType.DMA((n_ctx, KVH)),
                pltpu.SemaphoreType.DMA((n_ctx, 4)),
                pltpu.SemaphoreType.DMA((n_z,)),
                pltpu.SemaphoreType.DMA((n_z,)),
                pltpu.SemaphoreType.DMA((n_z, 2)),
                pltpu.SemaphoreType.DMA((n_z, 2)),
            ],
            compiler_params=pltpu.CompilerParams(
                collective_id=0, has_side_effects=True, vmem_limit_bytes=60 * 1024 * 1024
            ),
        )(ck, cv, nq, nk, nv, cq, sk, sv, ws, pfx, length)

    def body(ck, cv, nq, nk, nv, cq, sk, sv, ws, pfx, length):
        half, width = ck.shape
        rows = nq.shape[0]
        conts = cq.shape[0]
        total = GROUP * (rows + conts)
        anywhere = pl.BlockSpec(memory_space=pl.ANY)
        vmem = pl.BlockSpec(memory_space=pltpu.VMEM)
        return pl.pallas_call(
            functools.partial(kernel, n_z, n_y),
            out_shape=(
                pltpu.VMEM(nq.shape, jnp.bfloat16),
                pltpu.VMEM(cq.shape, jnp.bfloat16),
            ),
            in_specs=[anywhere] * 11,
            out_specs=(vmem, vmem),
            scratch_shapes=[
                pltpu.VMEM((n_ctx, 2, 2 * half, width), jnp.bfloat16),
                pltpu.VMEM((KVH, total, HD), jnp.bfloat16),
                pltpu.VMEM(sk.shape, jnp.bfloat16),
                pltpu.VMEM(sv.shape, jnp.bfloat16),
                pltpu.VMEM((KVH, GROUP * conts, HD), jnp.float32),
                pltpu.VMEM((total, HD), jnp.int32),
                pltpu.VMEM((KVH, total, HD), jnp.float32),
                pltpu.VMEM((KVH, total, HD), jnp.float32),
                pltpu.VMEM((KVH, total, HD), jnp.float32),
                pltpu.VMEM(cq.shape, jnp.bfloat16),
                pltpu.SMEM(ws.shape, jnp.int32),
                pltpu.SMEM(pfx.shape, jnp.int32),
                pltpu.SMEM(length.shape, jnp.int32),
                pltpu.SemaphoreType.DMA((PIECES,)),
                pltpu.SemaphoreType.DMA,
                pltpu.SemaphoreType.DMA((2,)),
                pltpu.SemaphoreType.DMA((n_ctx, PIECES)),
                pltpu.SemaphoreType.DMA((n_ctx,)),
                pltpu.SemaphoreType.DMA((n_ctx, 5)),
                pltpu.SemaphoreType.DMA((4,)),
            ],
            compiler_params=pltpu.CompilerParams(
                collective_id=0, has_side_effects=True, vmem_limit_bytes=60 * 1024 * 1024
            ),
        )(ck, cv, nq, nk, nv, cq, sk, sv, ws, pfx, length)

    part = P(("grp", "ctx"), None)
    part3 = P(("grp", "ctx"), None, None)
    in_specs = (part,) * 6 + (part3, part3, P("grp"), P("grp"), P(("grp", "ctx")))
    return jax.shard_map(
        plane_body if n_y == 2 and n_z > 2 else body,
        mesh=mesh, in_specs=in_specs, out_specs=(part, part), check_vma=False
    )
```

```python
import functools
import math

import jax
import jax.numpy as jnp
from jax import lax
from jax.experimental import pallas as pl
from jax.experimental.pallas import tpu as pltpu
from jax.sharding import PartitionSpec as P

KVH = 4
HD = 128
GROUP = 8
CORES = 2
PIECES = 4
EXTRA = 3
ORDER = (EXTRA, 0, 1, 2)
MESH = pl.DeviceIdType.MESH
SCALE2 = HD ** (-0.5) * math.log2(math.e)
HIDDEN = 1 << 30


def kernel(
    n_z,
    n_y,
    ck_ref,
    cv_ref,
    nq_ref,
    nk_ref,
    nv_ref,
    cq_hbm,
    sk_ref,
    sv_ref,
    start_hbm,
    prefix_hbm,
    length_hbm,
    out_ref,
    cont_ref,
    kv,
    q,
    sk,
    sv,
    rows16,
    limit,
    row_max,
    row_sum,
    acc,
    cq_ref,
    start_ref,
    prefix_ref,
    length_ref,
    local_sem,
    query_sem,
    suffix_sem,
    recv_sem,
    pair_sem,
    send_sem,
    small_sem,
):
    half = ck_ref.shape[0]
    prompt_rows = nq_ref.shape[0]
    conts = cq_hbm.shape[0]
    suffix_rows = sk_ref.shape[1]
    many = GROUP * prompt_rows
    total = many + GROUP * conts
    me = lax.axis_index("ctx")
    core = me % CORES
    chip = me // CORES
    y = chip % n_y
    z = chip // n_y

    def device(zz, yy, cc):
        return (zz * n_y + yy) * CORES + cc

    own = []
    for p, ref in enumerate((ck_ref, nk_ref, cv_ref, nv_ref)):
        copy = pltpu.make_async_copy(
            ref, kv.at[me, p // 2, pl.ds((p % 2) * half, half)], local_sem.at[p]
        )
        copy.start()
        own.append(copy)
    for h in range(KVH):
        for g in range(GROUP):
            pltpu.make_async_copy(
                nq_ref.at[:, pl.ds((h * GROUP + g) * HD, HD)],
                q.at[h, pl.ds(g * prompt_rows, prompt_rows)],
                query_sem,
            ).start()
    suffix_copies = [
        pltpu.make_async_copy(sk_ref, sk, suffix_sem.at[0]),
        pltpu.make_async_copy(sv_ref, sv, suffix_sem.at[1]),
    ]
    small_copies = [
        pltpu.make_async_copy(src, dst, small_sem.at[i])
        for i, (src, dst) in enumerate(
            (
                (cq_hbm, cq_ref),
                (start_hbm, start_ref),
                (prefix_hbm, prefix_ref),
                (length_hbm, length_ref),
            )
        )
    ]
    for copy in suffix_copies + small_copies:
        copy.start()

    barrier = pltpu.get_barrier_semaphore()

    def greet(target):
        pl.semaphore_signal(barrier, inc=1, device_id={"ctx": target}, device_id_type=MESH)

    greet(device(z, y, 1 - core))
    if n_y == 2:
        greet(device(z, 1 - y, core))

    @pl.when(z > 0)
    def _():
        greet(device(z - 1, y, core))

    @pl.when(z < n_z - 1)
    def _():
        greet(device(z + 1, y, core))

    line_neighbours = (z + n_z - 1) // n_z + (2 * n_z - 2 - z) // n_z
    pl.semaphore_wait(barrier, n_y + line_neighbours)

    def piece(source, p):
        return kv.at[source, p // 2, pl.ds((p % 2) * half, half)]

    def send(source, p, target, kind):
        ref = piece(source, p)
        sem = pair_sem.at[source] if kind == 2 else recv_sem.at[source, p]
        pltpu.make_async_remote_copy(
            src_ref=ref,
            dst_ref=ref,
            send_sem=send_sem.at[source, kind],
            recv_sem=sem,
            device_id={"ctx": target},
            device_id_type=MESH,
        ).start()

    def arrived(source, p):
        ref = piece(source, p)
        pltpu.make_async_copy(ref, ref, recv_sem.at[source, p]).wait()

    def pair_arrived(source):
        pltpu.make_async_copy(kv.at[source], kv.at[source], pair_sem.at[source]).wait()

    def sent(source, kind, pieces=PIECES):
        ref = kv.at[source]
        if pieces == 1:
            ref = piece(source, EXTRA)
        elif pieces < PIECES:
            ref = kv.at[source, :, pl.ds(0, pieces * half // 2)]
        pltpu.make_async_copy(ref, ref, send_sem.at[source, kind]).wait()

    def by_line(zs):
        return ((zs < z) & (zs < n_z - 2)) | ((zs > z) & (zs > 1))

    def not_by_line(zs):
        return ((zs < z) & (zs >= n_z - 2)) | ((zs > z) & (zs <= 1)) | (zs == z)

    partner = device(z, y, 1 - core)
    across = device(z, 1 - y, core)
    above = device(z + 1, y, core)
    below = device(z - 1, y, core)

    for p in ORDER:
        own[p].wait()

        @pl.when(z < n_z - 1)
        def _():
            send(me, p, above, 0)

        if n_y == 2:
            send(me, p, across, 4 if p == EXTRA else 1)

        @pl.when(z > 0)
        def _():
            send(me, p, below, 3)

        send(me, p, partner, 2)

    near = jnp.minimum(z, n_z - 1 - z)

    def z_at(t):
        if isinstance(t, int) and t == 0:
            return z
        step = (t + 1) // 2
        both = z + step * (1 - 2 * (t % 2))
        far = jnp.where(z + z < n_z - 1, t, n_z - 1 - t)
        return jnp.where(t <= 2 * near, both, far)

    row = lax.broadcasted_iota(jnp.int32, (total, HD), 0)
    limit[...] = jnp.where(row < many, me * prompt_rows + row % prompt_rows, HIDDEN - 1)
    row_max[...] = jnp.full_like(row_max, -1e30)
    row_sum[...] = jnp.zeros_like(row_sum)
    acc[...] = jnp.zeros_like(acc)
    for copy in small_copies:
        copy.wait()
    for h in range(KVH):
        for g in range(GROUP):
            column = (h * GROUP + g) * HD
            rows16[h, g * conts : (g + 1) * conts, :] = cq_ref[:, column : column + HD].astype(
                jnp.float32
            )
    q[:, many:, :] = rows16[...].astype(jnp.bfloat16)

    for copy in suffix_copies:
        copy.wait()
    for h in range(KVH):
        keys = sk[:, :, h * HD : (h + 1) * HD].reshape(conts * suffix_rows, HD)
        values = sv[:, :, h * HD : (h + 1) * HD].reshape(conts * suffix_rows, HD)
        s = lax.dot_general(
            q[h, many:, :], keys, (((1,), (1,)), ((), ())), preferred_element_type=jnp.float32
        )
        who = lax.broadcasted_iota(jnp.int32, s.shape, 0) % conts
        column = lax.broadcasted_iota(jnp.int32, s.shape, 1)
        reach = jnp.zeros_like(who)
        for c in range(conts):
            reach = jnp.where(who == c, length_ref[c], reach)
        seen = (column // suffix_rows == who) & (column % suffix_rows < reach)
        s = jnp.where(seen, s * SCALE2, -1e30)
        top = jnp.max(s, axis=1, keepdims=True)
        w = jnp.exp2(s - top)
        row_max[h, many:, :] = jnp.broadcast_to(top, (GROUP * conts, HD))
        folded = w[:, :HD]
        for b in range(1, s.shape[1] // HD):
            folded = folded + w[:, b * HD : (b + 1) * HD]
        row_sum[h, many:, :] = folded
        acc[h, many:, :] = jnp.dot(
            w.astype(jnp.bfloat16), values, preferred_element_type=jnp.float32
        )

    span = CORES * 2 * half
    window_first = start_ref[0]
    prefix_last = prefix_ref[0]

    def places(chip_index):
        column = lax.broadcasted_iota(jnp.int32, (1, span), 1)
        within = column % (2 * half)
        position = (chip_index * CORES + column // (2 * half)) * half + within % half
        cached = jnp.where(
            (position >= window_first) & (position < prefix_last), -1, HIDDEN
        )
        return jnp.where(within < half, cached, position)

    def attend(h, chips, marks):
        cols = slice(h * HD, (h + 1) * HD)
        keys = [kv[pl.ds(c * CORES, CORES), 0, :, cols].reshape(span, HD) for c in chips]
        values = [kv[pl.ds(c * CORES, CORES), 1, :, cols].reshape(span, HD) for c in chips]
        keys = jnp.concatenate(keys, axis=0)
        values = jnp.concatenate(values, axis=0)
        mark = jnp.concatenate(marks, axis=1)
        count = span * len(chips)
        cut = (total // 2 + 15) // 16 * 16
        for lo, hi in ((0, cut), (cut, total)):
            s = lax.dot_general(
                q[h, lo:hi, :], keys, (((1,), (1,)), ((), ())), preferred_element_type=jnp.float32
            )
            bound = limit[lo:hi, :]
            blocks = []
            for b in range(count // HD):
                part = slice(b * HD, (b + 1) * HD)
                blocks.append(jnp.where(mark[:, part] <= bound, s[:, part] * SCALE2, -1e30))
            peak = functools.reduce(jnp.maximum, blocks)
            old = row_max[h, lo:hi, :]
            new = jnp.maximum(old, jnp.max(peak, axis=1, keepdims=True))
            alpha = jnp.exp2(old - new)
            w = [jnp.exp2(b - new) for b in blocks]
            row_max[h, lo:hi, :] = new
            row_sum[h, lo:hi, :] = row_sum[h, lo:hi, :] * alpha + functools.reduce(jnp.add, w)
            wb = jnp.concatenate([b.astype(jnp.bfloat16) for b in w], axis=1)
            acc[h, lo:hi, :] = acc[h, lo:hi, :] * alpha + jnp.dot(
                wb, values, preferred_element_type=jnp.float32
            )

    def onward(source, zs, p):
        @pl.when((zs < z) & (z < n_z - 1))
        def _():
            send(source, p, above, 0)

        @pl.when((zs > z) & (z > 0))
        def _():
            send(source, p, below, 0)

    def receive_z(zs, p):
        source = device(zs, y, core)
        arrived(source, p)
        onward(source, zs, p)
        if n_y == 2 and p == EXTRA:

            @pl.when(not_by_line(zs))
            def _():
                send(source, p, across, 4)

        elif n_y == 2:
            send(source, p, across, 1)
        send(source, p, partner, 2)

    def receive_extra(zs):
        @pl.when(by_line(zs))
        def _():
            source = device(zs, 1 - y, core)
            arrived(source, EXTRA)
            onward(source, zs, EXTRA)
            send(source, EXTRA, partner, 2)

    def receive_far(d):
        low = z - d

        @pl.when(low >= 0)
        def _():
            pltpu.make_async_copy(far_cq.at[low], far_cq.at[low], far_recv.at[low]).wait()

            @pl.when(z < last)
            def _():
                far_copy(low, above).start()

    def receive_line(d, i):
        for zs, inside in ((z - d, z - d >= 0), (z + d, z + d < n_z)):

            @pl.when(inside)
            def _():
                receive_z(zs, ORDER[i])
                if n_y == 2 and i == PIECES - 1:
                    receive_extra(zs)

    def receive_y(zs, i):
        source = device(zs, 1 - y, core)
        p = ORDER[i]

        def take():
            arrived(source, p)
            send(source, p, partner, 2)

        if p == EXTRA:
            pl.when(not_by_line(zs))(take)
        else:
            take()

    def receive_pair(i):
        receive_y(z, i)
        if ORDER[i] == EXTRA:
            source = device(z, 1 - y, core)

            @pl.when(z < n_z - 2)
            def _():
                send(source, EXTRA, above, 0)

            @pl.when(z > 1)
            def _():
                send(source, EXTRA, below, 3)

    pltpu.make_async_copy(q.at[:, pl.ds(0, many)], q.at[:, pl.ds(0, many)], query_sem).wait()
    pair_arrived(partner)
    mark = places(chip)
    for h in range(KVH):
        attend(h, [chip], [mark])
        receive_line(1, h)
        if n_y == 2:
            receive_pair(h)

    def step(t, carry):
        zs, zb = z_at(t), z_at(t - 1)
        pair_arrived(device(zs, y, 1 - core))
        chips = [zs * n_y + y]
        if n_y == 2:
            pair_arrived(device(zb, 1 - y, 1 - core))
            chips.append(zb * n_y + 1 - y)
        marks = [places(c) for c in chips]
        for h in range(KVH):
            attend(h, chips, marks)

            @pl.when(t < n_z - 1)
            def _():
                receive_line(t + 1, h)

            if n_y == 2:
                receive_y(zs, h)
        return carry

    lax.fori_loop(1, n_z, step, 0)
    chips = []
    if n_y == 2:
        zb = z_at(jnp.int32(n_z - 1))
        pair_arrived(device(zb, 1 - y, 1 - core))
        chips = [zb * n_y + 1 - y]
    marks = [places(c) for c in chips]
    for h in range(KVH):
        if n_y == 2:
            attend(h, chips, marks)
        mixed = acc[h] / jnp.sum(row_sum[h], axis=1, keepdims=True)
        for g in range(GROUP):
            column = (h * GROUP + g) * HD
            out_ref[:, column : column + HD] = mixed[
                g * prompt_rows : (g + 1) * prompt_rows, :
            ].astype(jnp.bfloat16)
        rows16[h] = mixed[many:, :]
        for g in range(GROUP):
            column = (h * GROUP + g) * HD
            cont_ref[:, column : column + HD] = rows16[
                h, g * conts : (g + 1) * conts, :
            ].astype(jnp.bfloat16)

    @pl.when(z < n_z - 1)
    def _():
        sent(me, 0)

    @pl.when(z > 0)
    def _():
        sent(me, 3)

    sent(me, 2)
    if n_y == 2:
        pair = device(z, 1 - y, core)
        sent(me, 1, PIECES - 1)
        sent(me, 4, 1)

        @pl.when(z < n_z - 2)
        def _():
            sent(pair, 0, 1)

        @pl.when(z > 1)
        def _():
            sent(pair, 3, 1)

    def drain(zs, carry):
        source = device(zs, y, core)
        middle = ((zs < z) & (z < n_z - 1)) | ((zs > z) & (z > 0))

        @pl.when(middle)
        def _():
            sent(source, 0)

        @pl.when(zs != z)
        def _():
            if n_y == 2:
                sent(source, 1, PIECES - 1)
            sent(source, 2)

        if n_y == 2:
            other = device(zs, 1 - y, core)

            @pl.when((zs != z) & not_by_line(zs))
            def _():
                sent(source, 4, 1)

            @pl.when(middle & by_line(zs))
            def _():
                sent(other, 0, len(BY_LINE))

            sent(other, 2)
        return carry

    lax.fori_loop(0, n_z, drain, 0)


HEADS = (0, 1, 2, 3)
BY_LINE = (3,)
LEAD = 2
AHEAD = 2


def pack_rows(values):
    lane = lax.broadcasted_iota(jnp.int32, (8, HD), 1)
    tile = jnp.zeros((8, HD), jnp.float32)
    for i in range(values.shape[0] // 8):
        tile = jnp.where(lane == i, values[8 * i : 8 * i + 8, :], tile)
    return tile


def unpack_rows(tile, first, count):
    lane = lax.broadcasted_iota(jnp.int32, (8, HD), 1)
    blocks = [
        jnp.max(jnp.where(lane == i, tile, -3e38), axis=1, keepdims=True)
        for i in range(first // 8, (first + count) // 8)
    ]
    return jnp.concatenate(blocks, axis=0)


def plane_kernel(
    n_z,
    ck_ref,
    cv_ref,
    nq_ref,
    nk_ref,
    nv_ref,
    cq_hbm,
    sk_ref,
    sv_ref,
    start_hbm,
    prefix_hbm,
    length_hbm,
    out_ref,
    cont_ref,
    kv,
    q,
    sk,
    sv,
    rows16,
    limit,
    row_max,
    row_sum,
    acc,
    cq,
    far_cq,
    far_rows,
    part_out,
    part_in,
    lse_out,
    lse_in,
    start_ref,
    prefix_ref,
    length_ref,
    local_sem,
    query_sem,
    suffix_sem,
    small_sem,
    recv_sem,
    send_sem,
    far_recv,
    far_send,
    part_recv,
    part_send,
):
    n_y = 2
    half = ck_ref.shape[0]
    prompt_rows = nq_ref.shape[0]
    conts = cq_hbm.shape[0]
    suffix_rows = sk_ref.shape[1]
    many = GROUP * prompt_rows
    few = GROUP * conts
    total = many + few
    me = lax.axis_index("ctx")
    core = me % CORES
    chip = me // CORES
    y = chip % n_y
    z = chip // n_y
    last = n_z - 1
    lines = n_z - 2
    plane = n_y * CORES
    span = plane * half

    def device(zz, yy, cc):
        return (zz * n_y + yy) * CORES + cc

    partner = device(z, y, 1 - core)
    across = device(z, 1 - y, core)
    above = device(z + 1, y, core)
    below = device(z - 1, y, core)

    barrier = pltpu.get_barrier_semaphore()

    def greet(target):
        pl.semaphore_signal(barrier, inc=1, device_id={"ctx": target}, device_id_type=MESH)

    greet(partner)
    greet(across)

    @pl.when(z > 0)
    def _():
        greet(below)

    @pl.when(z < last)
    def _():
        greet(above)

    for h in HEADS:
        cols = pl.ds(h * HD, HD)
        for kind, pair in enumerate(((ck_ref, cv_ref), (nk_ref, nv_ref))):
            for i, ref in enumerate(pair):
                pltpu.make_async_copy(ref.at[:, cols], kv.at[me, h, kind, i], local_sem.at[h]).start()
    small = [
        pltpu.make_async_copy(src, dst, small_sem.at[i])
        for i, (src, dst) in enumerate(
            (
                (cq_hbm, cq),
                (start_hbm, start_ref),
                (prefix_hbm, prefix_ref),
                (length_hbm, length_ref),
            )
        )
    ]
    for copy in small:
        copy.start()
    for h in HEADS:
        for g in range(GROUP):
            pltpu.make_async_copy(
                nq_ref.at[:, pl.ds((h * GROUP + g) * HD, HD)],
                q.at[h, pl.ds(g * prompt_rows, prompt_rows)],
                query_sem,
            ).start()
    suffix_copies = [
        pltpu.make_async_copy(sk_ref, sk, suffix_sem.at[0]),
        pltpu.make_async_copy(sv_ref, sv, suffix_sem.at[1]),
    ]
    for copy in suffix_copies:
        copy.start()

    line_neighbours = (z + n_z - 1) // n_z + (2 * n_z - 2 - z) // n_z
    pl.semaphore_wait(barrier, n_y + line_neighbours)

    def full(source, h):
        return kv.at[source, h]

    def cached(source, h):
        return kv.at[source, h, 0]

    def send(ref, source, h, target, kind):
        pltpu.make_async_remote_copy(
            src_ref=ref,
            dst_ref=ref,
            send_sem=send_sem.at[source, kind],
            recv_sem=recv_sem.at[source, h],
            device_id={"ctx": target},
            device_id_type=MESH,
        ).start()

    def arrived(ref, source, h):
        pltpu.make_async_copy(ref, ref, recv_sem.at[source, h]).wait()

    def far_copy(zs, target):
        return pltpu.make_async_remote_copy(
            src_ref=far_cq.at[zs],
            dst_ref=far_cq.at[zs],
            send_sem=far_send.at[zs],
            recv_sem=far_recv.at[zs],
            device_id={"ctx": target},
            device_id_type=MESH,
        )

    small[0].wait()

    @pl.when(z < last)
    def _():
        pltpu.make_async_remote_copy(
            src_ref=cq,
            dst_ref=far_cq.at[z],
            send_sem=far_send.at[z],
            recv_sem=far_recv.at[z],
            device_id={"ctx": above},
            device_id_type=MESH,
        ).start()

    for h in HEADS:
        pltpu.make_async_copy(full(me, h), full(me, h), local_sem.at[h]).wait()

        @pl.when(z < last)
        def _():
            send(full(me, h), me, h, above, 0)

        send(full(me, h), me, h, across, 1)

        @pl.when(z > 0)
        def _():
            send(cached(me, h), me, h, below, 3)

        send(full(me, h), me, h, partner, 2)

    near = jnp.minimum(z, last - z)

    def z_at(t):
        step = (t + 1) // 2
        both = z + step * (1 - 2 * (t % 2))
        far = jnp.where(z + z < last, t, last - t)
        return jnp.where(t <= 2 * near, both, far)

    row = lax.broadcasted_iota(jnp.int32, (total, HD), 0)
    limit[...] = jnp.where(row < many, (me % plane) * prompt_rows + row % prompt_rows, HIDDEN)
    row_max[...] = jnp.full_like(row_max, -1e30)
    row_sum[...] = jnp.zeros_like(row_sum)
    acc[...] = jnp.zeros_like(acc)

    def spread(rows):
        for h in range(KVH):
            for g in range(GROUP):
                column = (h * GROUP + g) * HD
                rows16[h, g * conts : (g + 1) * conts, :] = rows[:, column : column + HD].astype(
                    jnp.float32
                )

    for zs in range(last):

        @pl.when(zs >= z)
        def _():
            far_cq[zs] = jnp.zeros(far_cq.shape[1:], jnp.bfloat16)

    spread(cq)
    q[:, many:, :] = rows16[...].astype(jnp.bfloat16)
    for copy in small[1:]:
        copy.wait()
    for copy in suffix_copies:
        copy.wait()
    for h in range(KVH):
        keys = sk[:, :, h * HD : (h + 1) * HD].reshape(conts * suffix_rows, HD)
        values = sv[:, :, h * HD : (h + 1) * HD].reshape(conts * suffix_rows, HD)
        s = lax.dot_general(
            q[h, many:, :], keys, (((1,), (1,)), ((), ())), preferred_element_type=jnp.float32
        )
        who = lax.broadcasted_iota(jnp.int32, s.shape, 0) % conts
        column = lax.broadcasted_iota(jnp.int32, s.shape, 1)
        reach = jnp.zeros_like(who)
        for c in range(conts):
            reach = jnp.where(who == c, length_ref[c], reach)
        seen = (column // suffix_rows == who) & (column % suffix_rows < reach)
        s = jnp.where(seen, s * SCALE2, -1e30)
        top = jnp.max(s, axis=1, keepdims=True)
        w = jnp.exp2(s - top)
        row_max[h, many:, :] = jnp.broadcast_to(top, (few, HD))
        row_sum[h, many:, :] = jnp.broadcast_to(jnp.sum(w, axis=1, keepdims=True), (few, HD))
        acc[h, many:, :] = jnp.dot(
            w.astype(jnp.bfloat16), values, preferred_element_type=jnp.float32
        )

    window_first = start_ref[0]
    prefix_last = prefix_ref[0]

    def cache_bias(zs):
        position = zs * span + lax.broadcasted_iota(jnp.int32, (1, span), 1)
        return jnp.where((position >= window_first) & (position < prefix_last), 0.0, -1e30)

    def plane_rows(zs, h, kind, i):
        return kv[pl.ds(zs * plane, plane), h, kind, i].reshape(span, HD)

    def summed(values):
        return jnp.concatenate([values, jnp.ones(values.shape, jnp.bfloat16)], axis=1)

    def attend(h, zs, mode, bias):
        keys = plane_rows(zs, h, 0, 0)
        values = plane_rows(zs, h, 0, 1)
        if mode != "cache":
            keys = jnp.concatenate([keys, plane_rows(zs, h, 1, 0)], axis=0)
            values = jnp.concatenate([values, plane_rows(zs, h, 1, 1)], axis=0)
        values = summed(values)
        cut = (total // 2 + 15) // 16 * 16
        for lo, hi in ((0, cut), (cut, total)):
            s = lax.dot_general(
                q[h, lo:hi, :], keys, (((1,), (1,)), ((), ())), preferred_element_type=jnp.float32
            )
            blocks = []
            for b in range(keys.shape[0] // HD):
                part = s[:, b * HD : (b + 1) * HD] * SCALE2
                if b < span // HD:
                    part = part + bias[:, b * HD : (b + 1) * HD]
                elif mode == "own":
                    at = (b - span // HD) * HD + lax.broadcasted_iota(jnp.int32, (1, HD), 1)
                    part = jnp.where(at <= limit[lo:hi, :], part, -1e30)
                blocks.append(part)
            peak = functools.reduce(jnp.maximum, blocks)
            old = row_max[h, lo:hi, :]
            new = jnp.maximum(old, jnp.max(peak, axis=1, keepdims=True))
            alpha = jnp.exp2(old - new)
            w = [jnp.exp2(b - new) for b in blocks]
            row_max[h, lo:hi, :] = new
            wb = jnp.concatenate([b.astype(jnp.bfloat16) for b in w], axis=1)
            mixed = jnp.dot(wb, values, preferred_element_type=jnp.float32)
            acc[h, lo:hi, :] = acc[h, lo:hi, :] * alpha + mixed[:, :HD]
            row_sum[h, lo:hi, :] = row_sum[h, lo:hi, :] * alpha + mixed[:, HD:]

    def foreign():
        for zs in range(last):
            rows = far_cq.at[zs]
            for h in range(KVH):
                for g in range(GROUP):
                    column = (h * GROUP + g) * HD
                    first = zs * few + g * conts
                    far_rows[h, first : first + conts, :] = rows[:, column : column + HD].astype(
                        jnp.float32
                    )
        sums = []
        for h in range(KVH):
            s = lax.dot_general(
                far_rows[h].astype(jnp.bfloat16),
                plane_rows(z, h, 1, 0),
                (((1,), (1,)), ((), ())),
                preferred_element_type=jnp.float32,
            )
            s = s * SCALE2
            top = jnp.max(s, axis=1, keepdims=True)
            w = jnp.exp2(s - top)
            both = jnp.dot(
                w.astype(jnp.bfloat16),
                summed(plane_rows(z, h, 1, 1)),
                preferred_element_type=jnp.float32,
            )
            under = both[:, HD:]
            mixed = both[:, :HD] / under
            for zs in range(last):
                part_out[zs, h * few : (h + 1) * few, :] = mixed[zs * few : (zs + 1) * few, :]
            sums.append(top + jnp.log2(under))
        for zs in range(last):
            lse_out[zs] = pack_rows(
                jnp.concatenate([level[zs * few : (zs + 1) * few, :] for level in sums], axis=0)
            )

    def part_copies(zs):
        return [
            pltpu.make_async_remote_copy(
                src_ref=src.at[zs],
                dst_ref=dst.at[z],
                send_sem=part_send.at[zs, i],
                recv_sem=part_recv.at[z, i],
                device_id={"ctx": device(zs, y, core)},
                device_id_type=MESH,
            )
            for i, (src, dst) in enumerate(((part_out, part_in), (lse_out, lse_in)))
        ]

    def merge(zs):
        for i, ref in enumerate((part_in, lse_in)):
            pltpu.make_async_copy(ref.at[zs], ref.at[zs], part_recv.at[zs, i]).wait()
        tile = lse_in[zs]
        for h in range(KVH):
            level = unpack_rows(tile, h * few, few)
            old = row_max[h, many:, :]
            new = jnp.maximum(old, level)
            alpha = jnp.exp2(old - new)
            beta = jnp.exp2(level - new)
            row_max[h, many:, :] = new
            row_sum[h, many:, :] = row_sum[h, many:, :] * alpha + beta
            acc[h, many:, :] = (
                acc[h, many:, :] * alpha + part_in[zs, h * few : (h + 1) * few, :] * beta
            )

    def receive_far(d):
        low = z - d

        @pl.when(low >= 0)
        def _():
            pltpu.make_async_copy(far_cq.at[low], far_cq.at[low], far_recv.at[low]).wait()

            @pl.when(z < last)
            def _():
                far_copy(low, above).start()

    def receive_line(d, i):
        h = HEADS[i]
        low, high = z - d, z + d

        @pl.when(low >= 0)
        def _():
            source = device(low, y, core)
            ref = full(source, h)
            arrived(ref, source, h)

            @pl.when(z < last)
            def _():
                send(ref, source, h, above, 0)

            if h in BY_LINE:

                @pl.when(low >= lines)
                def _():
                    send(ref, source, h, across, 1)

            else:
                send(ref, source, h, across, 1)
            send(ref, source, h, partner, 2)
        @pl.when(high < n_z)
        def _():
            source = device(high, y, core)
            ref = cached(source, h)
            arrived(ref, source, h)

            @pl.when(z > 0)
            def _():
                send(ref, source, h, below, 0)

            send(ref, source, h, across, 1)
            send(ref, source, h, partner, 2)

    def receive_y(zs, i):
        h = HEADS[i]
        source = device(zs, 1 - y, core)

        def take(ref):
            arrived(ref, source, h)
            send(ref, source, h, partner, 2)

        pl.when(zs <= z)(lambda: take(full(source, h)))
        if h in BY_LINE:
            pl.when((zs < lines) & (zs < z) & (z < last))(
                lambda: send(full(source, h), source, h, above, 0)
            )
        pl.when(zs > z)(lambda: take(cached(source, h)))

    def receive_own(i):
        h = HEADS[i]
        arrived(full(across, h), across, h)
        send(full(across, h), across, h, partner, 2)
        if h in BY_LINE:

            @pl.when((z < last) & (z < lines))
            def _():
                send(full(across, h), across, h, above, 0)

    def pair_arrived(zs, i):
        h = HEADS[i]
        for yy in (y, 1 - y):
            source = device(zs, yy, 1 - core)
            pl.when(zs <= z)(lambda source=source: arrived(full(source, h), source, h))
            pl.when(zs > z)(lambda source=source: arrived(cached(source, h), source, h))

    pltpu.make_async_copy(
        q.at[pl.ds(0, KVH), pl.ds(0, many)], q.at[pl.ds(0, KVH), pl.ds(0, many)], query_sem
    ).wait()
    def receive(t, i):
        q, r = divmod(i + AHEAD - 1, KVH)
        receive_line(t + 1 + q, r)
        q, r = divmod(i + LEAD, KVH)
        if isinstance(t, int):
            receive_own(r) if t + q == 0 else receive_y(z_at(t + q), r)
        else:
            pl.when(t + q < n_z)(lambda: receive_y(z_at(t + q), r))

    def give(zs):
        for copy in part_copies(zs):
            copy.start()

    for j in range(AHEAD - 1):
        receive_line(1 + j // KVH, j % KVH)
    for j in range(LEAD):
        receive_own(j)
    bias = cache_bias(z)
    for i, h in enumerate(HEADS):
        receive(0, i)
        for yy in (y, 1 - y):
            source = device(z, yy, 1 - core)
            arrived(full(source, h), source, h)
        attend(h, z, "own", bias)
        if i == 0:
            receive_far(1)

    receive_far(2)

    def step(t, carry):
        zs = z_at(t)
        bias = cache_bias(zs)
        for i, h in enumerate(HEADS):
            receive(t, i)
            pair_arrived(zs, i)
            pl.when(zs < z)(lambda: attend(h, zs, "all", bias))
            pl.when(zs > z)(lambda: attend(h, zs, "cache", bias))
            if i > 0:

                @pl.when((t == 1) & (z > 0))
                def _():
                    if i == 1:
                        for d in range(3, n_z):
                            receive_far(d)
                    if i == 2:
                        foreign()
                    if i == 3:
                        for d in range(1, n_z):
                            pl.when(z >= d)(lambda: give(z - d))

        return carry

    lax.fori_loop(1, n_z, step, 0)

    def collect(zs, carry):
        merge(zs)
        return carry

    lax.fori_loop(z + 1, n_z, collect, 0)
    for h in range(KVH):
        mixed = acc[h] / row_sum[h]
        for g in range(GROUP):
            column = (h * GROUP + g) * HD
            out_ref[:, column : column + HD] = mixed[
                g * prompt_rows : (g + 1) * prompt_rows, :
            ].astype(jnp.bfloat16)
        rows16[h] = mixed[many:, :]
        for g in range(GROUP):
            column = (h * GROUP + g) * HD
            cont_ref[:, column : column + HD] = rows16[
                h, g * conts : (g + 1) * conts, :
            ].astype(jnp.bfloat16)

    def sent(source, kind, count, cache_only=False):
        ref = kv.at[source, pl.ds(0, count)]
        if cache_only:
            ref = kv.at[source, pl.ds(0, count), 0]
        pltpu.make_async_copy(ref, ref, send_sem.at[source, kind]).wait()

    @pl.when(z < last)
    def _():
        sent(me, 0, KVH)
        pltpu.make_async_copy(cq, cq, far_send.at[z]).wait()

    @pl.when(z > 0)
    def _():
        sent(me, 3, KVH, True)

    sent(me, 1, KVH)
    sent(me, 2, KVH)

    def drain(zs, carry):
        source = device(zs, y, core)
        other = device(zs, 1 - y, core)

        @pl.when(zs < z)
        def _():
            @pl.when(z < last)
            def _():
                sent(source, 0, KVH)
                pltpu.make_async_copy(far_cq.at[zs], far_cq.at[zs], far_send.at[zs]).wait()

            pl.when(zs < lines)(lambda: sent(source, 1, KVH - len(BY_LINE)))
            pl.when(zs >= lines)(lambda: sent(source, 1, KVH))
            sent(source, 2, KVH)
            for copy in part_copies(zs):
                copy.wait_send()

        @pl.when(zs > z)
        def _():
            pl.when(z > 0)(lambda: sent(source, 0, KVH, True))
            sent(source, 1, KVH, True)
            sent(source, 2, KVH, True)
            sent(other, 2, KVH, True)

        @pl.when(zs <= z)
        def _():
            sent(other, 2, KVH)
            pl.when((z < last) & (zs < lines))(lambda: sent(other, 0, len(BY_LINE)))

        return carry

    lax.fori_loop(0, n_z, drain, 0)


def line_shape(mesh):
    chips = mesh.shape["ctx"] // CORES
    place = mesh.axis_names.index("ctx")
    index = [0] * mesh.devices.ndim
    index[place] = slice(None)
    coords = [getattr(d, "coords", None) for d in mesh.devices[tuple(index)]]
    n_y = 1
    if all(c is not None for c in coords) and len({c[1] for c in coords}) == 2:
        n_y = 2
    return chips // n_y, n_y


def solution(mesh):
    n_z, n_y = line_shape(mesh)
    n_ctx = mesh.shape["ctx"]

    def plane_body(ck, cv, nq, nk, nv, cq, sk, sv, ws, pfx, length):
        half = ck.shape[0]
        few = GROUP * cq.shape[0]
        total = GROUP * nq.shape[0] + few
        anywhere = pl.BlockSpec(memory_space=pl.ANY)
        vmem = pl.BlockSpec(memory_space=pltpu.VMEM)
        state = pltpu.VMEM((KVH, total, HD), jnp.float32)
        part = pltpu.VMEM((n_z, KVH * few, HD), jnp.float32)
        levels = pltpu.VMEM((n_z, 8, HD), jnp.float32)
        return pl.pallas_call(
            functools.partial(plane_kernel, n_z),
            out_shape=(
                pltpu.VMEM(nq.shape, jnp.bfloat16),
                pltpu.VMEM(cq.shape, jnp.bfloat16),
            ),
            in_specs=[anywhere] * 11,
            out_specs=(vmem, vmem),
            scratch_shapes=[
                pltpu.VMEM((n_ctx, KVH, 2, 2, half, HD), jnp.bfloat16),
                pltpu.VMEM((KVH, total, HD), jnp.bfloat16),
                pltpu.VMEM(sk.shape, jnp.bfloat16),
                pltpu.VMEM(sv.shape, jnp.bfloat16),
                pltpu.VMEM((KVH, few, HD), jnp.float32),
                pltpu.VMEM((total, HD), jnp.int32),
                state,
                state,
                state,
                pltpu.VMEM(cq.shape, jnp.bfloat16),
                pltpu.VMEM((n_z,) + cq.shape, jnp.bfloat16),
                pltpu.VMEM((KVH, few * (n_z - 1), HD), jnp.float32),
                part,
                part,
                levels,
                levels,
                pltpu.SMEM(ws.shape, jnp.int32),
                pltpu.SMEM(pfx.shape, jnp.int32),
                pltpu.SMEM(length.shape, jnp.int32),
                pltpu.SemaphoreType.DMA((KVH,)),
                pltpu.SemaphoreType.DMA,
                pltpu.SemaphoreType.DMA((2,)),
                pltpu.SemaphoreType.DMA((4,)),
                pltpu.SemaphoreType.DMA((n_ctx, KVH)),
                pltpu.SemaphoreType.DMA((n_ctx, 4)),
                pltpu.SemaphoreType.DMA((n_z,)),
                pltpu.SemaphoreType.DMA((n_z,)),
                pltpu.SemaphoreType.DMA((n_z, 2)),
                pltpu.SemaphoreType.DMA((n_z, 2)),
            ],
            compiler_params=pltpu.CompilerParams(
                collective_id=0, has_side_effects=True, vmem_limit_bytes=60 * 1024 * 1024
            ),
        )(ck, cv, nq, nk, nv, cq, sk, sv, ws, pfx, length)

    def body(ck, cv, nq, nk, nv, cq, sk, sv, ws, pfx, length):
        half, width = ck.shape
        rows = nq.shape[0]
        conts = cq.shape[0]
        total = GROUP * (rows + conts)
        anywhere = pl.BlockSpec(memory_space=pl.ANY)
        vmem = pl.BlockSpec(memory_space=pltpu.VMEM)
        return pl.pallas_call(
            functools.partial(kernel, n_z, n_y),
            out_shape=(
                pltpu.VMEM(nq.shape, jnp.bfloat16),
                pltpu.VMEM(cq.shape, jnp.bfloat16),
            ),
            in_specs=[anywhere] * 11,
            out_specs=(vmem, vmem),
            scratch_shapes=[
                pltpu.VMEM((n_ctx, 2, 2 * half, width), jnp.bfloat16),
                pltpu.VMEM((KVH, total, HD), jnp.bfloat16),
                pltpu.VMEM(sk.shape, jnp.bfloat16),
                pltpu.VMEM(sv.shape, jnp.bfloat16),
                pltpu.VMEM((KVH, GROUP * conts, HD), jnp.float32),
                pltpu.VMEM((total, HD), jnp.int32),
                pltpu.VMEM((KVH, total, HD), jnp.float32),
                pltpu.VMEM((KVH, total, HD), jnp.float32),
                pltpu.VMEM((KVH, total, HD), jnp.float32),
                pltpu.VMEM(cq.shape, jnp.bfloat16),
                pltpu.SMEM(ws.shape, jnp.int32),
                pltpu.SMEM(pfx.shape, jnp.int32),
                pltpu.SMEM(length.shape, jnp.int32),
                pltpu.SemaphoreType.DMA((PIECES,)),
                pltpu.SemaphoreType.DMA,
                pltpu.SemaphoreType.DMA((2,)),
                pltpu.SemaphoreType.DMA((n_ctx, PIECES)),
                pltpu.SemaphoreType.DMA((n_ctx,)),
                pltpu.SemaphoreType.DMA((n_ctx, 5)),
                pltpu.SemaphoreType.DMA((4,)),
            ],
            compiler_params=pltpu.CompilerParams(
                collective_id=0, has_side_effects=True, vmem_limit_bytes=60 * 1024 * 1024
            ),
        )(ck, cv, nq, nk, nv, cq, sk, sv, ws, pfx, length)

    part = P(("grp", "ctx"), None)
    part3 = P(("grp", "ctx"), None, None)
    in_specs = (part,) * 6 + (part3, part3, P("grp"), P("grp"), P(("grp", "ctx")))
    return jax.shard_map(
        plane_body if n_y == 2 and n_z > 2 else body,
        mesh=mesh, in_specs=in_specs, out_specs=(part, part), check_vma=False
    )
```

```python
import functools
import math

import jax
import jax.numpy as jnp
from jax import lax
from jax.experimental import pallas as pl
from jax.experimental.pallas import tpu as pltpu
from jax.sharding import PartitionSpec as P

KVH = 4
HD = 128
GROUP = 8
CORES = 2
PIECES = 4
EXTRA = 3
ORDER = (EXTRA, 0, 1, 2)
MESH = pl.DeviceIdType.MESH
SCALE2 = HD ** (-0.5) * math.log2(math.e)
HIDDEN = 1 << 30


def kernel(
    n_z,
    n_y,
    ck_ref,
    cv_ref,
    nq_ref,
    nk_ref,
    nv_ref,
    cq_hbm,
    sk_ref,
    sv_ref,
    start_hbm,
    prefix_hbm,
    length_hbm,
    out_ref,
    cont_ref,
    kv,
    q,
    sk,
    sv,
    rows16,
    limit,
    row_max,
    row_sum,
    acc,
    cq_ref,
    start_ref,
    prefix_ref,
    length_ref,
    local_sem,
    query_sem,
    suffix_sem,
    recv_sem,
    pair_sem,
    send_sem,
    small_sem,
):
    half = ck_ref.shape[0]
    prompt_rows = nq_ref.shape[0]
    conts = cq_hbm.shape[0]
    suffix_rows = sk_ref.shape[1]
    many = GROUP * prompt_rows
    total = many + GROUP * conts
    me = lax.axis_index("ctx")
    core = me % CORES
    chip = me // CORES
    y = chip % n_y
    z = chip // n_y

    def device(zz, yy, cc):
        return (zz * n_y + yy) * CORES + cc

    own = []
    for p, ref in enumerate((ck_ref, nk_ref, cv_ref, nv_ref)):
        copy = pltpu.make_async_copy(
            ref, kv.at[me, p // 2, pl.ds((p % 2) * half, half)], local_sem.at[p]
        )
        copy.start()
        own.append(copy)
    for h in range(KVH):
        for g in range(GROUP):
            pltpu.make_async_copy(
                nq_ref.at[:, pl.ds((h * GROUP + g) * HD, HD)],
                q.at[h, pl.ds(g * prompt_rows, prompt_rows)],
                query_sem,
            ).start()
    suffix_copies = [
        pltpu.make_async_copy(sk_ref, sk, suffix_sem.at[0]),
        pltpu.make_async_copy(sv_ref, sv, suffix_sem.at[1]),
    ]
    small_copies = [
        pltpu.make_async_copy(src, dst, small_sem.at[i])
        for i, (src, dst) in enumerate(
            (
                (cq_hbm, cq_ref),
                (start_hbm, start_ref),
                (prefix_hbm, prefix_ref),
                (length_hbm, length_ref),
            )
        )
    ]
    for copy in suffix_copies + small_copies:
        copy.start()

    barrier = pltpu.get_barrier_semaphore()

    def greet(target):
        pl.semaphore_signal(barrier, inc=1, device_id={"ctx": target}, device_id_type=MESH)

    greet(device(z, y, 1 - core))
    if n_y == 2:
        greet(device(z, 1 - y, core))

    @pl.when(z > 0)
    def _():
        greet(device(z - 1, y, core))

    @pl.when(z < n_z - 1)
    def _():
        greet(device(z + 1, y, core))

    line_neighbours = (z + n_z - 1) // n_z + (2 * n_z - 2 - z) // n_z
    pl.semaphore_wait(barrier, n_y + line_neighbours)

    def piece(source, p):
        return kv.at[source, p // 2, pl.ds((p % 2) * half, half)]

    def send(source, p, target, kind):
        ref = piece(source, p)
        sem = pair_sem.at[source] if kind == 2 else recv_sem.at[source, p]
        pltpu.make_async_remote_copy(
            src_ref=ref,
            dst_ref=ref,
            send_sem=send_sem.at[source, kind],
            recv_sem=sem,
            device_id={"ctx": target},
            device_id_type=MESH,
        ).start()

    def arrived(source, p):
        ref = piece(source, p)
        pltpu.make_async_copy(ref, ref, recv_sem.at[source, p]).wait()

    def pair_arrived(source):
        pltpu.make_async_copy(kv.at[source], kv.at[source], pair_sem.at[source]).wait()

    def sent(source, kind, pieces=PIECES):
        ref = kv.at[source]
        if pieces == 1:
            ref = piece(source, EXTRA)
        elif pieces < PIECES:
            ref = kv.at[source, :, pl.ds(0, pieces * half // 2)]
        pltpu.make_async_copy(ref, ref, send_sem.at[source, kind]).wait()

    def by_line(zs):
        return ((zs < z) & (zs < n_z - 2)) | ((zs > z) & (zs > 1))

    def not_by_line(zs):
        return ((zs < z) & (zs >= n_z - 2)) | ((zs > z) & (zs <= 1)) | (zs == z)

    partner = device(z, y, 1 - core)
    across = device(z, 1 - y, core)
    above = device(z + 1, y, core)
    below = device(z - 1, y, core)

    for p in ORDER:
        own[p].wait()

        @pl.when(z < n_z - 1)
        def _():
            send(me, p, above, 0)

        if n_y == 2:
            send(me, p, across, 4 if p == EXTRA else 1)

        @pl.when(z > 0)
        def _():
            send(me, p, below, 3)

        send(me, p, partner, 2)

    near = jnp.minimum(z, n_z - 1 - z)

    def z_at(t):
        if isinstance(t, int) and t == 0:
            return z
        step = (t + 1) // 2
        both = z + step * (1 - 2 * (t % 2))
        far = jnp.where(z + z < n_z - 1, t, n_z - 1 - t)
        return jnp.where(t <= 2 * near, both, far)

    row = lax.broadcasted_iota(jnp.int32, (total, HD), 0)
    limit[...] = jnp.where(row < many, me * prompt_rows + row % prompt_rows, HIDDEN - 1)
    row_max[...] = jnp.full_like(row_max, -1e30)
    row_sum[...] = jnp.zeros_like(row_sum)
    acc[...] = jnp.zeros_like(acc)
    for copy in small_copies:
        copy.wait()
    for h in range(KVH):
        for g in range(GROUP):
            column = (h * GROUP + g) * HD
            rows16[h, g * conts : (g + 1) * conts, :] = cq_ref[:, column : column + HD].astype(
                jnp.float32
            )
    q[:, many:, :] = rows16[...].astype(jnp.bfloat16)

    for copy in suffix_copies:
        copy.wait()
    for h in range(KVH):
        keys = sk[:, :, h * HD : (h + 1) * HD].reshape(conts * suffix_rows, HD)
        values = sv[:, :, h * HD : (h + 1) * HD].reshape(conts * suffix_rows, HD)
        s = lax.dot_general(
            q[h, many:, :], keys, (((1,), (1,)), ((), ())), preferred_element_type=jnp.float32
        )
        who = lax.broadcasted_iota(jnp.int32, s.shape, 0) % conts
        column = lax.broadcasted_iota(jnp.int32, s.shape, 1)
        reach = jnp.zeros_like(who)
        for c in range(conts):
            reach = jnp.where(who == c, length_ref[c], reach)
        seen = (column // suffix_rows == who) & (column % suffix_rows < reach)
        s = jnp.where(seen, s * SCALE2, -1e30)
        top = jnp.max(s, axis=1, keepdims=True)
        w = jnp.exp2(s - top)
        row_max[h, many:, :] = jnp.broadcast_to(top, (GROUP * conts, HD))
        folded = w[:, :HD]
        for b in range(1, s.shape[1] // HD):
            folded = folded + w[:, b * HD : (b + 1) * HD]
        row_sum[h, many:, :] = folded
        acc[h, many:, :] = jnp.dot(
            w.astype(jnp.bfloat16), values, preferred_element_type=jnp.float32
        )

    span = CORES * 2 * half
    window_first = start_ref[0]
    prefix_last = prefix_ref[0]

    def places(chip_index):
        column = lax.broadcasted_iota(jnp.int32, (1, span), 1)
        within = column % (2 * half)
        position = (chip_index * CORES + column // (2 * half)) * half + within % half
        cached = jnp.where(
            (position >= window_first) & (position < prefix_last), -1, HIDDEN
        )
        return jnp.where(within < half, cached, position)

    def attend(h, chips, marks):
        cols = slice(h * HD, (h + 1) * HD)
        keys = [kv[pl.ds(c * CORES, CORES), 0, :, cols].reshape(span, HD) for c in chips]
        values = [kv[pl.ds(c * CORES, CORES), 1, :, cols].reshape(span, HD) for c in chips]
        keys = jnp.concatenate(keys, axis=0)
        values = jnp.concatenate(values, axis=0)
        mark = jnp.concatenate(marks, axis=1)
        count = span * len(chips)
        cut = (total // 2 + 15) // 16 * 16
        for lo, hi in ((0, cut), (cut, total)):
            s = lax.dot_general(
                q[h, lo:hi, :], keys, (((1,), (1,)), ((), ())), preferred_element_type=jnp.float32
            )
            bound = limit[lo:hi, :]
            blocks = []
            for b in range(count // HD):
                part = slice(b * HD, (b + 1) * HD)
                blocks.append(jnp.where(mark[:, part] <= bound, s[:, part] * SCALE2, -1e30))
            peak = functools.reduce(jnp.maximum, blocks)
            old = row_max[h, lo:hi, :]
            new = jnp.maximum(old, jnp.max(peak, axis=1, keepdims=True))
            alpha = jnp.exp2(old - new)
            w = [jnp.exp2(b - new) for b in blocks]
            row_max[h, lo:hi, :] = new
            row_sum[h, lo:hi, :] = row_sum[h, lo:hi, :] * alpha + functools.reduce(jnp.add, w)
            wb = jnp.concatenate([b.astype(jnp.bfloat16) for b in w], axis=1)
            acc[h, lo:hi, :] = acc[h, lo:hi, :] * alpha + jnp.dot(
                wb, values, preferred_element_type=jnp.float32
            )

    def onward(source, zs, p):
        @pl.when((zs < z) & (z < n_z - 1))
        def _():
            send(source, p, above, 0)

        @pl.when((zs > z) & (z > 0))
        def _():
            send(source, p, below, 0)

    def receive_z(zs, p):
        source = device(zs, y, core)
        arrived(source, p)
        onward(source, zs, p)
        if n_y == 2 and p == EXTRA:

            @pl.when(not_by_line(zs))
            def _():
                send(source, p, across, 4)

        elif n_y == 2:
            send(source, p, across, 1)
        send(source, p, partner, 2)

    def receive_extra(zs):
        @pl.when(by_line(zs))
        def _():
            source = device(zs, 1 - y, core)
            arrived(source, EXTRA)
            onward(source, zs, EXTRA)
            send(source, EXTRA, partner, 2)

    def receive_far(d):
        low = z - d

        @pl.when(low >= 0)
        def _():
            pltpu.make_async_copy(far_cq.at[low], far_cq.at[low], far_recv.at[low]).wait()

            @pl.when(z < last)
            def _():
                far_copy(low, above).start()

    def receive_line(d, i):
        for zs, inside in ((z - d, z - d >= 0), (z + d, z + d < n_z)):

            @pl.when(inside)
            def _():
                receive_z(zs, ORDER[i])
                if n_y == 2 and i == PIECES - 1:
                    receive_extra(zs)

    def receive_y(zs, i):
        source = device(zs, 1 - y, core)
        p = ORDER[i]

        def take():
            arrived(source, p)
            send(source, p, partner, 2)

        if p == EXTRA:
            pl.when(not_by_line(zs))(take)
        else:
            take()

    def receive_pair(i):
        receive_y(z, i)
        if ORDER[i] == EXTRA:
            source = device(z, 1 - y, core)

            @pl.when(z < n_z - 2)
            def _():
                send(source, EXTRA, above, 0)

            @pl.when(z > 1)
            def _():
                send(source, EXTRA, below, 3)

    pltpu.make_async_copy(q.at[:, pl.ds(0, many)], q.at[:, pl.ds(0, many)], query_sem).wait()
    pair_arrived(partner)
    mark = places(chip)
    for h in range(KVH):
        attend(h, [chip], [mark])
        receive_line(1, h)
        if n_y == 2:
            receive_pair(h)

    def step(t, carry):
        zs, zb = z_at(t), z_at(t - 1)
        pair_arrived(device(zs, y, 1 - core))
        chips = [zs * n_y + y]
        if n_y == 2:
            pair_arrived(device(zb, 1 - y, 1 - core))
            chips.append(zb * n_y + 1 - y)
        marks = [places(c) for c in chips]
        for h in range(KVH):
            attend(h, chips, marks)

            @pl.when(t < n_z - 1)
            def _():
                receive_line(t + 1, h)

            if n_y == 2:
                receive_y(zs, h)
        return carry

    lax.fori_loop(1, n_z, step, 0)
    chips = []
    if n_y == 2:
        zb = z_at(jnp.int32(n_z - 1))
        pair_arrived(device(zb, 1 - y, 1 - core))
        chips = [zb * n_y + 1 - y]
    marks = [places(c) for c in chips]
    for h in range(KVH):
        if n_y == 2:
            attend(h, chips, marks)
        mixed = acc[h] / jnp.sum(row_sum[h], axis=1, keepdims=True)
        for g in range(GROUP):
            column = (h * GROUP + g) * HD
            out_ref[:, column : column + HD] = mixed[
                g * prompt_rows : (g + 1) * prompt_rows, :
            ].astype(jnp.bfloat16)
        rows16[h] = mixed[many:, :]
        for g in range(GROUP):
            column = (h * GROUP + g) * HD
            cont_ref[:, column : column + HD] = rows16[
                h, g * conts : (g + 1) * conts, :
            ].astype(jnp.bfloat16)

    @pl.when(z < n_z - 1)
    def _():
        sent(me, 0)

    @pl.when(z > 0)
    def _():
        sent(me, 3)

    sent(me, 2)
    if n_y == 2:
        pair = device(z, 1 - y, core)
        sent(me, 1, PIECES - 1)
        sent(me, 4, 1)

        @pl.when(z < n_z - 2)
        def _():
            sent(pair, 0, 1)

        @pl.when(z > 1)
        def _():
            sent(pair, 3, 1)

    def drain(zs, carry):
        source = device(zs, y, core)
        middle = ((zs < z) & (z < n_z - 1)) | ((zs > z) & (z > 0))

        @pl.when(middle)
        def _():
            sent(source, 0)

        @pl.when(zs != z)
        def _():
            if n_y == 2:
                sent(source, 1, PIECES - 1)
            sent(source, 2)

        if n_y == 2:
            other = device(zs, 1 - y, core)

            @pl.when((zs != z) & not_by_line(zs))
            def _():
                sent(source, 4, 1)

            @pl.when(middle & by_line(zs))
            def _():
                sent(other, 0, len(BY_LINE))

            sent(other, 2)
        return carry

    lax.fori_loop(0, n_z, drain, 0)


HEADS = (0, 1, 2, 3)
BY_LINE = (3,)
LEAD = 2
AHEAD = 2


def pack_rows(values):
    lane = lax.broadcasted_iota(jnp.int32, (8, HD), 1)
    tile = jnp.zeros((8, HD), jnp.float32)
    for i in range(values.shape[0] // 8):
        tile = jnp.where(lane == i, values[8 * i : 8 * i + 8, :], tile)
    return tile


def unpack_rows(tile, first, count):
    lane = lax.broadcasted_iota(jnp.int32, (8, HD), 1)
    blocks = [
        jnp.max(jnp.where(lane == i, tile, -3e38), axis=1, keepdims=True)
        for i in range(first // 8, (first + count) // 8)
    ]
    return jnp.concatenate(blocks, axis=0)


def plane_kernel(
    n_z,
    ck_ref,
    cv_ref,
    nq_ref,
    nk_ref,
    nv_ref,
    cq_hbm,
    sk_ref,
    sv_ref,
    start_hbm,
    prefix_hbm,
    length_hbm,
    out_ref,
    cont_ref,
    kv,
    q,
    sk,
    sv,
    rows16,
    limit,
    row_max,
    row_sum,
    acc,
    cq,
    far_cq,
    far_rows,
    part_out,
    part_in,
    lse_out,
    lse_in,
    start_ref,
    prefix_ref,
    length_ref,
    local_sem,
    query_sem,
    suffix_sem,
    small_sem,
    recv_sem,
    send_sem,
    far_recv,
    far_send,
    part_recv,
    part_send,
):
    n_y = 2
    half = ck_ref.shape[0]
    prompt_rows = nq_ref.shape[0]
    conts = cq_hbm.shape[0]
    suffix_rows = sk_ref.shape[1]
    many = GROUP * prompt_rows
    few = GROUP * conts
    total = many + few
    me = lax.axis_index("ctx")
    core = me % CORES
    chip = me // CORES
    y = chip % n_y
    z = chip // n_y
    last = n_z - 1
    lines = n_z - 2
    plane = n_y * CORES
    span = plane * half

    def device(zz, yy, cc):
        return (zz * n_y + yy) * CORES + cc

    partner = device(z, y, 1 - core)
    across = device(z, 1 - y, core)
    above = device(z + 1, y, core)
    below = device(z - 1, y, core)

    barrier = pltpu.get_barrier_semaphore()

    def greet(target):
        pl.semaphore_signal(barrier, inc=1, device_id={"ctx": target}, device_id_type=MESH)

    greet(partner)
    greet(across)

    @pl.when(z > 0)
    def _():
        greet(below)

    @pl.when(z < last)
    def _():
        greet(above)

    for h in HEADS:
        cols = pl.ds(h * HD, HD)
        for kind, pair in enumerate(((ck_ref, cv_ref), (nk_ref, nv_ref))):
            for i, ref in enumerate(pair):
                pltpu.make_async_copy(ref.at[:, cols], kv.at[me, h, kind, i], local_sem.at[h]).start()
    small = [
        pltpu.make_async_copy(src, dst, small_sem.at[i])
        for i, (src, dst) in enumerate(
            (
                (cq_hbm, cq),
                (start_hbm, start_ref),
                (prefix_hbm, prefix_ref),
                (length_hbm, length_ref),
            )
        )
    ]
    for copy in small:
        copy.start()
    suffix_copies = [
        pltpu.make_async_copy(sk_ref, sk, suffix_sem.at[0]),
        pltpu.make_async_copy(sv_ref, sv, suffix_sem.at[1]),
    ]
    for copy in suffix_copies:
        copy.start()

    line_neighbours = (z + n_z - 1) // n_z + (2 * n_z - 2 - z) // n_z
    pl.semaphore_wait(barrier, n_y + line_neighbours)

    def full(source, h):
        return kv.at[source, h]

    def cached(source, h):
        return kv.at[source, h, 0]

    def send(ref, source, h, target, kind):
        pltpu.make_async_remote_copy(
            src_ref=ref,
            dst_ref=ref,
            send_sem=send_sem.at[source, kind],
            recv_sem=recv_sem.at[source, h],
            device_id={"ctx": target},
            device_id_type=MESH,
        ).start()

    def arrived(ref, source, h):
        pltpu.make_async_copy(ref, ref, recv_sem.at[source, h]).wait()

    def far_copy(zs, target):
        return pltpu.make_async_remote_copy(
            src_ref=far_cq.at[zs],
            dst_ref=far_cq.at[zs],
            send_sem=far_send.at[zs],
            recv_sem=far_recv.at[zs],
            device_id={"ctx": target},
            device_id_type=MESH,
        )

    small[0].wait()

    @pl.when(z < last)
    def _():
        pltpu.make_async_remote_copy(
            src_ref=cq,
            dst_ref=far_cq.at[z],
            send_sem=far_send.at[z],
            recv_sem=far_recv.at[z],
            device_id={"ctx": above},
            device_id_type=MESH,
        ).start()

    for h in HEADS:
        pltpu.make_async_copy(full(me, h), full(me, h), local_sem.at[h]).wait()

        @pl.when(z < last)
        def _():
            send(full(me, h), me, h, above, 0)

        send(full(me, h), me, h, across, 1)

        @pl.when(z > 0)
        def _():
            send(cached(me, h), me, h, below, 3)

        send(full(me, h), me, h, partner, 2)

    for h in HEADS:
        for g in range(GROUP):
            pltpu.make_async_copy(
                nq_ref.at[:, pl.ds((h * GROUP + g) * HD, HD)],
                q.at[h, pl.ds(g * prompt_rows, prompt_rows)],
                query_sem,
            ).start()
    near = jnp.minimum(z, last - z)

    def z_at(t):
        step = (t + 1) // 2
        both = z + step * (1 - 2 * (t % 2))
        far = jnp.where(z + z < last, t, last - t)
        return jnp.where(t <= 2 * near, both, far)

    row = lax.broadcasted_iota(jnp.int32, (total, HD), 0)
    limit[...] = jnp.where(row < many, (me % plane) * prompt_rows + row % prompt_rows, HIDDEN)
    row_max[...] = jnp.full_like(row_max, -1e30)
    row_sum[...] = jnp.zeros_like(row_sum)
    acc[...] = jnp.zeros_like(acc)

    def spread(rows):
        for h in range(KVH):
            for g in range(GROUP):
                column = (h * GROUP + g) * HD
                rows16[h, g * conts : (g + 1) * conts, :] = rows[:, column : column + HD].astype(
                    jnp.float32
                )

    for zs in range(last):

        @pl.when(zs >= z)
        def _():
            far_cq[zs] = jnp.zeros(far_cq.shape[1:], jnp.bfloat16)

    spread(cq)
    q[:, many:, :] = rows16[...].astype(jnp.bfloat16)
    for copy in small[1:]:
        copy.wait()
    for copy in suffix_copies:
        copy.wait()
    for h in range(KVH):
        keys = sk[:, :, h * HD : (h + 1) * HD].reshape(conts * suffix_rows, HD)
        values = sv[:, :, h * HD : (h + 1) * HD].reshape(conts * suffix_rows, HD)
        s = lax.dot_general(
            q[h, many:, :], keys, (((1,), (1,)), ((), ())), preferred_element_type=jnp.float32
        )
        who = lax.broadcasted_iota(jnp.int32, s.shape, 0) % conts
        column = lax.broadcasted_iota(jnp.int32, s.shape, 1)
        reach = jnp.zeros_like(who)
        for c in range(conts):
            reach = jnp.where(who == c, length_ref[c], reach)
        seen = (column // suffix_rows == who) & (column % suffix_rows < reach)
        s = jnp.where(seen, s * SCALE2, -1e30)
        top = jnp.max(s, axis=1, keepdims=True)
        w = jnp.exp2(s - top)
        row_max[h, many:, :] = jnp.broadcast_to(top, (few, HD))
        row_sum[h, many:, :] = jnp.broadcast_to(jnp.sum(w, axis=1, keepdims=True), (few, HD))
        acc[h, many:, :] = jnp.dot(
            w.astype(jnp.bfloat16), values, preferred_element_type=jnp.float32
        )

    window_first = start_ref[0]
    prefix_last = prefix_ref[0]

    def cache_bias(zs):
        position = zs * span + lax.broadcasted_iota(jnp.int32, (1, span), 1)
        return jnp.where((position >= window_first) & (position < prefix_last), 0.0, -1e30)

    def plane_rows(zs, h, kind, i):
        return kv[pl.ds(zs * plane, plane), h, kind, i].reshape(span, HD)

    def summed(values):
        return jnp.concatenate([values, jnp.ones(values.shape, jnp.bfloat16)], axis=1)

    def attend(h, zs, mode, bias):
        keys = plane_rows(zs, h, 0, 0)
        values = plane_rows(zs, h, 0, 1)
        if mode != "cache":
            keys = jnp.concatenate([keys, plane_rows(zs, h, 1, 0)], axis=0)
            values = jnp.concatenate([values, plane_rows(zs, h, 1, 1)], axis=0)
        values = summed(values)
        cut = (total // 2 + 15) // 16 * 16
        for lo, hi in ((0, cut), (cut, total)):
            s = lax.dot_general(
                q[h, lo:hi, :], keys, (((1,), (1,)), ((), ())), preferred_element_type=jnp.float32
            )
            blocks = []
            for b in range(keys.shape[0] // HD):
                part = s[:, b * HD : (b + 1) * HD] * SCALE2
                if b < span // HD:
                    part = part + bias[:, b * HD : (b + 1) * HD]
                elif mode == "own":
                    at = (b - span // HD) * HD + lax.broadcasted_iota(jnp.int32, (1, HD), 1)
                    part = jnp.where(at <= limit[lo:hi, :], part, -1e30)
                blocks.append(part)
            peak = functools.reduce(jnp.maximum, blocks)
            old = row_max[h, lo:hi, :]
            new = jnp.maximum(old, jnp.max(peak, axis=1, keepdims=True))
            alpha = jnp.exp2(old - new)
            w = [jnp.exp2(b - new) for b in blocks]
            row_max[h, lo:hi, :] = new
            wb = jnp.concatenate([b.astype(jnp.bfloat16) for b in w], axis=1)
            mixed = jnp.dot(wb, values, preferred_element_type=jnp.float32)
            acc[h, lo:hi, :] = acc[h, lo:hi, :] * alpha + mixed[:, :HD]
            row_sum[h, lo:hi, :] = row_sum[h, lo:hi, :] * alpha + mixed[:, HD:]

    def foreign():
        for zs in range(last):
            rows = far_cq.at[zs]
            for h in range(KVH):
                for g in range(GROUP):
                    column = (h * GROUP + g) * HD
                    first = zs * few + g * conts
                    far_rows[h, first : first + conts, :] = rows[:, column : column + HD].astype(
                        jnp.float32
                    )
        sums = []
        for h in range(KVH):
            s = lax.dot_general(
                far_rows[h].astype(jnp.bfloat16),
                plane_rows(z, h, 1, 0),
                (((1,), (1,)), ((), ())),
                preferred_element_type=jnp.float32,
            )
            s = s * SCALE2
            top = jnp.max(s, axis=1, keepdims=True)
            w = jnp.exp2(s - top)
            both = jnp.dot(
                w.astype(jnp.bfloat16),
                summed(plane_rows(z, h, 1, 1)),
                preferred_element_type=jnp.float32,
            )
            under = both[:, HD:]
            mixed = both[:, :HD] / under
            for zs in range(last):
                part_out[zs, h * few : (h + 1) * few, :] = mixed[zs * few : (zs + 1) * few, :]
            sums.append(top + jnp.log2(under))
        for zs in range(last):
            lse_out[zs] = pack_rows(
                jnp.concatenate([level[zs * few : (zs + 1) * few, :] for level in sums], axis=0)
            )

    def part_copies(zs):
        return [
            pltpu.make_async_remote_copy(
                src_ref=src.at[zs],
                dst_ref=dst.at[z],
                send_sem=part_send.at[zs, i],
                recv_sem=part_recv.at[z, i],
                device_id={"ctx": device(zs, y, core)},
                device_id_type=MESH,
            )
            for i, (src, dst) in enumerate(((part_out, part_in), (lse_out, lse_in)))
        ]

    def merge(zs):
        for i, ref in enumerate((part_in, lse_in)):
            pltpu.make_async_copy(ref.at[zs], ref.at[zs], part_recv.at[zs, i]).wait()
        tile = lse_in[zs]
        for h in range(KVH):
            level = unpack_rows(tile, h * few, few)
            old = row_max[h, many:, :]
            new = jnp.maximum(old, level)
            alpha = jnp.exp2(old - new)
            beta = jnp.exp2(level - new)
            row_max[h, many:, :] = new
            row_sum[h, many:, :] = row_sum[h, many:, :] * alpha + beta
            acc[h, many:, :] = (
                acc[h, many:, :] * alpha + part_in[zs, h * few : (h + 1) * few, :] * beta
            )

    def receive_far(d):
        low = z - d

        @pl.when(low >= 0)
        def _():
            pltpu.make_async_copy(far_cq.at[low], far_cq.at[low], far_recv.at[low]).wait()

            @pl.when(z < last)
            def _():
                far_copy(low, above).start()

    def receive_line(d, i):
        h = HEADS[i]
        low, high = z - d, z + d

        @pl.when(low >= 0)
        def _():
            source = device(low, y, core)
            ref = full(source, h)
            arrived(ref, source, h)

            @pl.when(z < last)
            def _():
                send(ref, source, h, above, 0)

            if h in BY_LINE:

                @pl.when(low >= lines)
                def _():
                    send(ref, source, h, across, 1)

            else:
                send(ref, source, h, across, 1)
            send(ref, source, h, partner, 2)
        @pl.when(high < n_z)
        def _():
            source = device(high, y, core)
            ref = cached(source, h)
            arrived(ref, source, h)

            @pl.when(z > 0)
            def _():
                send(ref, source, h, below, 0)

            send(ref, source, h, across, 1)
            send(ref, source, h, partner, 2)

    def receive_y(zs, i):
        h = HEADS[i]
        source = device(zs, 1 - y, core)

        def take(ref):
            arrived(ref, source, h)
            send(ref, source, h, partner, 2)

        pl.when(zs <= z)(lambda: take(full(source, h)))
        if h in BY_LINE:
            pl.when((zs < lines) & (zs < z) & (z < last))(
                lambda: send(full(source, h), source, h, above, 0)
            )
        pl.when(zs > z)(lambda: take(cached(source, h)))

    def receive_own(i):
        h = HEADS[i]
        arrived(full(across, h), across, h)
        send(full(across, h), across, h, partner, 2)
        if h in BY_LINE:

            @pl.when((z < last) & (z < lines))
            def _():
                send(full(across, h), across, h, above, 0)

    def pair_arrived(zs, i):
        h = HEADS[i]
        for yy in (y, 1 - y):
            source = device(zs, yy, 1 - core)
            pl.when(zs <= z)(lambda source=source: arrived(full(source, h), source, h))
            pl.when(zs > z)(lambda source=source: arrived(cached(source, h), source, h))

    pltpu.make_async_copy(
        q.at[pl.ds(0, KVH), pl.ds(0, many)], q.at[pl.ds(0, KVH), pl.ds(0, many)], query_sem
    ).wait()
    def receive(t, i):
        q, r = divmod(i + AHEAD - 1, KVH)
        receive_line(t + 1 + q, r)
        q, r = divmod(i + LEAD, KVH)
        if isinstance(t, int):
            receive_own(r) if t + q == 0 else receive_y(z_at(t + q), r)
        else:
            pl.when(t + q < n_z)(lambda: receive_y(z_at(t + q), r))

    def give(zs):
        for copy in part_copies(zs):
            copy.start()

    for j in range(AHEAD - 1):
        receive_line(1 + j // KVH, j % KVH)
    for j in range(LEAD):
        receive_own(j)
    bias = cache_bias(z)
    for i, h in enumerate(HEADS):
        receive(0, i)
        for yy in (y, 1 - y):
            source = device(z, yy, 1 - core)
            arrived(full(source, h), source, h)
        attend(h, z, "own", bias)
        if i == 0:
            receive_far(1)

    receive_far(2)

    def step(t, carry):
        zs = z_at(t)
        bias = cache_bias(zs)
        for i, h in enumerate(HEADS):
            receive(t, i)
            pair_arrived(zs, i)
            pl.when(zs < z)(lambda: attend(h, zs, "all", bias))
            pl.when(zs > z)(lambda: attend(h, zs, "cache", bias))
            if i > 0:

                @pl.when((t == 1) & (z > 0))
                def _():
                    if i == 1:
                        for d in range(3, n_z):
                            receive_far(d)
                    if i == 2:
                        foreign()
                    if i == 3:
                        for d in range(1, n_z):
                            pl.when(z >= d)(lambda: give(z - d))

        return carry

    lax.fori_loop(1, n_z, step, 0)

    def collect(zs, carry):
        merge(zs)
        return carry

    lax.fori_loop(z + 1, n_z, collect, 0)
    for h in range(KVH):
        mixed = acc[h] / row_sum[h]
        for g in range(GROUP):
            column = (h * GROUP + g) * HD
            out_ref[:, column : column + HD] = mixed[
                g * prompt_rows : (g + 1) * prompt_rows, :
            ].astype(jnp.bfloat16)
        rows16[h] = mixed[many:, :]
        for g in range(GROUP):
            column = (h * GROUP + g) * HD
            cont_ref[:, column : column + HD] = rows16[
                h, g * conts : (g + 1) * conts, :
            ].astype(jnp.bfloat16)

    def sent(source, kind, count, cache_only=False):
        ref = kv.at[source, pl.ds(0, count)]
        if cache_only:
            ref = kv.at[source, pl.ds(0, count), 0]
        pltpu.make_async_copy(ref, ref, send_sem.at[source, kind]).wait()

    @pl.when(z < last)
    def _():
        sent(me, 0, KVH)
        pltpu.make_async_copy(cq, cq, far_send.at[z]).wait()

    @pl.when(z > 0)
    def _():
        sent(me, 3, KVH, True)

    sent(me, 1, KVH)
    sent(me, 2, KVH)

    def drain(zs, carry):
        source = device(zs, y, core)
        other = device(zs, 1 - y, core)

        @pl.when(zs < z)
        def _():
            @pl.when(z < last)
            def _():
                sent(source, 0, KVH)
                pltpu.make_async_copy(far_cq.at[zs], far_cq.at[zs], far_send.at[zs]).wait()

            pl.when(zs < lines)(lambda: sent(source, 1, KVH - len(BY_LINE)))
            pl.when(zs >= lines)(lambda: sent(source, 1, KVH))
            sent(source, 2, KVH)
            for copy in part_copies(zs):
                copy.wait_send()

        @pl.when(zs > z)
        def _():
            pl.when(z > 0)(lambda: sent(source, 0, KVH, True))
            sent(source, 1, KVH, True)
            sent(source, 2, KVH, True)
            sent(other, 2, KVH, True)

        @pl.when(zs <= z)
        def _():
            sent(other, 2, KVH)
            pl.when((z < last) & (zs < lines))(lambda: sent(other, 0, len(BY_LINE)))

        return carry

    lax.fori_loop(0, n_z, drain, 0)


def line_shape(mesh):
    chips = mesh.shape["ctx"] // CORES
    place = mesh.axis_names.index("ctx")
    index = [0] * mesh.devices.ndim
    index[place] = slice(None)
    coords = [getattr(d, "coords", None) for d in mesh.devices[tuple(index)]]
    n_y = 1
    if all(c is not None for c in coords) and len({c[1] for c in coords}) == 2:
        n_y = 2
    return chips // n_y, n_y


def solution(mesh):
    n_z, n_y = line_shape(mesh)
    n_ctx = mesh.shape["ctx"]

    def plane_body(ck, cv, nq, nk, nv, cq, sk, sv, ws, pfx, length):
        half = ck.shape[0]
        few = GROUP * cq.shape[0]
        total = GROUP * nq.shape[0] + few
        anywhere = pl.BlockSpec(memory_space=pl.ANY)
        vmem = pl.BlockSpec(memory_space=pltpu.VMEM)
        state = pltpu.VMEM((KVH, total, HD), jnp.float32)
        part = pltpu.VMEM((n_z, KVH * few, HD), jnp.float32)
        levels = pltpu.VMEM((n_z, 8, HD), jnp.float32)
        return pl.pallas_call(
            functools.partial(plane_kernel, n_z),
            out_shape=(
                pltpu.VMEM(nq.shape, jnp.bfloat16),
                pltpu.VMEM(cq.shape, jnp.bfloat16),
            ),
            in_specs=[anywhere] * 11,
            out_specs=(vmem, vmem),
            scratch_shapes=[
                pltpu.VMEM((n_ctx, KVH, 2, 2, half, HD), jnp.bfloat16),
                pltpu.VMEM((KVH, total, HD), jnp.bfloat16),
                pltpu.VMEM(sk.shape, jnp.bfloat16),
                pltpu.VMEM(sv.shape, jnp.bfloat16),
                pltpu.VMEM((KVH, few, HD), jnp.float32),
                pltpu.VMEM((total, HD), jnp.int32),
                state,
                state,
                state,
                pltpu.VMEM(cq.shape, jnp.bfloat16),
                pltpu.VMEM((n_z,) + cq.shape, jnp.bfloat16),
                pltpu.VMEM((KVH, few * (n_z - 1), HD), jnp.float32),
                part,
                part,
                levels,
                levels,
                pltpu.SMEM(ws.shape, jnp.int32),
                pltpu.SMEM(pfx.shape, jnp.int32),
                pltpu.SMEM(length.shape, jnp.int32),
                pltpu.SemaphoreType.DMA((KVH,)),
                pltpu.SemaphoreType.DMA,
                pltpu.SemaphoreType.DMA((2,)),
                pltpu.SemaphoreType.DMA((4,)),
                pltpu.SemaphoreType.DMA((n_ctx, KVH)),
                pltpu.SemaphoreType.DMA((n_ctx, 4)),
                pltpu.SemaphoreType.DMA((n_z,)),
                pltpu.SemaphoreType.DMA((n_z,)),
                pltpu.SemaphoreType.DMA((n_z, 2)),
                pltpu.SemaphoreType.DMA((n_z, 2)),
            ],
            compiler_params=pltpu.CompilerParams(
                collective_id=0, has_side_effects=True, vmem_limit_bytes=60 * 1024 * 1024
            ),
        )(ck, cv, nq, nk, nv, cq, sk, sv, ws, pfx, length)

    def body(ck, cv, nq, nk, nv, cq, sk, sv, ws, pfx, length):
        half, width = ck.shape
        rows = nq.shape[0]
        conts = cq.shape[0]
        total = GROUP * (rows + conts)
        anywhere = pl.BlockSpec(memory_space=pl.ANY)
        vmem = pl.BlockSpec(memory_space=pltpu.VMEM)
        return pl.pallas_call(
            functools.partial(kernel, n_z, n_y),
            out_shape=(
                pltpu.VMEM(nq.shape, jnp.bfloat16),
                pltpu.VMEM(cq.shape, jnp.bfloat16),
            ),
            in_specs=[anywhere] * 11,
            out_specs=(vmem, vmem),
            scratch_shapes=[
                pltpu.VMEM((n_ctx, 2, 2 * half, width), jnp.bfloat16),
                pltpu.VMEM((KVH, total, HD), jnp.bfloat16),
                pltpu.VMEM(sk.shape, jnp.bfloat16),
                pltpu.VMEM(sv.shape, jnp.bfloat16),
                pltpu.VMEM((KVH, GROUP * conts, HD), jnp.float32),
                pltpu.VMEM((total, HD), jnp.int32),
                pltpu.VMEM((KVH, total, HD), jnp.float32),
                pltpu.VMEM((KVH, total, HD), jnp.float32),
                pltpu.VMEM((KVH, total, HD), jnp.float32),
                pltpu.VMEM(cq.shape, jnp.bfloat16),
                pltpu.SMEM(ws.shape, jnp.int32),
                pltpu.SMEM(pfx.shape, jnp.int32),
                pltpu.SMEM(length.shape, jnp.int32),
                pltpu.SemaphoreType.DMA((PIECES,)),
                pltpu.SemaphoreType.DMA,
                pltpu.SemaphoreType.DMA((2,)),
                pltpu.SemaphoreType.DMA((n_ctx, PIECES)),
                pltpu.SemaphoreType.DMA((n_ctx,)),
                pltpu.SemaphoreType.DMA((n_ctx, 5)),
                pltpu.SemaphoreType.DMA((4,)),
            ],
            compiler_params=pltpu.CompilerParams(
                collective_id=0, has_side_effects=True, vmem_limit_bytes=60 * 1024 * 1024
            ),
        )(ck, cv, nq, nk, nv, cq, sk, sv, ws, pfx, length)

    part = P(("grp", "ctx"), None)
    part3 = P(("grp", "ctx"), None, None)
    in_specs = (part,) * 6 + (part3, part3, P("grp"), P("grp"), P(("grp", "ctx")))
    return jax.shard_map(
        plane_body if n_y == 2 and n_z > 2 else body,
        mesh=mesh, in_specs=in_specs, out_specs=(part, part), check_vma=False
    )
```

```python
import functools
import math

import jax
import jax.numpy as jnp
from jax import lax
from jax.experimental import pallas as pl
from jax.experimental.pallas import tpu as pltpu
from jax.sharding import PartitionSpec as P

KVH = 4
HD = 128
GROUP = 8
CORES = 2
PIECES = 4
EXTRA = 3
ORDER = (EXTRA, 0, 1, 2)
MESH = pl.DeviceIdType.MESH
SCALE2 = HD ** (-0.5) * math.log2(math.e)
HIDDEN = 1 << 30


def kernel(
    n_z,
    n_y,
    ck_ref,
    cv_ref,
    nq_ref,
    nk_ref,
    nv_ref,
    cq_hbm,
    sk_ref,
    sv_ref,
    start_hbm,
    prefix_hbm,
    length_hbm,
    out_ref,
    cont_ref,
    kv,
    q,
    sk,
    sv,
    rows16,
    limit,
    row_max,
    row_sum,
    acc,
    cq_ref,
    start_ref,
    prefix_ref,
    length_ref,
    local_sem,
    query_sem,
    suffix_sem,
    recv_sem,
    pair_sem,
    send_sem,
    small_sem,
):
    half = ck_ref.shape[0]
    prompt_rows = nq_ref.shape[0]
    conts = cq_hbm.shape[0]
    suffix_rows = sk_ref.shape[1]
    many = GROUP * prompt_rows
    total = many + GROUP * conts
    me = lax.axis_index("ctx")
    core = me % CORES
    chip = me // CORES
    y = chip % n_y
    z = chip // n_y

    def device(zz, yy, cc):
        return (zz * n_y + yy) * CORES + cc

    own = []
    for p, ref in enumerate((ck_ref, nk_ref, cv_ref, nv_ref)):
        copy = pltpu.make_async_copy(
            ref, kv.at[me, p // 2, pl.ds((p % 2) * half, half)], local_sem.at[p]
        )
        copy.start()
        own.append(copy)
    for h in range(KVH):
        for g in range(GROUP):
            pltpu.make_async_copy(
                nq_ref.at[:, pl.ds((h * GROUP + g) * HD, HD)],
                q.at[h, pl.ds(g * prompt_rows, prompt_rows)],
                query_sem,
            ).start()
    suffix_copies = [
        pltpu.make_async_copy(sk_ref, sk, suffix_sem.at[0]),
        pltpu.make_async_copy(sv_ref, sv, suffix_sem.at[1]),
    ]
    small_copies = [
        pltpu.make_async_copy(src, dst, small_sem.at[i])
        for i, (src, dst) in enumerate(
            (
                (cq_hbm, cq_ref),
                (start_hbm, start_ref),
                (prefix_hbm, prefix_ref),
                (length_hbm, length_ref),
            )
        )
    ]
    for copy in suffix_copies + small_copies:
        copy.start()

    barrier = pltpu.get_barrier_semaphore()

    def greet(target):
        pl.semaphore_signal(barrier, inc=1, device_id={"ctx": target}, device_id_type=MESH)

    greet(device(z, y, 1 - core))
    if n_y == 2:
        greet(device(z, 1 - y, core))

    @pl.when(z > 0)
    def _():
        greet(device(z - 1, y, core))

    @pl.when(z < n_z - 1)
    def _():
        greet(device(z + 1, y, core))

    line_neighbours = (z + n_z - 1) // n_z + (2 * n_z - 2 - z) // n_z
    pl.semaphore_wait(barrier, n_y + line_neighbours)

    def piece(source, p):
        return kv.at[source, p // 2, pl.ds((p % 2) * half, half)]

    def send(source, p, target, kind):
        ref = piece(source, p)
        sem = pair_sem.at[source] if kind == 2 else recv_sem.at[source, p]
        pltpu.make_async_remote_copy(
            src_ref=ref,
            dst_ref=ref,
            send_sem=send_sem.at[source, kind],
            recv_sem=sem,
            device_id={"ctx": target},
            device_id_type=MESH,
        ).start()

    def arrived(source, p):
        ref = piece(source, p)
        pltpu.make_async_copy(ref, ref, recv_sem.at[source, p]).wait()

    def pair_arrived(source):
        pltpu.make_async_copy(kv.at[source], kv.at[source], pair_sem.at[source]).wait()

    def sent(source, kind, pieces=PIECES):
        ref = kv.at[source]
        if pieces == 1:
            ref = piece(source, EXTRA)
        elif pieces < PIECES:
            ref = kv.at[source, :, pl.ds(0, pieces * half // 2)]
        pltpu.make_async_copy(ref, ref, send_sem.at[source, kind]).wait()

    def by_line(zs):
        return ((zs < z) & (zs < n_z - 2)) | ((zs > z) & (zs > 1))

    def not_by_line(zs):
        return ((zs < z) & (zs >= n_z - 2)) | ((zs > z) & (zs <= 1)) | (zs == z)

    partner = device(z, y, 1 - core)
    across = device(z, 1 - y, core)
    above = device(z + 1, y, core)
    below = device(z - 1, y, core)

    for p in ORDER:
        own[p].wait()

        @pl.when(z < n_z - 1)
        def _():
            send(me, p, above, 0)

        if n_y == 2:
            send(me, p, across, 4 if p == EXTRA else 1)

        @pl.when(z > 0)
        def _():
            send(me, p, below, 3)

        send(me, p, partner, 2)

    near = jnp.minimum(z, n_z - 1 - z)

    def z_at(t):
        if isinstance(t, int) and t == 0:
            return z
        step = (t + 1) // 2
        both = z + step * (1 - 2 * (t % 2))
        far = jnp.where(z + z < n_z - 1, t, n_z - 1 - t)
        return jnp.where(t <= 2 * near, both, far)

    row = lax.broadcasted_iota(jnp.int32, (total, HD), 0)
    limit[...] = jnp.where(row < many, me * prompt_rows + row % prompt_rows, HIDDEN - 1)
    row_max[...] = jnp.full_like(row_max, -1e30)
    row_sum[...] = jnp.zeros_like(row_sum)
    acc[...] = jnp.zeros_like(acc)
    for copy in small_copies:
        copy.wait()
    for h in range(KVH):
        for g in range(GROUP):
            column = (h * GROUP + g) * HD
            rows16[h, g * conts : (g + 1) * conts, :] = cq_ref[:, column : column + HD].astype(
                jnp.float32
            )
    q[:, many:, :] = rows16[...].astype(jnp.bfloat16)

    for copy in suffix_copies:
        copy.wait()
    for h in range(KVH):
        keys = sk[:, :, h * HD : (h + 1) * HD].reshape(conts * suffix_rows, HD)
        values = sv[:, :, h * HD : (h + 1) * HD].reshape(conts * suffix_rows, HD)
        s = lax.dot_general(
            q[h, many:, :], keys, (((1,), (1,)), ((), ())), preferred_element_type=jnp.float32
        )
        who = lax.broadcasted_iota(jnp.int32, s.shape, 0) % conts
        column = lax.broadcasted_iota(jnp.int32, s.shape, 1)
        reach = jnp.zeros_like(who)
        for c in range(conts):
            reach = jnp.where(who == c, length_ref[c], reach)
        seen = (column // suffix_rows == who) & (column % suffix_rows < reach)
        s = jnp.where(seen, s * SCALE2, -1e30)
        top = jnp.max(s, axis=1, keepdims=True)
        w = jnp.exp2(s - top)
        row_max[h, many:, :] = jnp.broadcast_to(top, (GROUP * conts, HD))
        folded = w[:, :HD]
        for b in range(1, s.shape[1] // HD):
            folded = folded + w[:, b * HD : (b + 1) * HD]
        row_sum[h, many:, :] = folded
        acc[h, many:, :] = jnp.dot(
            w.astype(jnp.bfloat16), values, preferred_element_type=jnp.float32
        )

    span = CORES * 2 * half
    window_first = start_ref[0]
    prefix_last = prefix_ref[0]

    def places(chip_index):
        column = lax.broadcasted_iota(jnp.int32, (1, span), 1)
        within = column % (2 * half)
        position = (chip_index * CORES + column // (2 * half)) * half + within % half
        cached = jnp.where(
            (position >= window_first) & (position < prefix_last), -1, HIDDEN
        )
        return jnp.where(within < half, cached, position)

    def attend(h, chips, marks):
        cols = slice(h * HD, (h + 1) * HD)
        keys = [kv[pl.ds(c * CORES, CORES), 0, :, cols].reshape(span, HD) for c in chips]
        values = [kv[pl.ds(c * CORES, CORES), 1, :, cols].reshape(span, HD) for c in chips]
        keys = jnp.concatenate(keys, axis=0)
        values = jnp.concatenate(values, axis=0)
        mark = jnp.concatenate(marks, axis=1)
        count = span * len(chips)
        cut = (total // 2 + 15) // 16 * 16
        for lo, hi in ((0, cut), (cut, total)):
            s = lax.dot_general(
                q[h, lo:hi, :], keys, (((1,), (1,)), ((), ())), preferred_element_type=jnp.float32
            )
            bound = limit[lo:hi, :]
            blocks = []
            for b in range(count // HD):
                part = slice(b * HD, (b + 1) * HD)
                blocks.append(jnp.where(mark[:, part] <= bound, s[:, part] * SCALE2, -1e30))
            peak = functools.reduce(jnp.maximum, blocks)
            old = row_max[h, lo:hi, :]
            new = jnp.maximum(old, jnp.max(peak, axis=1, keepdims=True))
            alpha = jnp.exp2(old - new)
            w = [jnp.exp2(b - new) for b in blocks]
            row_max[h, lo:hi, :] = new
            row_sum[h, lo:hi, :] = row_sum[h, lo:hi, :] * alpha + functools.reduce(jnp.add, w)
            wb = jnp.concatenate([b.astype(jnp.bfloat16) for b in w], axis=1)
            acc[h, lo:hi, :] = acc[h, lo:hi, :] * alpha + jnp.dot(
                wb, values, preferred_element_type=jnp.float32
            )

    def onward(source, zs, p):
        @pl.when((zs < z) & (z < n_z - 1))
        def _():
            send(source, p, above, 0)

        @pl.when((zs > z) & (z > 0))
        def _():
            send(source, p, below, 0)

    def receive_z(zs, p):
        source = device(zs, y, core)
        arrived(source, p)
        onward(source, zs, p)
        if n_y == 2 and p == EXTRA:

            @pl.when(not_by_line(zs))
            def _():
                send(source, p, across, 4)

        elif n_y == 2:
            send(source, p, across, 1)
        send(source, p, partner, 2)

    def receive_extra(zs):
        @pl.when(by_line(zs))
        def _():
            source = device(zs, 1 - y, core)
            arrived(source, EXTRA)
            onward(source, zs, EXTRA)
            send(source, EXTRA, partner, 2)

    def receive_far(d):
        low = z - d

        @pl.when(low >= 0)
        def _():
            pltpu.make_async_copy(far_cq.at[low], far_cq.at[low], far_recv.at[low]).wait()

            @pl.when(z < last)
            def _():
                far_copy(low, above).start()

    def receive_line(d, i):
        for zs, inside in ((z - d, z - d >= 0), (z + d, z + d < n_z)):

            @pl.when(inside)
            def _():
                receive_z(zs, ORDER[i])
                if n_y == 2 and i == PIECES - 1:
                    receive_extra(zs)

    def receive_y(zs, i):
        source = device(zs, 1 - y, core)
        p = ORDER[i]

        def take():
            arrived(source, p)
            send(source, p, partner, 2)

        if p == EXTRA:
            pl.when(not_by_line(zs))(take)
        else:
            take()

    def receive_pair(i):
        receive_y(z, i)
        if ORDER[i] == EXTRA:
            source = device(z, 1 - y, core)

            @pl.when(z < n_z - 2)
            def _():
                send(source, EXTRA, above, 0)

            @pl.when(z > 1)
            def _():
                send(source, EXTRA, below, 3)

    pltpu.make_async_copy(q.at[:, pl.ds(0, many)], q.at[:, pl.ds(0, many)], query_sem).wait()
    pair_arrived(partner)
    mark = places(chip)
    for h in range(KVH):
        attend(h, [chip], [mark])
        receive_line(1, h)
        if n_y == 2:
            receive_pair(h)

    def step(t, carry):
        zs, zb = z_at(t), z_at(t - 1)
        pair_arrived(device(zs, y, 1 - core))
        chips = [zs * n_y + y]
        if n_y == 2:
            pair_arrived(device(zb, 1 - y, 1 - core))
            chips.append(zb * n_y + 1 - y)
        marks = [places(c) for c in chips]
        for h in range(KVH):
            attend(h, chips, marks)

            @pl.when(t < n_z - 1)
            def _():
                receive_line(t + 1, h)

            if n_y == 2:
                receive_y(zs, h)
        return carry

    lax.fori_loop(1, n_z, step, 0)
    chips = []
    if n_y == 2:
        zb = z_at(jnp.int32(n_z - 1))
        pair_arrived(device(zb, 1 - y, 1 - core))
        chips = [zb * n_y + 1 - y]
    marks = [places(c) for c in chips]
    for h in range(KVH):
        if n_y == 2:
            attend(h, chips, marks)
        mixed = acc[h] / jnp.sum(row_sum[h], axis=1, keepdims=True)
        for g in range(GROUP):
            column = (h * GROUP + g) * HD
            out_ref[:, column : column + HD] = mixed[
                g * prompt_rows : (g + 1) * prompt_rows, :
            ].astype(jnp.bfloat16)
        rows16[h] = mixed[many:, :]
        for g in range(GROUP):
            column = (h * GROUP + g) * HD
            cont_ref[:, column : column + HD] = rows16[
                h, g * conts : (g + 1) * conts, :
            ].astype(jnp.bfloat16)

    @pl.when(z < n_z - 1)
    def _():
        sent(me, 0)

    @pl.when(z > 0)
    def _():
        sent(me, 3)

    sent(me, 2)
    if n_y == 2:
        pair = device(z, 1 - y, core)
        sent(me, 1, PIECES - 1)
        sent(me, 4, 1)

        @pl.when(z < n_z - 2)
        def _():
            sent(pair, 0, 1)

        @pl.when(z > 1)
        def _():
            sent(pair, 3, 1)

    def drain(zs, carry):
        source = device(zs, y, core)
        middle = ((zs < z) & (z < n_z - 1)) | ((zs > z) & (z > 0))

        @pl.when(middle)
        def _():
            sent(source, 0)

        @pl.when(zs != z)
        def _():
            if n_y == 2:
                sent(source, 1, PIECES - 1)
            sent(source, 2)

        if n_y == 2:
            other = device(zs, 1 - y, core)

            @pl.when((zs != z) & not_by_line(zs))
            def _():
                sent(source, 4, 1)

            @pl.when(middle & by_line(zs))
            def _():
                sent(other, 0, len(BY_LINE))

            sent(other, 2)
        return carry

    lax.fori_loop(0, n_z, drain, 0)


HEADS = (0, 1, 2, 3)
BY_LINE = (3,)
LEAD = 2
AHEAD = 2


def pack_rows(values):
    lane = lax.broadcasted_iota(jnp.int32, (8, HD), 1)
    tile = jnp.zeros((8, HD), jnp.float32)
    for i in range(values.shape[0] // 8):
        tile = jnp.where(lane == i, values[8 * i : 8 * i + 8, :], tile)
    return tile


def unpack_rows(tile, first, count):
    lane = lax.broadcasted_iota(jnp.int32, (8, HD), 1)
    blocks = [
        jnp.max(jnp.where(lane == i, tile, -3e38), axis=1, keepdims=True)
        for i in range(first // 8, (first + count) // 8)
    ]
    return jnp.concatenate(blocks, axis=0)


def plane_kernel(
    n_z,
    ck_ref,
    cv_ref,
    nq_ref,
    nk_ref,
    nv_ref,
    cq_hbm,
    sk_ref,
    sv_ref,
    start_hbm,
    prefix_hbm,
    length_hbm,
    out_ref,
    cont_ref,
    kv,
    q,
    sk,
    sv,
    rows16,
    limit,
    row_max,
    row_sum,
    acc,
    cq,
    far_cq,
    far_rows,
    part_out,
    part_in,
    lse_out,
    lse_in,
    start_ref,
    prefix_ref,
    length_ref,
    local_sem,
    query_sem,
    suffix_sem,
    small_sem,
    recv_sem,
    send_sem,
    far_recv,
    far_send,
    part_recv,
    part_send,
):
    n_y = 2
    half = ck_ref.shape[0]
    prompt_rows = nq_ref.shape[0]
    conts = cq_hbm.shape[0]
    suffix_rows = sk_ref.shape[1]
    many = GROUP * prompt_rows
    few = GROUP * conts
    total = many + few
    me = lax.axis_index("ctx")
    core = me % CORES
    chip = me // CORES
    y = chip % n_y
    z = chip // n_y
    last = n_z - 1
    lines = n_z - 2
    plane = n_y * CORES
    span = plane * half

    def device(zz, yy, cc):
        return (zz * n_y + yy) * CORES + cc

    partner = device(z, y, 1 - core)
    across = device(z, 1 - y, core)
    above = device(z + 1, y, core)
    below = device(z - 1, y, core)

    barrier = pltpu.get_barrier_semaphore()

    def greet(target):
        pl.semaphore_signal(barrier, inc=1, device_id={"ctx": target}, device_id_type=MESH)

    greet(partner)
    greet(across)

    @pl.when(z > 0)
    def _():
        greet(below)

    @pl.when(z < last)
    def _():
        greet(above)

    for h in HEADS:
        cols = pl.ds(h * HD, HD)
        for kind, pair in enumerate(((ck_ref, cv_ref), (nk_ref, nv_ref))):
            for i, ref in enumerate(pair):
                pltpu.make_async_copy(ref.at[:, cols], kv.at[me, h, kind, i], local_sem.at[h]).start()
    small = [
        pltpu.make_async_copy(src, dst, small_sem.at[i])
        for i, (src, dst) in enumerate(
            (
                (cq_hbm, cq),
                (start_hbm, start_ref),
                (prefix_hbm, prefix_ref),
                (length_hbm, length_ref),
            )
        )
    ]
    for copy in small:
        copy.start()
    suffix_copies = [
        pltpu.make_async_copy(sk_ref, sk, suffix_sem.at[0]),
        pltpu.make_async_copy(sv_ref, sv, suffix_sem.at[1]),
    ]
    for copy in suffix_copies:
        copy.start()

    line_neighbours = (z + n_z - 1) // n_z + (2 * n_z - 2 - z) // n_z
    pl.semaphore_wait(barrier, n_y + line_neighbours)

    def full(source, h):
        return kv.at[source, h]

    def cached(source, h):
        return kv.at[source, h, 0]

    def send(ref, source, h, target, kind):
        pltpu.make_async_remote_copy(
            src_ref=ref,
            dst_ref=ref,
            send_sem=send_sem.at[source, kind],
            recv_sem=recv_sem.at[source, h],
            device_id={"ctx": target},
            device_id_type=MESH,
        ).start()

    def arrived(ref, source, h):
        pltpu.make_async_copy(ref, ref, recv_sem.at[source, h]).wait()

    def far_copy(zs, target):
        return pltpu.make_async_remote_copy(
            src_ref=far_cq.at[zs],
            dst_ref=far_cq.at[zs],
            send_sem=far_send.at[zs],
            recv_sem=far_recv.at[zs],
            device_id={"ctx": target},
            device_id_type=MESH,
        )

    for h in HEADS:
        pltpu.make_async_copy(full(me, h), full(me, h), local_sem.at[h]).wait()

        @pl.when(z < last)
        def _():
            send(full(me, h), me, h, above, 0)

        send(full(me, h), me, h, across, 1)

        @pl.when(z > 0)
        def _():
            send(cached(me, h), me, h, below, 3)

        send(full(me, h), me, h, partner, 2)

    small[0].wait()

    @pl.when(z < last)
    def _():
        pltpu.make_async_remote_copy(
            src_ref=cq,
            dst_ref=far_cq.at[z],
            send_sem=far_send.at[z],
            recv_sem=far_recv.at[z],
            device_id={"ctx": above},
            device_id_type=MESH,
        ).start()

    for h in HEADS:
        for g in range(GROUP):
            pltpu.make_async_copy(
                nq_ref.at[:, pl.ds((h * GROUP + g) * HD, HD)],
                q.at[h, pl.ds(g * prompt_rows, prompt_rows)],
                query_sem,
            ).start()
    near = jnp.minimum(z, last - z)

    def z_at(t):
        step = (t + 1) // 2
        both = z + step * (1 - 2 * (t % 2))
        far = jnp.where(z + z < last, t, last - t)
        return jnp.where(t <= 2 * near, both, far)

    row = lax.broadcasted_iota(jnp.int32, (total, HD), 0)
    limit[...] = jnp.where(row < many, (me % plane) * prompt_rows + row % prompt_rows, HIDDEN)
    row_max[...] = jnp.full_like(row_max, -1e30)
    row_sum[...] = jnp.zeros_like(row_sum)
    acc[...] = jnp.zeros_like(acc)

    def spread(rows):
        for h in range(KVH):
            for g in range(GROUP):
                column = (h * GROUP + g) * HD
                rows16[h, g * conts : (g + 1) * conts, :] = rows[:, column : column + HD].astype(
                    jnp.float32
                )

    for zs in range(last):

        @pl.when(zs >= z)
        def _():
            far_cq[zs] = jnp.zeros(far_cq.shape[1:], jnp.bfloat16)

    spread(cq)
    q[:, many:, :] = rows16[...].astype(jnp.bfloat16)
    for copy in small[1:]:
        copy.wait()
    for copy in suffix_copies:
        copy.wait()
    for h in range(KVH):
        keys = sk[:, :, h * HD : (h + 1) * HD].reshape(conts * suffix_rows, HD)
        values = sv[:, :, h * HD : (h + 1) * HD].reshape(conts * suffix_rows, HD)
        s = lax.dot_general(
            q[h, many:, :], keys, (((1,), (1,)), ((), ())), preferred_element_type=jnp.float32
        )
        who = lax.broadcasted_iota(jnp.int32, s.shape, 0) % conts
        column = lax.broadcasted_iota(jnp.int32, s.shape, 1)
        reach = jnp.zeros_like(who)
        for c in range(conts):
            reach = jnp.where(who == c, length_ref[c], reach)
        seen = (column // suffix_rows == who) & (column % suffix_rows < reach)
        s = jnp.where(seen, s * SCALE2, -1e30)
        top = jnp.max(s, axis=1, keepdims=True)
        w = jnp.exp2(s - top)
        row_max[h, many:, :] = jnp.broadcast_to(top, (few, HD))
        row_sum[h, many:, :] = jnp.broadcast_to(jnp.sum(w, axis=1, keepdims=True), (few, HD))
        acc[h, many:, :] = jnp.dot(
            w.astype(jnp.bfloat16), values, preferred_element_type=jnp.float32
        )

    window_first = start_ref[0]
    prefix_last = prefix_ref[0]

    def cache_bias(zs):
        position = zs * span + lax.broadcasted_iota(jnp.int32, (1, span), 1)
        return jnp.where((position >= window_first) & (position < prefix_last), 0.0, -1e30)

    def plane_rows(zs, h, kind, i):
        return kv[pl.ds(zs * plane, plane), h, kind, i].reshape(span, HD)

    def summed(values):
        return jnp.concatenate([values, jnp.ones(values.shape, jnp.bfloat16)], axis=1)

    def attend(h, zs, mode, bias):
        keys = plane_rows(zs, h, 0, 0)
        values = plane_rows(zs, h, 0, 1)
        if mode != "cache":
            keys = jnp.concatenate([keys, plane_rows(zs, h, 1, 0)], axis=0)
            values = jnp.concatenate([values, plane_rows(zs, h, 1, 1)], axis=0)
        values = summed(values)
        cut = (total // 2 + 15) // 16 * 16
        for lo, hi in ((0, cut), (cut, total)):
            s = lax.dot_general(
                q[h, lo:hi, :], keys, (((1,), (1,)), ((), ())), preferred_element_type=jnp.float32
            )
            blocks = []
            for b in range(keys.shape[0] // HD):
                part = s[:, b * HD : (b + 1) * HD] * SCALE2
                if b < span // HD:
                    part = part + bias[:, b * HD : (b + 1) * HD]
                elif mode == "own":
                    at = (b - span // HD) * HD + lax.broadcasted_iota(jnp.int32, (1, HD), 1)
                    part = jnp.where(at <= limit[lo:hi, :], part, -1e30)
                blocks.append(part)
            peak = functools.reduce(jnp.maximum, blocks)
            old = row_max[h, lo:hi, :]
            new = jnp.maximum(old, jnp.max(peak, axis=1, keepdims=True))
            alpha = jnp.exp2(old - new)
            w = [jnp.exp2(b - new) for b in blocks]
            row_max[h, lo:hi, :] = new
            wb = jnp.concatenate([b.astype(jnp.bfloat16) for b in w], axis=1)
            mixed = jnp.dot(wb, values, preferred_element_type=jnp.float32)
            acc[h, lo:hi, :] = acc[h, lo:hi, :] * alpha + mixed[:, :HD]
            row_sum[h, lo:hi, :] = row_sum[h, lo:hi, :] * alpha + mixed[:, HD:]

    def foreign():
        for zs in range(last):
            rows = far_cq.at[zs]
            for h in range(KVH):
                for g in range(GROUP):
                    column = (h * GROUP + g) * HD
                    first = zs * few + g * conts
                    far_rows[h, first : first + conts, :] = rows[:, column : column + HD].astype(
                        jnp.float32
                    )
        sums = []
        for h in range(KVH):
            s = lax.dot_general(
                far_rows[h].astype(jnp.bfloat16),
                plane_rows(z, h, 1, 0),
                (((1,), (1,)), ((), ())),
                preferred_element_type=jnp.float32,
            )
            s = s * SCALE2
            top = jnp.max(s, axis=1, keepdims=True)
            w = jnp.exp2(s - top)
            both = jnp.dot(
                w.astype(jnp.bfloat16),
                summed(plane_rows(z, h, 1, 1)),
                preferred_element_type=jnp.float32,
            )
            under = both[:, HD:]
            mixed = both[:, :HD] / under
            for zs in range(last):
                part_out[zs, h * few : (h + 1) * few, :] = mixed[zs * few : (zs + 1) * few, :]
            sums.append(top + jnp.log2(under))
        for zs in range(last):
            lse_out[zs] = pack_rows(
                jnp.concatenate([level[zs * few : (zs + 1) * few, :] for level in sums], axis=0)
            )

    def part_copies(zs):
        return [
            pltpu.make_async_remote_copy(
                src_ref=src.at[zs],
                dst_ref=dst.at[z],
                send_sem=part_send.at[zs, i],
                recv_sem=part_recv.at[z, i],
                device_id={"ctx": device(zs, y, core)},
                device_id_type=MESH,
            )
            for i, (src, dst) in enumerate(((part_out, part_in), (lse_out, lse_in)))
        ]

    def merge(zs):
        for i, ref in enumerate((part_in, lse_in)):
            pltpu.make_async_copy(ref.at[zs], ref.at[zs], part_recv.at[zs, i]).wait()
        tile = lse_in[zs]
        for h in range(KVH):
            level = unpack_rows(tile, h * few, few)
            old = row_max[h, many:, :]
            new = jnp.maximum(old, level)
            alpha = jnp.exp2(old - new)
            beta = jnp.exp2(level - new)
            row_max[h, many:, :] = new
            row_sum[h, many:, :] = row_sum[h, many:, :] * alpha + beta
            acc[h, many:, :] = (
                acc[h, many:, :] * alpha + part_in[zs, h * few : (h + 1) * few, :] * beta
            )

    def receive_far(d):
        low = z - d

        @pl.when(low >= 0)
        def _():
            pltpu.make_async_copy(far_cq.at[low], far_cq.at[low], far_recv.at[low]).wait()

            @pl.when(z < last)
            def _():
                far_copy(low, above).start()

    def receive_line(d, i):
        h = HEADS[i]
        low, high = z - d, z + d

        @pl.when(low >= 0)
        def _():
            source = device(low, y, core)
            ref = full(source, h)
            arrived(ref, source, h)

            @pl.when(z < last)
            def _():
                send(ref, source, h, above, 0)

            if h in BY_LINE:

                @pl.when(low >= lines)
                def _():
                    send(ref, source, h, across, 1)

            else:
                send(ref, source, h, across, 1)
            send(ref, source, h, partner, 2)
        @pl.when(high < n_z)
        def _():
            source = device(high, y, core)
            ref = cached(source, h)
            arrived(ref, source, h)

            @pl.when(z > 0)
            def _():
                send(ref, source, h, below, 0)

            send(ref, source, h, across, 1)
            send(ref, source, h, partner, 2)

    def receive_y(zs, i):
        h = HEADS[i]
        source = device(zs, 1 - y, core)

        def take(ref):
            arrived(ref, source, h)
            send(ref, source, h, partner, 2)

        pl.when(zs <= z)(lambda: take(full(source, h)))
        if h in BY_LINE:
            pl.when((zs < lines) & (zs < z) & (z < last))(
                lambda: send(full(source, h), source, h, above, 0)
            )
        pl.when(zs > z)(lambda: take(cached(source, h)))

    def receive_own(i):
        h = HEADS[i]
        arrived(full(across, h), across, h)
        send(full(across, h), across, h, partner, 2)
        if h in BY_LINE:

            @pl.when((z < last) & (z < lines))
            def _():
                send(full(across, h), across, h, above, 0)

    def pair_arrived(zs, i):
        h = HEADS[i]
        for yy in (y, 1 - y):
            source = device(zs, yy, 1 - core)
            pl.when(zs <= z)(lambda source=source: arrived(full(source, h), source, h))
            pl.when(zs > z)(lambda source=source: arrived(cached(source, h), source, h))

    pltpu.make_async_copy(
        q.at[pl.ds(0, KVH), pl.ds(0, many)], q.at[pl.ds(0, KVH), pl.ds(0, many)], query_sem
    ).wait()
    def receive(t, i):
        q, r = divmod(i + AHEAD - 1, KVH)
        receive_line(t + 1 + q, r)
        q, r = divmod(i + LEAD, KVH)
        if isinstance(t, int):
            receive_own(r) if t + q == 0 else receive_y(z_at(t + q), r)
        else:
            pl.when(t + q < n_z)(lambda: receive_y(z_at(t + q), r))

    def give(zs):
        for copy in part_copies(zs):
            copy.start()

    for j in range(AHEAD - 1):
        receive_line(1 + j // KVH, j % KVH)
    for j in range(LEAD):
        receive_own(j)
    bias = cache_bias(z)
    for i, h in enumerate(HEADS):
        receive(0, i)
        for yy in (y, 1 - y):
            source = device(z, yy, 1 - core)
            arrived(full(source, h), source, h)
        attend(h, z, "own", bias)
        if i == 0:
            receive_far(1)

    receive_far(2)

    def step(t, carry):
        zs = z_at(t)
        bias = cache_bias(zs)
        for i, h in enumerate(HEADS):
            receive(t, i)
            pair_arrived(zs, i)
            pl.when(zs < z)(lambda: attend(h, zs, "all", bias))
            pl.when(zs > z)(lambda: attend(h, zs, "cache", bias))
            if i > 0:

                @pl.when((t == 1) & (z > 0))
                def _():
                    if i == 1:
                        for d in range(3, n_z):
                            receive_far(d)
                    if i == 2:
                        foreign()
                    if i == 3:
                        for d in range(1, n_z):
                            pl.when(z >= d)(lambda: give(z - d))

        return carry

    lax.fori_loop(1, n_z, step, 0)

    def collect(zs, carry):
        merge(zs)
        return carry

    lax.fori_loop(z + 1, n_z, collect, 0)
    for h in range(KVH):
        mixed = acc[h] / row_sum[h]
        for g in range(GROUP):
            column = (h * GROUP + g) * HD
            out_ref[:, column : column + HD] = mixed[
                g * prompt_rows : (g + 1) * prompt_rows, :
            ].astype(jnp.bfloat16)
        rows16[h] = mixed[many:, :]
        for g in range(GROUP):
            column = (h * GROUP + g) * HD
            cont_ref[:, column : column + HD] = rows16[
                h, g * conts : (g + 1) * conts, :
            ].astype(jnp.bfloat16)

    def sent(source, kind, count, cache_only=False):
        ref = kv.at[source, pl.ds(0, count)]
        if cache_only:
            ref = kv.at[source, pl.ds(0, count), 0]
        pltpu.make_async_copy(ref, ref, send_sem.at[source, kind]).wait()

    @pl.when(z < last)
    def _():
        sent(me, 0, KVH)
        pltpu.make_async_copy(cq, cq, far_send.at[z]).wait()

    @pl.when(z > 0)
    def _():
        sent(me, 3, KVH, True)

    sent(me, 1, KVH)
    sent(me, 2, KVH)

    def drain(zs, carry):
        source = device(zs, y, core)
        other = device(zs, 1 - y, core)

        @pl.when(zs < z)
        def _():
            @pl.when(z < last)
            def _():
                sent(source, 0, KVH)
                pltpu.make_async_copy(far_cq.at[zs], far_cq.at[zs], far_send.at[zs]).wait()

            pl.when(zs < lines)(lambda: sent(source, 1, KVH - len(BY_LINE)))
            pl.when(zs >= lines)(lambda: sent(source, 1, KVH))
            sent(source, 2, KVH)
            for copy in part_copies(zs):
                copy.wait_send()

        @pl.when(zs > z)
        def _():
            pl.when(z > 0)(lambda: sent(source, 0, KVH, True))
            sent(source, 1, KVH, True)
            sent(source, 2, KVH, True)
            sent(other, 2, KVH, True)

        @pl.when(zs <= z)
        def _():
            sent(other, 2, KVH)
            pl.when((z < last) & (zs < lines))(lambda: sent(other, 0, len(BY_LINE)))

        return carry

    lax.fori_loop(0, n_z, drain, 0)


def line_shape(mesh):
    chips = mesh.shape["ctx"] // CORES
    place = mesh.axis_names.index("ctx")
    index = [0] * mesh.devices.ndim
    index[place] = slice(None)
    coords = [getattr(d, "coords", None) for d in mesh.devices[tuple(index)]]
    n_y = 1
    if all(c is not None for c in coords) and len({c[1] for c in coords}) == 2:
        n_y = 2
    return chips // n_y, n_y


def solution(mesh):
    n_z, n_y = line_shape(mesh)
    n_ctx = mesh.shape["ctx"]

    def plane_body(ck, cv, nq, nk, nv, cq, sk, sv, ws, pfx, length):
        half = ck.shape[0]
        few = GROUP * cq.shape[0]
        total = GROUP * nq.shape[0] + few
        anywhere = pl.BlockSpec(memory_space=pl.ANY)
        vmem = pl.BlockSpec(memory_space=pltpu.VMEM)
        state = pltpu.VMEM((KVH, total, HD), jnp.float32)
        part = pltpu.VMEM((n_z, KVH * few, HD), jnp.float32)
        levels = pltpu.VMEM((n_z, 8, HD), jnp.float32)
        return pl.pallas_call(
            functools.partial(plane_kernel, n_z),
            out_shape=(
                pltpu.VMEM(nq.shape, jnp.bfloat16),
                pltpu.VMEM(cq.shape, jnp.bfloat16),
            ),
            in_specs=[anywhere] * 11,
            out_specs=(vmem, vmem),
            scratch_shapes=[
                pltpu.VMEM((n_ctx, KVH, 2, 2, half, HD), jnp.bfloat16),
                pltpu.VMEM((KVH, total, HD), jnp.bfloat16),
                pltpu.VMEM(sk.shape, jnp.bfloat16),
                pltpu.VMEM(sv.shape, jnp.bfloat16),
                pltpu.VMEM((KVH, few, HD), jnp.float32),
                pltpu.VMEM((total, HD), jnp.int32),
                state,
                state,
                state,
                pltpu.VMEM(cq.shape, jnp.bfloat16),
                pltpu.VMEM((n_z,) + cq.shape, jnp.bfloat16),
                pltpu.VMEM((KVH, few * (n_z - 1), HD), jnp.float32),
                part,
                part,
                levels,
                levels,
                pltpu.SMEM(ws.shape, jnp.int32),
                pltpu.SMEM(pfx.shape, jnp.int32),
                pltpu.SMEM(length.shape, jnp.int32),
                pltpu.SemaphoreType.DMA((KVH,)),
                pltpu.SemaphoreType.DMA,
                pltpu.SemaphoreType.DMA((2,)),
                pltpu.SemaphoreType.DMA((4,)),
                pltpu.SemaphoreType.DMA((n_ctx, KVH)),
                pltpu.SemaphoreType.DMA((n_ctx, 4)),
                pltpu.SemaphoreType.DMA((n_z,)),
                pltpu.SemaphoreType.DMA((n_z,)),
                pltpu.SemaphoreType.DMA((n_z, 2)),
                pltpu.SemaphoreType.DMA((n_z, 2)),
            ],
            compiler_params=pltpu.CompilerParams(
                collective_id=0, has_side_effects=True, vmem_limit_bytes=60 * 1024 * 1024
            ),
        )(ck, cv, nq, nk, nv, cq, sk, sv, ws, pfx, length)

    def body(ck, cv, nq, nk, nv, cq, sk, sv, ws, pfx, length):
        half, width = ck.shape
        rows = nq.shape[0]
        conts = cq.shape[0]
        total = GROUP * (rows + conts)
        anywhere = pl.BlockSpec(memory_space=pl.ANY)
        vmem = pl.BlockSpec(memory_space=pltpu.VMEM)
        return pl.pallas_call(
            functools.partial(kernel, n_z, n_y),
            out_shape=(
                pltpu.VMEM(nq.shape, jnp.bfloat16),
                pltpu.VMEM(cq.shape, jnp.bfloat16),
            ),
            in_specs=[anywhere] * 11,
            out_specs=(vmem, vmem),
            scratch_shapes=[
                pltpu.VMEM((n_ctx, 2, 2 * half, width), jnp.bfloat16),
                pltpu.VMEM((KVH, total, HD), jnp.bfloat16),
                pltpu.VMEM(sk.shape, jnp.bfloat16),
                pltpu.VMEM(sv.shape, jnp.bfloat16),
                pltpu.VMEM((KVH, GROUP * conts, HD), jnp.float32),
                pltpu.VMEM((total, HD), jnp.int32),
                pltpu.VMEM((KVH, total, HD), jnp.float32),
                pltpu.VMEM((KVH, total, HD), jnp.float32),
                pltpu.VMEM((KVH, total, HD), jnp.float32),
                pltpu.VMEM(cq.shape, jnp.bfloat16),
                pltpu.SMEM(ws.shape, jnp.int32),
                pltpu.SMEM(pfx.shape, jnp.int32),
                pltpu.SMEM(length.shape, jnp.int32),
                pltpu.SemaphoreType.DMA((PIECES,)),
                pltpu.SemaphoreType.DMA,
                pltpu.SemaphoreType.DMA((2,)),
                pltpu.SemaphoreType.DMA((n_ctx, PIECES)),
                pltpu.SemaphoreType.DMA((n_ctx,)),
                pltpu.SemaphoreType.DMA((n_ctx, 5)),
                pltpu.SemaphoreType.DMA((4,)),
            ],
            compiler_params=pltpu.CompilerParams(
                collective_id=0, has_side_effects=True, vmem_limit_bytes=60 * 1024 * 1024
            ),
        )(ck, cv, nq, nk, nv, cq, sk, sv, ws, pfx, length)

    part = P(("grp", "ctx"), None)
    part3 = P(("grp", "ctx"), None, None)
    in_specs = (part,) * 6 + (part3, part3, P("grp"), P("grp"), P(("grp", "ctx")))
    return jax.shard_map(
        plane_body if n_y == 2 and n_z > 2 else body,
        mesh=mesh, in_specs=in_specs, out_specs=(part, part), check_vma=False
    )
```
